256 devices in a mesh: ens: 8 (over y, core), gx: 4 (over x), gy: 8 (over z).
Axes of the slice: x: 4, y: 4, z: 8, core: 2. Of those that a mesh axis runs over, the one named last changes fastest.
Arguments:
- log_conductivity: float32 [256, 128, 256], P(('ens', 'gx'), 'gy'), parts along dimension 0, may hold values from -3 to 3
- state: float32 [256, 128, 256], P(('ens', 'gx'), 'gy'), parts along dimension 0, may hold values from -6 to 6
- gradient: float32 [256, 128, 256], P(('ens', 'gx'), 'gy'), parts along dimension 0, may hold values from -60 to 60
- prior_sample: float32 [256, 128, 256], P(('ens', 'gx'), 'gy'), parts along dimension 0, may hold values from -6 to 6
- sensor_cells: int32 [131072], P(('ens', 'gx', 'gy')), parts along dimension 0, may hold values from 0 to 1048575, as said below
- noise_precision: float32 [131072], P(('ens', 'gx', 'gy')), parts along dimension 0, may hold values from 20 to 200
Outputs:
- step_field: float32 [256, 128, 256], P(('ens', 'gx'), 'gy'), parts along dimension 0
- residual: float32 [256, 128, 256], P(('ens', 'gx'), 'gy'), parts along dimension 0
The draws below stay inside these ranges and needn't reach their ends.
There are 8 independent parts, one for each index of `ens`. The reference program is written for one: setup_inputs(seed, part) draws one part's arguments, and reference() takes and returns one part's arrays. A program takes and returns all parts, laid end to end along the dimension named above; each array names one. Nothing has to cross between parts.
Inputs may be any that keep to these rules, and one draw needn't show every extreme that they name: `sensor_cells`: sensors t * 512 to (t + 1) * 512 - 1 observe cells inside the block of cells held by the t-th device in the order gx, then gy (blocks of 8 x 16 x 256 cells); a cell may be observed by several sensors.
All inputs are finite; a program needn't handle non-finite values.
Results may differ from the reference program's by a relative error of at most 0.00015.
Values sent between devices are 32-bit elements; how exact they have to be, the bound alone decides.
A program may use at most 128 MiB of HBM per device.

```python
import math
import jax
import jax.numpy as jnp

CX = 8
CY = 16
CZ = 256
SENS_DEV = 512
LEVELS = 3
SWEEPS = 1
COARSE_SWEEPS = 6
VCYCLES = 1
CG_ITERS = 2
NX = 32
NY = 128
NZ = 256
SENSORS = 16384


def draw_gradient(key, part):
    first_key, second_key = jax.random.split(jax.random.fold_in(key, 17))
    extent = (NX, NY, NZ)
    along_x = jnp.arange(NX, dtype=jnp.float32)[:, None, None] / (NX - 1)
    along_y = jnp.arange(NY, dtype=jnp.float32)[None, :, None] / (NY - 1)
    exponent = 0.5 * (along_x + along_y)
    random_part = jnp.clip(jax.random.normal(first_key, extent, jnp.float32), -4.0, 4.0)
    roughness = jnp.exp(jax.random.uniform(second_key, extent, jnp.float32, -0.35, 0.35))
    return random_part * roughness * jnp.power(10.0, exponent)


def draw_sensor_cells(key, part):
    keys = jax.random.split(jax.random.fold_in(key, 29), 3)
    slot_block = jnp.arange(SENSORS, dtype=jnp.int32) // SENS_DEV
    blocks_y = NY // CY
    row_index = slot_block // blocks_y * CX + jax.random.randint(keys[0], (SENSORS,), 0, CX, dtype=jnp.int32)
    column_index = slot_block % blocks_y * CY + jax.random.randint(keys[1], (SENSORS,), 0, CY, dtype=jnp.int32)
    depth_index = jax.random.randint(keys[2], (SENSORS,), 0, CZ, dtype=jnp.int32)
    return (row_index * NY + column_index) * NZ + depth_index


def shard_levels(rng, dims, shards, smallest, top_value):
    loudness, own = 1.0, jax.random.fold_in(rng, 6)
    for dim, blocks in shards:
        draws = jnp.exp(jax.random.uniform(jax.random.fold_in(own, dim), (blocks,), jnp.float32, smallest / len(shards), top_value / len(shards)))
        loudness = loudness * jnp.repeat(draws, dims[dim] // blocks).reshape([-1 if axis == dim else 1 for axis in range(len(dims))])
    return loudness


def scatter_about(rng, dims, scale, bound, pieces=(), held_as=jnp.bfloat16):
    values = scale * jax.random.normal(rng, dims, jnp.float32)
    if pieces:
        values = values * shard_levels(rng, dims, pieces, -0.22, 0.18)
    return jnp.clip(values, -bound, bound).astype(held_as)


def setup_inputs(seed: int = 0, part: int = 0) -> dict:
    splits = jax.random.split(jax.random.key(seed), 7)
    own_keys = jax.random.split(jax.random.fold_in(splits[6], part), 7)
    return {
        "log_conductivity": scatter_about(own_keys[0], (NX, NY, NZ), 0.7, 3.0, ((0, 4), (1, 8)), jnp.float32),
        "state": scatter_about(own_keys[1], (NX, NY, NZ), 1.0, 6.0, ((0, 4), (1, 8)), jnp.float32),
        "gradient": draw_gradient(jax.random.fold_in(jax.random.fold_in(splits[6], part), 71), part),
        "prior_sample": scatter_about(own_keys[3], (NX, NY, NZ), 1.0, 6.0, ((0, 4), (1, 8)), jnp.float32),
        "sensor_cells": draw_sensor_cells(jax.random.fold_in(jax.random.fold_in(splits[6], part), 71), part),
        "noise_precision": jnp.clip(jnp.exp(math.log(200.0) - 2.3025851 * jax.random.uniform(own_keys[5], (SENSORS,), jnp.float32) ** shard_levels(own_keys[5], (SENSORS,), ((0, 32),), -0.2, 0.2)), 20.0, 200.0),
    }


DAMPING = 0.8
PRIOR_MASS = 0.5
PRIOR_STIFF = 1.0


def coarsen_sum(values):
    extent_x, extent_y, extent_z = values.shape
    blocks = values.reshape(extent_x // 2, 2, extent_y // 2, 2, extent_z // 2, 2)
    return blocks.sum(axis=(1, 3, 5))


def refine(values):
    return jnp.repeat(jnp.repeat(jnp.repeat(values, 2, axis=0), 2, axis=1), 2, axis=2)


def neighbours(padded):
    centre = padded[1:-1, 1:-1, :]
    border = jnp.zeros_like(centre[:, :, :1])
    beside = (padded[:-2, 1:-1, :], padded[2:, 1:-1, :], padded[1:-1, :-2, :], padded[1:-1, 2:, :],
              jnp.concatenate([border, centre[:, :, :-1]], axis=2),
              jnp.concatenate([centre[:, :, 1:], border], axis=2))
    return beside, centre


def summed(entries):
    result = entries[0]
    for entry in entries[1:]:
        result = result + entry
    return result


def inside_flags(index_x, index_y, extent_x, extent_y, extent_z):
    index_z = jnp.arange(extent_z, dtype=jnp.int32)[None, None, :]
    return (index_x > 0, index_x < extent_x - 1, index_y > 0, index_y < extent_y - 1,
            index_z > 0, index_z < extent_z - 1)


def face_weights(cond_padded, level_scale, interior):
    beside, centre = neighbours(cond_padded)
    return tuple(level_scale * jnp.where(is_inner, 0.5 * (centre + neighbour), centre)
                 for is_inner, neighbour in zip(interior, beside))


def apply_operator(padded, couplings, diagonal):
    beside, centre = neighbours(padded)
    return diagonal * centre - summed([weight * neighbour for weight, neighbour in zip(couplings, beside)])


def prior_apply(padded):
    beside, centre = neighbours(padded)
    return PRIOR_MASS * centre + PRIOR_STIFF * (6.0 * centre - summed(list(beside)))


def sensitivity(cond_padded, state_padded, probe_padded, interior):
    cond_side, cond_mid = neighbours(cond_padded)
    state_side, state_mid = neighbours(state_padded)
    probe_side, probe_mid = neighbours(probe_padded)
    flux_mid = cond_mid * probe_mid
    return summed([jnp.where(is_inner, 0.5 * (flux_mid + cond_near * probe_near), flux_mid) * (state_mid - state_near)
                   for is_inner, cond_near, probe_near, state_near
                   in zip(interior, cond_side, probe_side, state_side)])


def misfit_gradient(cond_padded, state_padded, adjoint_padded, interior):
    cond_mid = neighbours(cond_padded)[1]
    state_side, state_mid = neighbours(state_padded)
    adjoint_side, adjoint_mid = neighbours(adjoint_padded)
    return cond_mid * summed([jnp.where(is_inner, 0.5, 1.0) * (state_mid - state_near) * (adjoint_mid - adjoint_near)
                              for is_inner, state_near, adjoint_near in zip(interior, state_side, adjoint_side)])


def smooth(iterate, source, couplings, diagonal, padder, sweeps):
    for sweep_index in range(sweeps):
        if iterate is None:
            iterate = DAMPING * source / diagonal
        else:
            iterate = iterate + DAMPING * (source - apply_operator(padder(iterate), couplings, diagonal)) / diagonal
    return iterate


def vcycle(source, depth_index, operators, padders, coarse_solve):
    if depth_index == len(operators):
        return coarse_solve(source)
    couplings, diagonal = operators[depth_index]
    iterate = smooth(None, source, couplings, diagonal, padders[depth_index], SWEEPS)
    defect = source - apply_operator(padders[depth_index](iterate), couplings, diagonal)
    iterate = iterate + refine(vcycle(coarsen_sum(defect), depth_index + 1, operators, padders, coarse_solve))
    return smooth(iterate, source, couplings, diagonal, padders[depth_index], SWEEPS)


def solve(source, operators, padders, coarse_solve):
    iterate = None
    for cycle_index in range(VCYCLES):
        if iterate is None:
            iterate = vcycle(source, 0, operators, padders, coarse_solve)
        else:
            couplings, diagonal = operators[0]
            defect = source - apply_operator(padders[0](iterate), couplings, diagonal)
            iterate = iterate + vcycle(defect, 0, operators, padders, coarse_solve)
    return iterate


def plain_pad(values):
    return jnp.pad(values, ((1, 1), (1, 1), (0, 0)))


def level_flags(values):
    extent_x, extent_y, extent_z = values.shape
    return inside_flags(jnp.arange(extent_x, dtype=jnp.int32)[:, None, None],
                        jnp.arange(extent_y, dtype=jnp.int32)[None, :, None], extent_x, extent_y, extent_z)


def reference(log_conductivity, state, gradient, prior_sample, sensor_cells, noise_precision):
    cond_levels = [jnp.exp(log_conductivity)]
    for depth_index in range(LEVELS - 1):
        cond_levels.append(coarsen_sum(cond_levels[-1]) / 8.0)
    operators = []
    for depth_index in range(LEVELS - 1):
        couplings = face_weights(plain_pad(cond_levels[depth_index]), float(2 ** depth_index),
                                 level_flags(cond_levels[depth_index]))
        operators.append((couplings, summed(list(couplings))))
    coarsest = LEVELS - 1
    coarse_couplings = face_weights(plain_pad(cond_levels[coarsest]), float(2 ** coarsest),
                                    level_flags(cond_levels[coarsest]))
    coarse_diagonal = summed(list(coarse_couplings))
    padders = [plain_pad] * (LEVELS - 1)

    def coarse_solve(source):
        return smooth(None, source, coarse_couplings, coarse_diagonal, plain_pad, COARSE_SWEEPS)

    fine_flags = level_flags(cond_levels[0])
    weight_field = jnp.zeros((NX * NY * NZ,), jnp.float32).at[sensor_cells].add(noise_precision).reshape(NX, NY, NZ)
    cond_padded = plain_pad(cond_levels[0])
    state_padded = plain_pad(state)

    def hessian_apply(direction):
        direction_padded = plain_pad(direction)
        change = solve(sensitivity(cond_padded, state_padded, direction_padded, fine_flags), operators, padders, coarse_solve)
        adjoint = solve(weight_field * change, operators, padders, coarse_solve)
        return misfit_gradient(cond_padded, state_padded, plain_pad(adjoint), fine_flags) + prior_apply(direction_padded)

    source = prior_apply(plain_pad(prior_sample)) - gradient
    step_field = jnp.zeros_like(source)
    residual = source
    direction = source
    norm_now = jnp.sum(residual * residual)
    for iteration in range(CG_ITERS):
        curved = hessian_apply(direction)
        step_length = norm_now / jnp.sum(direction * curved)
        step_field = step_field + step_length * direction
        residual = residual - step_length * curved
        norm_next = jnp.sum(residual * residual)
        direction = residual + (norm_next / norm_now) * direction
        norm_now = norm_next
    return step_field, residual
```

```python
import jax
import jax.numpy as jnp
from jax import lax
from jax.experimental import pallas as pl
from jax.experimental.pallas import tpu as pltpu
from jax.sharding import PartitionSpec as P

MESH = pl.DeviceIdType.MESH
F32 = jnp.float32

NX, NY, NZ = 8, 16, 256
H, H1 = 4, 2
RX, RX1 = NX + 2 * H, NX // 2 + 2 * H1
ROWS = NY + 2 * H
PX, PY = 4, 8
GX, GY = NX * PX, NY * PY
REACH = 2
WIN = 2 * REACH + 1
COARSE_SWEEPS = 6
SENSORS = 512
OMEGA = 0.8
DIRS = ((1, 0), (-1, 0), (0, 1), (0, -1), (1, 1), (1, -1), (-1, 1), (-1, -1))
UNROLL = 2


def kernel(logk_ref, state_ref, grad_ref, prior_ref, cells_ref, prec_ref,
           step_ref, resid_ref,
           lk, st, pr, src, c0, z2, vl, ystage, yrecv, ystage1, yrecv1,
           kk, ca, wd, cd, sd, gg, zz, vv, cp, pp,
           c1, ca1, wd1, b1, v1, r1, p2,
           gat, chunk, cond2, ca2, wd2, rhs2, sol, weight, kc, dots, dchunk,
           h_send, h_recv, h1_send, h1_recv, g_send, g_recv, d_send, d_recv):
    px = lax.axis_index("gx")
    py = lax.axis_index("gy")
    row = lax.broadcasted_iota(jnp.int32, (ROWS, NZ), 0)
    lane = lax.broadcasted_iota(jnp.int32, (ROWS, NZ), 1)
    y_at = py * NY + jnp.where(row < NY + H, row, row - ROWS)

    def loop(low, high, body, unroll=UNROLL):
        def step(i, carry):
            body(i)
            return carry
        lax.fori_loop(low, high, step, 0, unroll=unroll)

    def exists(dx, dy):
        return (px + dx >= 0) & (px + dx < PX) & (py + dy >= 0) & (py + dy < PY)

    def halo_copy(field, ys, yr, n, h, wx, k, send, recv, reverse):
        dx, dy = DIRS[k]
        if dy == 0:
            source = field.at[h + n - wx:h + n, 0:NY] if dx == 1 else field.at[h:h + wx, 0:NY]
            target = field.at[h - wx:h, 0:NY] if dx == 1 else field.at[h + n:h + n + wx, 0:NY]
        else:
            side = 1 if dy == 1 else 0
            if dx == 0:
                source, target = ys.at[side], yr.at[side, h:h + n]
            elif dx == 1:
                source, target = ys.at[side, n - h:n], yr.at[side, 0:h]
            else:
                source, target = ys.at[side, 0:h], yr.at[side, h + n:h + n + h]
        if reverse:
            dx, dy = -dx, -dy
        return pltpu.make_async_remote_copy(
            src_ref=source, dst_ref=target, send_sem=send.at[k], recv_sem=recv.at[k],
            device_id={"gx": px + dx, "gy": py + dy}, device_id_type=MESH)

    def halo_clear(field, yr, n, h):
        @pl.when(px == 0)
        def _():
            field[0:h, 0:NY] = jnp.zeros((h, NY, NZ), F32)
            yr[:, 0:h] = jnp.zeros((2, h, H, NZ), F32)

        @pl.when(px == PX - 1)
        def _():
            field[h + n:, 0:NY] = jnp.zeros((h, NY, NZ), F32)
            yr[:, h + n:] = jnp.zeros((2, h, H, NZ), F32)

        @pl.when(py == 0)
        def _():
            yr[1] = jnp.zeros((n + 2 * h, H, NZ), F32)

        @pl.when(py == PY - 1)
        def _():
            yr[0] = jnp.zeros((n + 2 * h, H, NZ), F32)

    def put(field, ys, i, j, value):
        field[i, 0:NY] = value
        ys[0, j] = value[0:H]
        ys[1, j] = value[NY - H:NY]

    def halo_send(field, ys, yr, n, h, wx, send, recv, count=8):
        for k in range(count):
            @pl.when(exists(*DIRS[k]))
            def _(k=k):
                halo_copy(field, ys, yr, n, h, wx, k, send, recv, False).start()

    def halo_wait(field, ys, yr, n, h, wx, send, recv, count=8):
        for k in range(count):
            @pl.when(exists(-DIRS[k][0], -DIRS[k][1]))
            def _(k=k):
                halo_copy(field, ys, yr, n, h, wx, k, send, recv, True).wait_recv()

        def place(i):
            field[i, NY:ROWS] = jnp.concatenate([yr[0, i], yr[1, i]], axis=0)
        loop(0, n + 2 * h, place, 4)

    def halo_done(field, ys, yr, n, h, wx, send, recv, count=8):
        for k in range(count):
            @pl.when(exists(*DIRS[k]))
            def _(k=k):
                halo_copy(field, ys, yr, n, h, wx, k, send, recv, False).wait_send()

    def fine(field, slot, wx):
        return (field, ystage.at[slot], yrecv.at[slot], NX, H, wx, h_send.at[slot], h_recv.at[slot])

    def coarse(slot):
        return (vl.at[slot], ystage1.at[slot], yrecv1.at[slot], NX // 2, H1, H1, h1_send.at[slot], h1_recv.at[slot])

    PEERS = [(dx, dy) for dy in (0, 1, -1, 2, -2) for dx in (1, 3, 2, 0) if (dx, dy) != (0, 0)]

    def gather_copy(g, dx, dy):
        return pltpu.make_async_remote_copy(
            src_ref=chunk.at[g], dst_ref=gat.at[g, REACH - dy, px],
            send_sem=g_send.at[g, REACH - dy, dx], recv_sem=g_recv.at[g, REACH - dy, px],
            device_id={"gx": lax.rem(px + dx, PX), "gy": py + dy}, device_id_type=MESH)

    def gather_arrival(g, dx, dy):
        from_x = lax.rem(px + dx, PX)
        return pltpu.make_async_remote_copy(
            src_ref=chunk.at[g], dst_ref=gat.at[g, REACH + dy, from_x],
            send_sem=g_send.at[g, REACH - dy, dx], recv_sem=g_recv.at[g, REACH + dy, from_x],
            device_id={"gx": from_x, "gy": py + dy}, device_id_type=MESH)

    def gather_send(g):
        for dx, dy in PEERS:
            @pl.when((py + dy >= 0) & (py + dy < PY))
            def _(dx=dx, dy=dy):
                gather_copy(g, dx, dy).start()
        gat[g, REACH, px] = chunk[g]

    def gather_wait(g, out):
        for dx, dy in PEERS:
            @pl.when((py + dy >= 0) & (py + dy < PY))
            def _(dx=dx, dy=dy):
                gather_arrival(g, dx, dy).wait_recv()
        for d in range(WIN):
            valid = (py - REACH + d >= 0) & (py - REACH + d < PY)
            whole = jnp.concatenate([gat[g, d, p] for p in range(PX)], axis=0)
            out[d] = jnp.where(valid, whole, 0.0)

    def gather_done(g):
        for dx, dy in PEERS:
            @pl.when((py + dy >= 0) & (py + dy < PY))
            def _(dx=dx, dy=dy):
                gather_copy(g, dx, dy).wait_send()

    OTHERS = [(dx, dy) for dy in range(PY) for dx in range(PX) if (dx, dy) != (0, 0)]

    def dot_copy(g, dx, dy, arrival):
        to_x, to_y = lax.rem(px + dx, PX), lax.rem(py + dy, PY)
        slot = to_x * PY + to_y if arrival else px * PY + py
        return pltpu.make_async_remote_copy(
            src_ref=dchunk.at[g], dst_ref=dots.at[g, slot],
            send_sem=d_send.at[g, dx * PY + dy], recv_sem=d_recv.at[g, slot],
            device_id={"gx": to_x, "gy": to_y}, device_id_type=MESH)

    def dot_send(g, values):
        folded = [jnp.sum(v[:, 0:NZ // 2] + v[:, NZ // 2:NZ], axis=0, keepdims=True) for v in values]
        part = jnp.concatenate(folded, axis=0)
        dchunk[g] = part
        for dx, dy in OTHERS:
            dot_copy(g, dx, dy, False).start()
        dots[g, px * PY + py] = part

    def dot_wait(g):
        for dx, dy in OTHERS:
            dot_copy(g, dx, dy, True).wait_recv()
        total = dots[g, 0]
        for slot in range(1, PX * PY):
            total = total + dots[g, slot]
        for dx, dy in OTHERS:
            dot_copy(g, dx, dy, False).wait_send()
        return [jnp.sum(total[i:i + 1], axis=1, keepdims=True) for i in range(total.shape[0])]

    def beside(field, i, value, s):
        return (field[i - 1], field[i + 1], pltpu.roll(value, s, 0), pltpu.roll(value, ROWS - s, 0),
                pltpu.roll(value, s, 1), pltpu.roll(value, NZ - s, 1))

    def coupled(coefs, field, i, value, s):
        near = beside(field, i, value, s)
        total = coefs[0, i] * near[0]
        for f in range(1, 6):
            total = total + coefs[f, i] * near[f]
        return total

    def swap(value, s, axis):
        index, size = (row, ROWS) if axis == 0 else (lane, NZ)
        return jnp.where((index & s) == 0, pltpu.roll(value, size - s, axis), pltpu.roll(value, s, axis))

    def block_sum(low, high, s):
        total = low + high
        total = total + swap(total, s, 1)
        return total + swap(total, s, 0)

    def pick_chunk(value):
        mine = ((row & 3) == 0) & ((row >> 2) == (lane & 3)) & (row < NY)
        return jnp.sum(jnp.where(mine, value, 0.0), axis=0, keepdims=True)

    def inside_yz(s):
        return (y_at >= s, y_at < GY - s, lane >= s, lane < NZ - s)

    def cell_inside(x):
        return jnp.where((x >= 0) & (x < PX * NX), ((y_at >= 0) & (y_at < GY)).astype(F32), 0.0) > 0.5

    barrier = pltpu.get_barrier_semaphore()
    fields = [(lk, 0), (st, 1), (pr, 2), (src, 3), (z2.at[0], 4), (c0, 5), (z2.at[1], 6)]
    for field, slot in fields:
        halo_clear(field, yrecv.at[slot], NX, H)
    for slot in range(4):
        halo_clear(vl.at[slot], yrecv1.at[slot], NX // 2, H1)
    for dx, dy in OTHERS:
        pl.semaphore_signal(barrier, inc=1, device_id={"gx": lax.rem(px + dx, PX), "gy": lax.rem(py + dy, PY)},
                            device_id_type=MESH)

    def bring(i):
        put(pr, ystage.at[2], i + H, i, prior_ref[i])
        put(lk, ystage.at[0], i + H, i, logk_ref[i])
        put(st, ystage.at[1], i + H, i, state_ref[i])
    loop(0, NX, bring)
    pl.semaphore_wait(barrier, len(OTHERS))

    send_prior, send_lk, send_st = fine(pr, 2, 1), fine(lk, 0, H), fine(st, 1, H)
    halo_send(*send_prior, count=4)
    halo_send(*send_lk)
    halo_send(*send_st)

    cells = cells_ref[...]
    at_xy = ((cells >> 15) - px * NX) * NY + ((cells >> 8) & (GY - 1)) - py * NY
    at_z = cells & (NZ - 1)
    hot_xy = lax.broadcasted_iota(jnp.int32, (NX * NY, SENSORS), 0) == at_xy
    hot_z = (lax.broadcasted_iota(jnp.int32, (NZ, SENSORS), 0) == at_z).astype(F32).astype(jnp.bfloat16)
    left = jnp.where(hot_xy, prec_ref[...], 0.0)
    total = jnp.zeros((NX * NY, NZ), F32)
    for part in range(3):
        piece = left.astype(jnp.bfloat16)
        left = left - piece.astype(F32)
        total = total + lax.dot_general(piece, hot_z, (((1,), (1,)), ((), ())), preferred_element_type=F32)
    for i in range(NX):
        weight[i] = total[i * NY:(i + 1) * NY]

    halo_wait(*send_prior, count=4)

    def start_source(i):
        value = pr[i + H]
        near = beside(pr, i + H, value, 1)
        away = near[0] + near[1] + near[2] + near[3]
        away = away + jnp.where(lane >= 1, near[4], 0.0) + jnp.where(lane < NZ - 1, near[5], 0.0)
        own = (6.5 * value - away)[0:NY] - grad_ref[i]
        put(src, ystage.at[3], i + H, i, own)
    loop(0, NX, start_source)
    send_src = fine(src, 3, H)
    halo_send(*send_src)

    halo_wait(*send_lk)

    def start_cond(i):
        kk[i] = jnp.exp(lk[i])
    loop(0, RX, start_cond)

    inner = inside_yz(1)

    def start_couplings(i):
        value = kk[i]
        x = px * NX + i - H
        near = beside(kk, i, value, 1)
        in_x = (x > 0, x < GX - 1)
        diag = None
        for f in range(6):
            ok = in_x[f] if f < 2 else inner[f - 2]
            a = 0.5 * (value + jnp.where(ok, near[f], value))
            ca[f, i] = jnp.where(ok, a, 0.0)
            diag = a if diag is None else diag + a
        wd[i] = jnp.where(cell_inside(x), OMEGA / diag, 0.0)
    loop(1, RX - 1, start_couplings, 1)

    def start_level1(i):
        c1[i] = block_sum(kk[2 * i], kk[2 * i + 1], 1) * 0.125
    loop(0, RX1, start_level1)

    for i in range(2):
        chunk[0, i:i + 1] = pick_chunk(block_sum(c1[H1 + 2 * i], c1[H1 + 2 * i + 1], 2) * 0.125)
    gather_send(0)

    inner1 = inside_yz(2)

    def start_couplings1(i):
        value = c1[i]
        x = px * NX + 2 * i - H
        near = beside(c1, i, value, 2)
        in_x = (x > 0, x < GX - 2)
        diag = None
        for f in range(6):
            ok = in_x[f] if f < 2 else inner1[f - 2]
            a = value + jnp.where(ok, near[f], value)
            ca1[f, i] = jnp.where(ok, a, 0.0)
            diag = a if diag is None else diag + a
        wd1[i] = jnp.where(cell_inside(x), OMEGA / diag, 0.0)
    loop(1, RX1 - 1, start_couplings1, 1)

    halo_wait(*send_st)

    def start_state(i):
        value = st[i]
        x = px * NX + i - H
        near = beside(st, i, value, 1)
        in_x = (x > 0, x < GX - 1)
        diag = None
        for f in range(6):
            ok = in_x[f] if f < 2 else inner[f - 2]
            d = jnp.where(ok, 0.5 * (value - near[f]), value)
            cd[f, i] = jnp.where(ok, d, 0.0)
            diag = d if diag is None else diag + d
        sd[i] = diag
    loop(1, RX - 1, start_state, 1)

    row8 = lax.broadcasted_iota(jnp.int32, (8, NZ), 0)
    lane8 = lax.broadcasted_iota(jnp.int32, (8, NZ), 1)
    y_in = lane8 & 3

    def coarse_beside(values, d):
        v = values[d]
        zero = jnp.zeros_like(v)
        low = values[d - 1] if d > 0 else zero
        high = values[d + 1] if d < WIN - 1 else zero
        return (pltpu.roll(v, 1, 0), pltpu.roll(v, 7, 0),
                jnp.where(y_in > 0, pltpu.roll(v, 1, 1), pltpu.roll(low, NZ - 3, 1)),
                jnp.where(y_in < 3, pltpu.roll(v, NZ - 1, 1), pltpu.roll(high, 3, 1)),
                pltpu.roll(v, 4, 1), pltpu.roll(v, NZ - 4, 1))

    def coarse_couplings():
        values = [cond2[d] for d in range(WIN)]
        for d in range(WIN):
            place = py - REACH + d
            y = place * 4 + y_in
            inside = (row8 > 0, row8 < 7, y > 0, y < GY // 4 - 1, lane8 >= 4, lane8 < NZ - 4)
            diag = None
            for f, near in enumerate(coarse_beside(values, d)):
                a = 2.0 * (values[d] + jnp.where(inside[f], near, values[d]))
                ca2[f, d] = jnp.where(inside[f], a, 0.0)
                diag = a if diag is None else diag + a
            wd2[d] = jnp.where((place >= 0) & (place < PY), OMEGA / diag, 0.0)

    def coarse_solve():
        def sweep(s, values):
            out = []
            for d in range(WIN):
                total = rhs2[d]
                for f, near in enumerate(coarse_beside(values, d)):
                    total = total + ca2[f, d] * near
                out.append((1.0 - OMEGA) * values[d] + wd2[d] * total)
            return tuple(out)
        values = lax.fori_loop(1, COARSE_SWEEPS, sweep, tuple(wd2[d] * rhs2[d] for d in range(WIN)))
        for d in range(WIN):
            sol[d] = values[d]
        cell = jnp.where(row < NY, row >> 2, jnp.where(row < NY + H, 0, 3))
        for i in range(4):
            x = 2 * px - 1 + i
            at = jnp.clip(x, 0, 7)
            own, high, low = (sol[d, pl.ds(at, 1), :] for d in (REACH, REACH + 1, REACH - 1))
            spread = jnp.where(row < NY, own, jnp.where(row < NY + H, high, low))
            spread = jnp.where((lane & 3) == cell, spread, 0.0)
            spread = spread + swap(spread, 1, 1)
            spread = spread + swap(spread, 2, 1)
            p2[i] = jnp.where((x >= 0) & (x < 8), spread, 0.0)

    def solve(source, n, reach, finish, first):
        def presmooth(i):
            vv[i] = wd[i] * source[i]
        loop(1, RX - 1, presmooth)

        def restrict(i):
            parts = []
            for j in range(2):
                at = 2 * i + j
                parts.append((1.0 - OMEGA) * source[at] + coupled(ca, vv, at, vv[at], 1))
            total = block_sum(parts[0], parts[1], 1)
            b1[i] = total
            v1[i] = wd1[i] * total
        loop(1, RX1 - 1, restrict, 1)

        def level1_residual(i):
            return (1.0 - OMEGA) * b1[i] + coupled(ca1, v1, i, v1[i], 2)
        for i in range(2):
            chunk[n + 1, i:i + 1] = pick_chunk(
                block_sum(level1_residual(H1 + 2 * i), level1_residual(H1 + 2 * i + 1), 2))
        gather_send(n + 1)
        for i in range(NX // 2):
            put(vl.at[n], ystage1.at[n], H1 + i, i, v1[H1 + i, 0:NY])
        send_vl = coarse(n)
        halo_send(*send_vl)
        if first:
            gather_wait(0, cond2)
            coarse_couplings()
        gather_wait(n + 1, rhs2)
        coarse_solve()
        halo_wait(*send_vl)
        gather_done(n + 1)
        halo_done(*send_vl)

        for i in range(RX1):
            v1[i] = vl[n, i] + p2[i // 2]

        def postsmooth1(i):
            v = v1[i]
            r1[i] = (1.0 - OMEGA) * v + wd1[i] * (b1[i] + coupled(ca1, v1, i, v, 2))
        loop(1, RX1 - 1, postsmooth1)

        def correct(i):
            for j in range(2):
                vv[2 * i + j] = vv[2 * i + j] + r1[i]
        loop(1, RX1 - 1, correct)

        def postsmooth(i):
            v = vv[i]
            finish(i, (1.0 - OMEGA) * v + wd[i] * (source[i] + coupled(ca, vv, i, v, 1)))
        loop(H - reach, H + NX + reach, postsmooth)

    def hessian(r, n, keep):
        def scaled(i):
            gg[i] = kk[i] * r[i]
        loop(0, RX, scaled)

        def sensitivity(i):
            value = gg[i]
            zz[i] = sd[i] * value + coupled(cd, gg, i, value, 1)
        loop(1, RX - 1, sensitivity)

        second = z2.at[n]

        def weighted(i, value):
            put(second, ystage.at[4 + 2 * n], i, i - H, weight[i - H] * value[0:NY])
        solve(zz, 2 * n, 0, weighted, n == 0)
        send_z2 = fine(second, 4 + 2 * n, H - 1)
        halo_send(*send_z2)
        halo_wait(*send_z2)
        halo_done(*send_z2)

        def adjoint(i, value):
            pp[i] = value
        solve(second, 2 * n + 1, 1, adjoint, False)

        def assemble(i):
            p = pp[i]
            value = r[i]
            near = beside(r, i, value, 1)
            away = near[0] + near[1] + near[2] + near[3]
            away = away + jnp.where(lane >= 1, near[4], 0.0) + jnp.where(lane < NZ - 1, near[5], 0.0)
            misfit = kk[i] * (sd[i] * p - coupled(cd, pp, i, p, 1))
            keep(i, (misfit + 6.5 * value - away)[0:NY])
        loop(H, H + NX, assemble)

    halo_wait(*send_src)

    def keep_first(i, value):
        put(c0, ystage.at[5], i, i - H, value)
    hessian(src, 0, keep_first)
    send_c0 = fine(c0, 5, H)
    halo_send(*send_c0)

    def first_products(i, sums):
        r, c = src[i, 0:NY], c0[i, 0:NY]
        return sums[0] + r * r, sums[1] + r * c
    zero = jnp.zeros((NY, NZ), F32)
    both = lax.fori_loop(H, H + NX, first_products, (zero, zero))
    dot_send(0, (both[0], both[1], zero, zero))
    halo_wait(*send_c0)

    def keep_second(i, value):
        kc[i - H] = value
    hessian(c0, 1, keep_second)

    rr, rc = dot_wait(0)[:2]
    alpha = rr / rc

    def second_products(i, sums):
        r, c = src[i + H, 0:NY], c0[i + H, 0:NY]
        later = r - alpha * c
        curved = c - alpha * kc[i]
        return (sums[0] + later * later, sums[1] + later * curved, sums[2] + later * c, sums[3] + r * curved)
    four = lax.fori_loop(0, NX, second_products, (zero, zero, zero, zero))
    dot_send(1, four)
    norm, product, cross, crossed = dot_wait(1)
    ratio = norm / rr
    beta = norm / (product + ratio * (cross + crossed) + ratio * ratio * rc)

    def finish(i):
        r, c = src[i + H, 0:NY], c0[i + H, 0:NY]
        later = r - alpha * c
        curved = c - alpha * kc[i]
        step_ref[i] = alpha * r + beta * (later + ratio * r)
        resid_ref[i] = later - beta * (curved + ratio * c)
    loop(0, NX, finish)

    halo_done(*send_prior, count=4)
    for done in (send_lk, send_st, send_src, send_c0):
        halo_done(*done)
    gather_done(0)


def scratch():
    vmem = lambda *shape: pltpu.VMEM(shape, F32)
    fine = lambda *lead: vmem(*lead, RX, ROWS, NZ)
    level1 = lambda *lead: vmem(*lead, RX1, ROWS, NZ)
    dma = pltpu.SemaphoreType.DMA
    return [
        fine(), fine(), fine(), fine(), fine(), fine(2), level1(4),
        vmem(7, 2, NX, H, NZ), vmem(7, 2, RX, H, NZ), vmem(4, 2, NX // 2, H, NZ), vmem(4, 2, RX1, H, NZ),
        fine(), fine(6), fine(), fine(6), fine(), fine(), fine(), fine(), vmem(1, 8, 128), fine(),
        level1(), level1(6), level1(), level1(), level1(), level1(), vmem(4, ROWS, NZ),
        vmem(5, WIN, PX, 2, NZ), vmem(5, 2, NZ), vmem(WIN, 8, NZ), vmem(6, WIN, 8, NZ), vmem(WIN, 8, NZ),
        vmem(WIN, 8, NZ), vmem(WIN, 8, NZ), vmem(NX, NY, NZ), vmem(NX, NY, NZ),
        vmem(2, PX * PY, 4, 128), vmem(2, 4, 128),
        dma((7, 8)), dma((7, 8)), dma((4, 8)), dma((4, 8)), dma((5, WIN, PX)), dma((5, WIN, PX)),
        dma((2, PX * PY)), dma((2, PX * PY)),
    ]


def on_device(log_conductivity, state, gradient, prior_sample, sensor_cells, noise_precision):
    block = jax.ShapeDtypeStruct(log_conductivity.shape, F32)
    vmem = pl.BlockSpec(memory_space=pltpu.VMEM)
    return pl.pallas_call(
        kernel,
        out_shape=(block, block),
        in_specs=[vmem] * 6,
        out_specs=(vmem, vmem),
        scratch_shapes=scratch(),
        compiler_params=pltpu.CompilerParams(
            collective_id=0, has_side_effects=True, vmem_limit_bytes=60 * 1024 * 1024),
    )(log_conductivity, state, gradient, prior_sample,
      sensor_cells.reshape(1, SENSORS), noise_precision.reshape(1, SENSORS))


def solution(mesh):
    field, sensors = P(("ens", "gx"), "gy", None), P(("ens", "gx", "gy"))
    return jax.shard_map(
        on_device,
        mesh=mesh,
        in_specs=(field, field, field, field, sensors, sensors),
        out_specs=(field, field),
        check_vma=False,
    )
```

```python
import jax
import jax.numpy as jnp
from jax import lax
from jax.experimental import pallas as pl
from jax.experimental.pallas import tpu as pltpu
from jax.sharding import PartitionSpec as P

MESH = pl.DeviceIdType.MESH
F32 = jnp.float32

NX, NY, NZ = 8, 16, 256
H, H1 = 4, 2
RX, RX1 = NX + 2 * H, NX // 2 + 2 * H1
ROWS = NY + 2 * H
PX, PY = 4, 8
GX, GY = NX * PX, NY * PY
REACH = 2
WIN = 2 * REACH + 1
COARSE_SWEEPS = 6
SENSORS = 512
OMEGA = 0.8
DIRS = ((1, 0), (-1, 0), (0, 1), (0, -1), (1, 1), (1, -1), (-1, 1), (-1, -1))
UNROLL = 2


def kernel(logk_ref, state_ref, grad_ref, prior_ref, cells_ref, prec_ref,
           step_ref, resid_ref,
           lk, st, pr, src, c0, z2, vl, ystage, yrecv, ystage1, yrecv1, grad, cells_in, prec_in, r1f, wkeep,
           kk, ca, wd, cd, sd, gg, zz, vv, cp, pp,
           c1, ca1, wd1, b1, v1, r1, p2,
           gat, chunk, cond2, ca2, wd2, rhs2, sol, weight, kc, dots, dchunk,
           h_send, h_recv, h1_send, h1_recv, g_send, g_recv, d_send, d_recv, in_sem):
    px = lax.axis_index("gx")
    py = lax.axis_index("gy")
    row = lax.broadcasted_iota(jnp.int32, (ROWS, NZ), 0)
    lane = lax.broadcasted_iota(jnp.int32, (ROWS, NZ), 1)
    y_at = py * NY + jnp.where(row < NY + H, row, row - ROWS)

    def loop(low, high, body, unroll=UNROLL):
        whole = (high - low) // unroll

        def step(k, carry):
            for j in range(unroll):
                body(low + k * unroll + j)
            return carry
        if whole > 1:
            lax.fori_loop(0, whole, step, 0)
        for i in range(low + whole * unroll if whole > 1 else low, high):
            body(i)

    def exists(dx, dy):
        return (px + dx >= 0) & (px + dx < PX) & (py + dy >= 0) & (py + dy < PY)

    def halo_copy(field, ys, yr, n, h, wx, k, send, recv, reverse):
        dx, dy = DIRS[k]
        if dy == 0:
            source = field.at[h + n - wx:h + n, 0:NY] if dx == 1 else field.at[h:h + wx, 0:NY]
            target = field.at[h - wx:h, 0:NY] if dx == 1 else field.at[h + n:h + n + wx, 0:NY]
        else:
            side = 1 if dy == 1 else 0
            if dx == 0:
                source, target = ys.at[side], yr.at[side, h:h + n]
            elif dx == 1:
                source, target = ys.at[side, n - h:n], yr.at[side, 0:h]
            else:
                source, target = ys.at[side, 0:h], yr.at[side, h + n:h + n + h]
        if reverse:
            dx, dy = -dx, -dy
        return pltpu.make_async_remote_copy(
            src_ref=source, dst_ref=target, send_sem=send.at[k], recv_sem=recv.at[k],
            device_id={"gx": px + dx, "gy": py + dy}, device_id_type=MESH)

    def halo_clear(field, yr, n, h):
        @pl.when(px == 0)
        def _():
            field[0:h, 0:NY] = jnp.zeros((h, NY, NZ), F32)
            yr[:, 0:h] = jnp.zeros((2, h, H, NZ), F32)

        @pl.when(px == PX - 1)
        def _():
            field[h + n:, 0:NY] = jnp.zeros((h, NY, NZ), F32)
            yr[:, h + n:] = jnp.zeros((2, h, H, NZ), F32)

        @pl.when(py == 0)
        def _():
            yr[1] = jnp.zeros((n + 2 * h, H, NZ), F32)

        @pl.when(py == PY - 1)
        def _():
            yr[0] = jnp.zeros((n + 2 * h, H, NZ), F32)

    def put(field, ys, i, j, value):
        field[i, 0:NY] = value
        ys[0, j] = value[0:H]
        ys[1, j] = value[NY - H:NY]

    def halo_send(field, ys, yr, n, h, wx, send, recv, count=8):
        for k in range(count):
            @pl.when(exists(*DIRS[k]))
            def _(k=k):
                halo_copy(field, ys, yr, n, h, wx, k, send, recv, False).start()

    def halo_wait(field, ys, yr, n, h, wx, send, recv, count=8):
        for k in range(count):
            @pl.when(exists(-DIRS[k][0], -DIRS[k][1]))
            def _(k=k):
                halo_copy(field, ys, yr, n, h, wx, k, send, recv, True).wait_recv()

        def place(i):
            field[i, NY:ROWS] = jnp.concatenate([yr[0, i], yr[1, i]], axis=0)
        loop(0, n + 2 * h, place, 4)

    def halo_done(field, ys, yr, n, h, wx, send, recv, count=8):
        for k in range(count):
            @pl.when(exists(*DIRS[k]))
            def _(k=k):
                halo_copy(field, ys, yr, n, h, wx, k, send, recv, False).wait_send()

    def fine(field, slot, wx):
        return (field, ystage.at[slot], yrecv.at[slot], NX, H, wx, h_send.at[slot], h_recv.at[slot])

    def coarse(slot):
        return (vl.at[slot], ystage1.at[slot], yrecv1.at[slot], NX // 2, H1, H1, h1_send.at[slot], h1_recv.at[slot])

    PEERS = [(dx, dy) for dy in (0, 1, -1, 2, -2) for dx in (1, 3, 2, 0) if (dx, dy) != (0, 0)]

    def gather_copy(g, dx, dy):
        return pltpu.make_async_remote_copy(
            src_ref=chunk.at[g], dst_ref=gat.at[g, REACH - dy, px],
            send_sem=g_send.at[g, REACH - dy, dx], recv_sem=g_recv.at[g, REACH - dy, px],
            device_id={"gx": lax.rem(px + dx, PX), "gy": py + dy}, device_id_type=MESH)

    def gather_arrival(g, dx, dy):
        from_x = lax.rem(px + dx, PX)
        return pltpu.make_async_remote_copy(
            src_ref=chunk.at[g], dst_ref=gat.at[g, REACH + dy, from_x],
            send_sem=g_send.at[g, REACH - dy, dx], recv_sem=g_recv.at[g, REACH + dy, from_x],
            device_id={"gx": from_x, "gy": py + dy}, device_id_type=MESH)

    def gather_send(g):
        for dx, dy in PEERS:
            @pl.when((py + dy >= 0) & (py + dy < PY))
            def _(dx=dx, dy=dy):
                gather_copy(g, dx, dy).start()
        gat[g, REACH, px] = chunk[g]

    def gather_wait(g, out):
        for dx, dy in PEERS:
            @pl.when((py + dy >= 0) & (py + dy < PY))
            def _(dx=dx, dy=dy):
                gather_arrival(g, dx, dy).wait_recv()
        for d in range(WIN):
            valid = (py - REACH + d >= 0) & (py - REACH + d < PY)
            whole = jnp.concatenate([gat[g, d, p] for p in range(PX)], axis=0)
            out[d] = jnp.where(valid, whole, 0.0)

    def gather_done(g):
        for dx, dy in PEERS:
            @pl.when((py + dy >= 0) & (py + dy < PY))
            def _(dx=dx, dy=dy):
                gather_copy(g, dx, dy).wait_send()

    OTHERS = [(dx, dy) for dy in range(PY) for dx in range(PX) if (dx, dy) != (0, 0)]

    def dot_copy(g, dx, dy, arrival):
        to_x, to_y = lax.rem(px + dx, PX), lax.rem(py + dy, PY)
        slot = to_x * PY + to_y if arrival else px * PY + py
        return pltpu.make_async_remote_copy(
            src_ref=dchunk.at[g], dst_ref=dots.at[g, slot],
            send_sem=d_send.at[g, dx * PY + dy], recv_sem=d_recv.at[g, slot],
            device_id={"gx": to_x, "gy": to_y}, device_id_type=MESH)

    def dot_prepare(g, values):
        folded = [jnp.sum(v[:, 0:NZ // 2] + v[:, NZ // 2:NZ], axis=0, keepdims=True) for v in values]
        part = jnp.concatenate(folded, axis=0)
        dchunk[g] = part
        dots[g, px * PY + py] = part

    def dot_send(g):
        for dx, dy in OTHERS:
            dot_copy(g, dx, dy, False).start()

    def dot_wait(g):
        for dx, dy in OTHERS:
            dot_copy(g, dx, dy, True).wait_recv()
        total = dots[g, 0]
        for slot in range(1, PX * PY):
            total = total + dots[g, slot]
        for dx, dy in OTHERS:
            dot_copy(g, dx, dy, False).wait_send()
        return [jnp.sum(total[i:i + 1], axis=1, keepdims=True) for i in range(total.shape[0])]

    def beside(field, i, value, s):
        return (field[i - 1], field[i + 1], pltpu.roll(value, s, 0), pltpu.roll(value, ROWS - s, 0),
                pltpu.roll(value, s, 1), pltpu.roll(value, NZ - s, 1))

    def coupled(coefs, field, i, value, s):
        near = beside(field, i, value, s)
        total = coefs[0, i] * near[0]
        for f in range(1, 6):
            total = total + coefs[f, i] * near[f]
        return total

    def prior_row(field, i):
        value = field[i]
        near = beside(field, i, value, 1)
        away = near[0] + near[1] + near[2] + near[3]
        away = away + jnp.where(lane >= 1, near[4], 0.0) + jnp.where(lane < NZ - 1, near[5], 0.0)
        return (6.5 * value - away)[0:NY]

    def swap(value, s, axis):
        index, size = (row, ROWS) if axis == 0 else (lane, NZ)
        return jnp.where((index & s) == 0, pltpu.roll(value, size - s, axis), pltpu.roll(value, s, axis))

    def block_sum(low, high, s):
        total = low + high
        total = total + swap(total, s, 1)
        return total + swap(total, s, 0)

    def pick_chunk(value):
        mine = ((row & 3) == 0) & ((row >> 2) == (lane & 3)) & (row < NY)
        return jnp.sum(jnp.where(mine, value, 0.0), axis=0, keepdims=True)

    def inside_yz(s):
        return (y_at >= s, y_at < GY - s, lane >= s, lane < NZ - s)

    def cell_inside(x):
        return jnp.where((x >= 0) & (x < PX * NX), ((y_at >= 0) & (y_at < GY)).astype(F32), 0.0) > 0.5

    own = lambda field: field.at[H:H + NX, 0:NY]
    loads = [pltpu.make_async_copy(source, target, in_sem.at[k]) for k, (source, target) in enumerate((
        (prior_ref, own(pr)), (logk_ref, own(lk)), (state_ref, own(st)), (cells_ref, cells_in), (prec_ref, prec_in),
        (grad_ref, grad)))]
    for load in loads:
        load.start()
    barrier = pltpu.get_barrier_semaphore()
    fields = [(lk, 0), (st, 1), (pr, 2), (src, 3), (z2.at[0], 4), (c0, 5), (z2.at[1], 6)]
    for field, slot in fields:
        halo_clear(field, yrecv.at[slot], NX, H)
    for slot in range(4):
        halo_clear(vl.at[slot], yrecv1.at[slot], NX // 2, H1)
    for k in range(8):
        @pl.when(exists(*DIRS[k]))
        def _(k=k):
            pl.semaphore_signal(barrier, inc=1, device_id={"gx": px + DIRS[k][0], "gy": py + DIRS[k][1]},
                                device_id_type=MESH)

    def edges(field, slot):
        for i in range(NX):
            ystage[slot, 0, i] = field[H + i, 0:H]
            ystage[slot, 1, i] = field[H + i, NY - H:NY]
    loads[0].wait()
    edges(pr, 2)
    loads[1].wait()
    edges(lk, 0)
    loads[2].wait()
    edges(st, 1)
    across = jnp.where(px > 0, 1, 0) + jnp.where(px < PX - 1, 1, 0)
    along = jnp.where(py > 0, 1, 0) + jnp.where(py < PY - 1, 1, 0)
    pl.semaphore_wait(barrier, (across + 1) * (along + 1) - 1)

    send_prior, send_lk, send_st = fine(pr, 2, 1), fine(lk, 0, H), fine(st, 1, H)
    halo_send(*send_prior, count=4)
    halo_send(*send_lk)
    halo_send(*send_st)

    loads[3].wait()
    loads[4].wait()
    cells = cells_in[...]
    at_xy = ((cells >> 15) - px * NX) * NY + ((cells >> 8) & (GY - 1)) - py * NY
    at_z = cells & (NZ - 1)
    hot_xy = lax.broadcasted_iota(jnp.int32, (NX * NY, SENSORS), 0) == at_xy
    hot_z = (lax.broadcasted_iota(jnp.int32, (NZ, SENSORS), 0) == at_z).astype(F32).astype(jnp.bfloat16)
    left = jnp.where(hot_xy, prec_in[...], 0.0)
    total = jnp.zeros((NX * NY, NZ), F32)
    for part in range(3):
        piece = left.astype(jnp.bfloat16)
        left = left - piece.astype(F32)
        total = total + lax.dot_general(piece, hot_z, (((1,), (1,)), ((), ())), preferred_element_type=F32)
    for i in range(NX):
        weight[i] = total[i * NY:(i + 1) * NY]

    loads[5].wait()
    halo_wait(*send_prior, count=4)

    def start_source(i):
        put(src, ystage.at[3], i + H, i, prior_row(pr, i + H) - grad[i])
    loop(0, NX, start_source)
    send_src = fine(src, 3, H)
    halo_send(*send_src)

    halo_wait(*send_lk)

    def start_cond(i):
        kk[i] = jnp.exp(lk[i])
    loop(0, RX, start_cond)

    inner = inside_yz(1)

    def start_couplings(i):
        value = kk[i]
        x = px * NX + i - H
        near = beside(kk, i, value, 1)
        in_x = (x > 0, x < GX - 1)
        diag = None
        for f in range(6):
            ok = in_x[f] if f < 2 else inner[f - 2]
            a = 0.5 * (value + jnp.where(ok, near[f], value))
            ca[f, i] = jnp.where(ok, a, 0.0)
            diag = a if diag is None else diag + a
        wd[i] = jnp.where(cell_inside(x), OMEGA / diag, 0.0)
    loop(1, RX - 1, start_couplings, 1)

    def start_level1(i):
        c1[i] = block_sum(kk[2 * i], kk[2 * i + 1], 1) * 0.125
    loop(0, RX1, start_level1)

    for i in range(2):
        chunk[0, i:i + 1] = pick_chunk(block_sum(c1[H1 + 2 * i], c1[H1 + 2 * i + 1], 2) * 0.125)

    inner1 = inside_yz(2)

    def start_couplings1(i):
        value = c1[i]
        x = px * NX + 2 * i - H
        near = beside(c1, i, value, 2)
        in_x = (x > 0, x < GX - 2)
        diag = None
        for f in range(6):
            ok = in_x[f] if f < 2 else inner1[f - 2]
            a = value + jnp.where(ok, near[f], value)
            ca1[f, i] = jnp.where(ok, a, 0.0)
            diag = a if diag is None else diag + a
        wd1[i] = jnp.where(cell_inside(x), OMEGA / diag, 0.0)
    loop(1, RX1 - 1, start_couplings1, 1)

    halo_wait(*send_st)

    def start_state(i):
        value = st[i]
        x = px * NX + i - H
        near = beside(st, i, value, 1)
        in_x = (x > 0, x < GX - 1)
        diag = None
        for f in range(6):
            ok = in_x[f] if f < 2 else inner[f - 2]
            d = jnp.where(ok, 0.5 * (value - near[f]), value)
            cd[f, i] = jnp.where(ok, d, 0.0)
            diag = d if diag is None else diag + d
        sd[i] = diag
    loop(1, RX - 1, start_state, 1)

    row8 = lax.broadcasted_iota(jnp.int32, (8, NZ), 0)
    lane8 = lax.broadcasted_iota(jnp.int32, (8, NZ), 1)
    y_in = lane8 & 3

    def coarse_beside(values, d):
        v = values[d]
        zero = jnp.zeros_like(v)
        low = values[d - 1] if d > 0 else zero
        high = values[d + 1] if d < WIN - 1 else zero
        return (pltpu.roll(v, 1, 0), pltpu.roll(v, 7, 0),
                jnp.where(y_in > 0, pltpu.roll(v, 1, 1), pltpu.roll(low, NZ - 3, 1)),
                jnp.where(y_in < 3, pltpu.roll(v, NZ - 1, 1), pltpu.roll(high, 3, 1)),
                pltpu.roll(v, 4, 1), pltpu.roll(v, NZ - 4, 1))

    def coarse_couplings():
        values = [cond2[d] for d in range(WIN)]
        for d in range(WIN):
            place = py - REACH + d
            y = place * 4 + y_in
            inside = (row8 > 0, row8 < 7, y > 0, y < GY // 4 - 1, lane8 >= 4, lane8 < NZ - 4)
            diag = None
            for f, near in enumerate(coarse_beside(values, d)):
                a = 2.0 * (values[d] + jnp.where(inside[f], near, values[d]))
                ca2[f, d] = jnp.where(inside[f], a, 0.0)
                diag = a if diag is None else diag + a
            wd2[d] = jnp.where((place >= 0) & (place < PY), OMEGA / diag, 0.0)

    def coarse_solve():
        def sweep(s, values):
            out = []
            for d in range(WIN):
                total = rhs2[d]
                for f, near in enumerate(coarse_beside(values, d)):
                    total = total + ca2[f, d] * near
                out.append((1.0 - OMEGA) * values[d] + wd2[d] * total)
            return tuple(out)
        values = lax.fori_loop(1, COARSE_SWEEPS, sweep, tuple(wd2[d] * rhs2[d] for d in range(WIN)))
        for d in range(WIN):
            sol[d] = values[d]
        cell = jnp.where(row < NY, row >> 2, jnp.where(row < NY + H, 0, 3))
        for i in range(4):
            x = 2 * px - 1 + i
            at = jnp.clip(x, 0, 7)
            own, high, low = (sol[d, pl.ds(at, 1), :] for d in (REACH, REACH + 1, REACH - 1))
            spread = jnp.where(row < NY, own, jnp.where(row < NY + H, high, low))
            spread = jnp.where((lane & 3) == cell, spread, 0.0)
            spread = spread + swap(spread, 1, 1)
            spread = spread + swap(spread, 2, 1)
            p2[i] = jnp.where((x >= 0) & (x < 8), spread, 0.0)

    def solve(source, n, reach, finish, first, during=lambda: None, after=lambda: None):
        def presmooth(i):
            vv[i] = wd[i] * source[i]
        loop(1, RX - 1, presmooth)

        def restrict(i):
            parts = []
            for j in range(2):
                at = 2 * i + j
                parts.append((1.0 - OMEGA) * source[at] + coupled(ca, vv, at, vv[at], 1))
            total = block_sum(parts[0], parts[1], 1)
            b1[i] = total
            v1[i] = wd1[i] * total
        loop(1, RX1 - 1, restrict, 1)

        def level1_residual(i):
            return (1.0 - OMEGA) * b1[i] + coupled(ca1, v1, i, v1[i], 2)
        for i in range(2):
            chunk[n + 1, i:i + 1] = pick_chunk(
                block_sum(level1_residual(H1 + 2 * i), level1_residual(H1 + 2 * i + 1), 2))
        gather_send(n + 1)
        for i in range(NX // 2):
            put(vl.at[n], ystage1.at[n], H1 + i, i, v1[H1 + i, 0:NY])
        send_vl = coarse(n)
        halo_send(*send_vl)
        if first:
            gather_wait(0, cond2)
            coarse_couplings()
        during()
        gather_wait(n + 1, rhs2)
        after()
        coarse_solve()
        halo_wait(*send_vl)
        gather_done(n + 1)
        halo_done(*send_vl)

        for i in range(RX1):
            v1[i] = vl[n, i] + p2[i // 2]

        def postsmooth1(i):
            v = v1[i]
            r1[i] = (1.0 - OMEGA) * v + wd1[i] * (b1[i] + coupled(ca1, v1, i, v, 2))
        loop(1, RX1 - 1, postsmooth1)

        def correct(i):
            for j in range(2):
                vv[2 * i + j] = vv[2 * i + j] + r1[i]
        loop(1, RX1 - 1, correct)

        def postsmooth(i):
            v = vv[i]
            finish(i, (1.0 - OMEGA) * v + wd[i] * (source[i] + coupled(ca, vv, i, v, 1)))
        loop(H - reach, H + NX + reach, postsmooth)

    def hessian(r, n, keep, during, after):
        def scaled(i):
            gg[i] = kk[i] * r[i]
        loop(0, RX, scaled)

        def sensitivity(i):
            value = gg[i]
            zz[i] = sd[i] * value + coupled(cd, gg, i, value, 1)
        loop(1, RX - 1, sensitivity)

        second = z2.at[n]

        def weighted(i, value):
            wkeep[n, i - H] = value[0:NY]
            put(second, ystage.at[4 + 2 * n], i, i - H, weight[i - H] * value[0:NY])
        solve(zz, 2 * n, 0, weighted, n == 0)
        send_z2 = fine(second, 4 + 2 * n, H - 1)
        halo_send(*send_z2)
        halo_wait(*send_z2)
        halo_done(*send_z2)

        def adjoint(i, value):
            pp[i] = value
        solve(second, 2 * n + 1, 1, adjoint, False, during, after)

        def assemble(i):
            p = pp[i]
            misfit = kk[i] * (sd[i] * p - coupled(cd, pp, i, p, 1))
            keep(i, misfit[0:NY] + prior_row(r, i))
        loop(H, H + NX, assemble)

    halo_wait(*send_src)
    gather_send(0)

    zero = jnp.zeros((NY, NZ), F32)
    sums = {}

    def first_products():
        total = [zero, zero]
        for i in range(NX):
            r, w = src[i + H, 0:NY], wkeep[0, i]
            total[0] = total[0] + r * r
            total[1] = total[1] + weight[i] * w * w + r * prior_row(src, i + H)
        dot_prepare(0, (total[0], total[1], zero))

    def keep_first(i, value):
        put(c0, ystage.at[5], i, i - H, value)
    hessian(src, 0, keep_first, first_products, lambda: dot_send(0))
    send_c0 = fine(c0, 5, H)
    halo_send(*send_c0)
    halo_wait(*send_c0)

    def second_products():
        rr, rc = dot_wait(0)[:2]
        alpha = rr / rc
        sums.update(rr=rr, rc=rc, alpha=alpha)
        for i in range(H - 1, H + NX + 1):
            r1f[i] = src[i] - alpha * c0[i]
        total = [zero, zero, zero]
        for i in range(NX):
            r, w = r1f[i + H, 0:NY], wkeep[0, i] - alpha * wkeep[1, i]
            total[0] = total[0] + r * r
            total[1] = total[1] + weight[i] * w * w + r * prior_row(r1f, i + H)
            total[2] = total[2] + r * c0[i + H, 0:NY]
        dot_prepare(1, total)
        dot_send(1)

    def keep_second(i, value):
        kc[i - H] = value
    hessian(c0, 1, keep_second, second_products, lambda: None)

    norm, product, cross = dot_wait(1)
    alpha = sums["alpha"]
    ratio = norm / sums["rr"]
    beta = norm / (product + 2.0 * ratio * cross + ratio * ratio * sums["rc"])

    def finish(i):
        r, c, later = src[i + H, 0:NY], c0[i + H, 0:NY], r1f[i + H, 0:NY]
        curved = c - alpha * kc[i]
        step_ref[i] = alpha * r + beta * (later + ratio * r)
        resid_ref[i] = later - beta * (curved + ratio * c)
    loop(0, NX, finish)

    halo_done(*send_prior, count=4)
    for done in (send_lk, send_st, send_src, send_c0):
        halo_done(*done)
    gather_done(0)


def scratch():
    vmem = lambda *shape: pltpu.VMEM(shape, F32)
    fine = lambda *lead: vmem(*lead, RX, ROWS, NZ)
    level1 = lambda *lead: vmem(*lead, RX1, ROWS, NZ)
    dma = pltpu.SemaphoreType.DMA
    return [
        fine(), fine(), fine(), fine(), fine(), fine(2), level1(4),
        vmem(7, 2, NX, H, NZ), vmem(7, 2, RX, H, NZ), vmem(4, 2, NX // 2, H, NZ), vmem(4, 2, RX1, H, NZ),
        vmem(NX, NY, NZ), pltpu.VMEM((1, SENSORS), jnp.int32), vmem(1, SENSORS), fine(), vmem(2, NX, NY, NZ),
        fine(), fine(6), fine(), fine(6), fine(), fine(), fine(), fine(), vmem(1, 8, 128), fine(),
        level1(), level1(6), level1(), level1(), level1(), level1(), vmem(4, ROWS, NZ),
        vmem(5, WIN, PX, 2, NZ), vmem(5, 2, NZ), vmem(WIN, 8, NZ), vmem(6, WIN, 8, NZ), vmem(WIN, 8, NZ),
        vmem(WIN, 8, NZ), vmem(WIN, 8, NZ), vmem(NX, NY, NZ), vmem(NX, NY, NZ),
        vmem(2, PX * PY, 3, 128), vmem(2, 3, 128),
        dma((7, 8)), dma((7, 8)), dma((4, 8)), dma((4, 8)), dma((5, WIN, PX)), dma((5, WIN, PX)),
        dma((2, PX * PY)), dma((2, PX * PY)), dma((6,)),
    ]


def on_device(log_conductivity, state, gradient, prior_sample, sensor_cells, noise_precision):
    block = jax.ShapeDtypeStruct(log_conductivity.shape, F32)
    vmem = pl.BlockSpec(memory_space=pltpu.VMEM)
    return pl.pallas_call(
        kernel,
        out_shape=(block, block),
        in_specs=[pl.BlockSpec(memory_space=pltpu.HBM)] * 6,
        out_specs=(vmem, vmem),
        scratch_shapes=scratch(),
        compiler_params=pltpu.CompilerParams(
            collective_id=0, has_side_effects=True, vmem_limit_bytes=24 * 1024 * 1024),
    )(*(pltpu.with_memory_space_constraint(x, pltpu.HBM) for x in (
        log_conductivity, state, gradient, prior_sample,
        sensor_cells.reshape(1, SENSORS), noise_precision.reshape(1, SENSORS))))


def solution(mesh):
    field, sensors = P(("ens", "gx"), "gy", None), P(("ens", "gx", "gy"))
    return jax.shard_map(
        on_device,
        mesh=mesh,
        in_specs=(field, field, field, field, sensors, sensors),
        out_specs=(field, field),
        check_vma=False,
    )
```

```python
import jax
import jax.numpy as jnp
from jax import lax
from jax.experimental import pallas as pl
from jax.experimental.pallas import tpu as pltpu
from jax.sharding import PartitionSpec as P

MESH = pl.DeviceIdType.MESH
F32 = jnp.float32

NX, NY, NZ = 8, 16, 256
H, H1 = 4, 2
RX, RX1 = NX + 2 * H, NX // 2 + 2 * H1
ROWS = NY + 2 * H
PX, PY = 4, 8
GX, GY = NX * PX, NY * PY
REACH = 2
WIN = 2 * REACH + 1
COARSE_SWEEPS = 6
PIECES = 3
SENSORS = 512
OMEGA = 0.8
DIRS = ((1, 0), (-1, 0), (0, 1), (0, -1), (1, 1), (1, -1), (-1, 1), (-1, -1))
UNROLL = 2


def kernel(logk_ref, state_ref, grad_ref, prior_ref, cells_ref, prec_ref,
           step_ref, resid_ref,
           lk, st, pr, src, c0, z2, vl, ystage, yrecv, ystage1, yrecv1, grad, cells_in, prec_in, r1f, wkeep,
           kk, ca, wd, cd, sd, gg, zz, vv, cp, pp,
           c1, ca1, wd1, b1, v1, r1, p2,
           gp, zp1, vp1, zp2, vp2, bp, v1p, gat0, gat, chunk0, chunk, cond2, ca2, wd2, rhs2, sol, weight, kc, dots, dchunk,
           h_send, h_recv, g_send, g_recv, d_send, d_recv, in_sem):
    px = lax.axis_index("gx")
    py = lax.axis_index("gy")
    row = lax.broadcasted_iota(jnp.int32, (ROWS, NZ), 0)
    lane = lax.broadcasted_iota(jnp.int32, (ROWS, NZ), 1)
    row8 = lax.broadcasted_iota(jnp.int32, (8, NZ), 0)
    lane8 = lax.broadcasted_iota(jnp.int32, (8, NZ), 1)
    y_in = lane8 & 3
    y_at = py * NY + jnp.where(row < NY + H, row, row - ROWS)

    def loop(low, high, body, unroll=UNROLL):
        whole = (high - low) // unroll

        def step(k, carry):
            for j in range(unroll):
                body(low + k * unroll + j)
            return carry
        if whole > 1:
            lax.fori_loop(0, whole, step, 0)
        for i in range(low + whole * unroll if whole > 1 else low, high):
            body(i)

    def exists(dx, dy):
        return (px + dx >= 0) & (px + dx < PX) & (py + dy >= 0) & (py + dy < PY)

    def halo_copy(field, ys, yr, n, h, wx, k, send, recv, reverse):
        dx, dy = DIRS[k]
        if dy == 0:
            source = field.at[h + n - wx:h + n, 0:NY] if dx == 1 else field.at[h:h + wx, 0:NY]
            target = field.at[h - wx:h, 0:NY] if dx == 1 else field.at[h + n:h + n + wx, 0:NY]
        else:
            side = 1 if dy == 1 else 0
            if dx == 0:
                source, target = ys.at[side], yr.at[side, h:h + n]
            elif dx == 1:
                source, target = ys.at[side, n - h:n], yr.at[side, 0:h]
            else:
                source, target = ys.at[side, 0:h], yr.at[side, h + n:h + n + h]
        if reverse:
            dx, dy = -dx, -dy
        return pltpu.make_async_remote_copy(
            src_ref=source, dst_ref=target, send_sem=send.at[k], recv_sem=recv.at[k],
            device_id={"gx": px + dx, "gy": py + dy}, device_id_type=MESH)

    def halo_clear(field, yr, n, h):
        @pl.when(px == 0)
        def _():
            field[0:h, 0:NY] = jnp.zeros((h, NY, NZ), F32)
            yr[:, 0:h] = jnp.zeros((2, h, H, NZ), F32)

        @pl.when(px == PX - 1)
        def _():
            field[h + n:, 0:NY] = jnp.zeros((h, NY, NZ), F32)
            yr[:, h + n:] = jnp.zeros((2, h, H, NZ), F32)

        @pl.when(py == 0)
        def _():
            yr[1] = jnp.zeros((n + 2 * h, H, NZ), F32)

        @pl.when(py == PY - 1)
        def _():
            yr[0] = jnp.zeros((n + 2 * h, H, NZ), F32)

    def put(field, ys, i, j, value):
        field[i, 0:NY] = value
        ys[0, j] = value[0:H]
        ys[1, j] = value[NY - H:NY]

    def halo_send(field, ys, yr, n, h, wx, send, recv, count=8):
        for k in range(count):
            @pl.when(exists(*DIRS[k]))
            def _(k=k):
                halo_copy(field, ys, yr, n, h, wx, k, send, recv, False).start()

    def halo_wait(field, ys, yr, n, h, wx, send, recv, count=8):
        for k in range(count):
            @pl.when(exists(-DIRS[k][0], -DIRS[k][1]))
            def _(k=k):
                halo_copy(field, ys, yr, n, h, wx, k, send, recv, True).wait_recv()

        def place(i):
            field[i, NY:ROWS] = jnp.concatenate([yr[0, i], yr[1, i]], axis=0)
        loop(0, n + 2 * h, place, 4)

    def halo_done(field, ys, yr, n, h, wx, send, recv, count=8):
        for k in range(count):
            @pl.when(exists(*DIRS[k]))
            def _(k=k):
                halo_copy(field, ys, yr, n, h, wx, k, send, recv, False).wait_send()

    def fine(field, slot, wx, sems):
        return (field, ystage.at[slot], yrecv.at[slot], NX, H, wx, h_send.at[sems], h_recv.at[sems])

    def coarse(slot):
        return (vl.at[slot], ystage1.at[slot], yrecv1.at[slot], NX // 2, H1, H1, h_send.at[0], h_recv.at[0])

    PEERS = [(dx, dy) for dy in (0, 1, -1, 2, -2) for dx in (1, 3, 2, 0) if (dx, dy) != (0, 0)]

    REACHED = (0, 1, -1, 2, -2)

    def buffers(g):
        return (chunk0, gat0) if g == 0 else (chunk.at[g - 1], gat.at[g - 1])

    def sems(g):
        return (g_send.at[0], g_recv.at[0]) if g == 0 else (g_send.at[1], g_recv.at[1 + (g - 1) % 2])

    def gather_send(g):
        mine, all_ = buffers(g)
        sent, arrived = sems(g)
        for dx, dy in PEERS:
            @pl.when((py + dy >= 0) & (py + dy < PY))
            def _(dx=dx, dy=dy):
                pltpu.make_async_remote_copy(
                    src_ref=mine, dst_ref=all_.at[REACH - dy, px],
                    send_sem=sent.at[REACH + dy], recv_sem=arrived.at[REACH - dy],
                    device_id={"gx": lax.rem(px + dx, PX), "gy": py + dy}, device_id_type=MESH).start()
        all_[REACH, px] = mine[...]

    def gather_end(g, which):
        all_ = buffers(g)[1]
        for dy in REACHED:
            @pl.when((py + dy >= 0) & (py + dy < PY))
            def _(dy=dy):
                row_ = all_.at[REACH + dy, 0:PX - 1] if dy == 0 else all_.at[REACH + dy]
                pltpu.make_async_copy(row_, row_, sems(g)[which].at[REACH + dy]).wait()

    def valid(d):
        return (py - REACH + d >= 0) & (py - REACH + d < PY)

    def gather_cond():
        gather_end(0, 1)
        for d in range(WIN):
            whole = jnp.concatenate([gat0[d, p] for p in range(PX)], axis=0)
            cond2[d] = jnp.where(valid(d), whole, 0.0)

    def along_x(piece):
        moved = jnp.where((row8 & 1) == 0, pltpu.roll(piece, 2, 0), pltpu.roll(piece, 6, 0))
        return jnp.where((row8 > 0) & (row8 < 7), moved, 0.0)

    def gather_rhs(g):
        gather_end(g, 1)
        own, ring = [], []
        for d in range(WIN):
            piece = [jnp.concatenate([gat[g - 1, d, p, q] for p in range(PX)], axis=0) for q in range(PIECES)]
            corner = along_x(piece[2])
            corner = jnp.where(y_in == 0, pltpu.roll(corner, NZ - 1, 1), pltpu.roll(corner, 1, 1))
            own.append(jnp.where(valid(d), piece[0] + along_x(piece[1]), 0.0))
            ring.append(jnp.where(valid(d), piece[2] + corner, 0.0))
        zero8 = jnp.zeros((8, NZ), F32)
        for d in range(WIN):
            low = ring[d - 1] if d > 0 else zero8
            high = ring[d + 1] if d < WIN - 1 else zero8
            rhs2[d] = own[d] + jnp.where(y_in == 0, low, jnp.where(y_in == 3, high, 0.0))

    OTHERS = [(dx, dy) for dy in range(PY) for dx in range(PX) if (dx, dy) != (0, 0)]

    def dot_prepare(g, values):
        folded = [jnp.sum(v[:, 0:NZ // 2] + v[:, NZ // 2:NZ], axis=0, keepdims=True) for v in values]
        part = jnp.concatenate(folded, axis=0)
        dchunk[g] = part
        dots[g, px * PY + py] = part

    def dot_send(g):
        for dx, dy in OTHERS:
            pltpu.make_async_remote_copy(
                src_ref=dchunk.at[g], dst_ref=dots.at[g, px * PY + py], send_sem=d_send.at[0], recv_sem=d_recv.at[g],
                device_id={"gx": lax.rem(px + dx, PX), "gy": lax.rem(py + dy, PY)}, device_id_type=MESH).start()

    def dot_wait(g):
        others = dots.at[g, 0:PX * PY - 1]
        pltpu.make_async_copy(others, others, d_recv.at[g]).wait()
        total = dots[g, 0]
        for slot in range(1, PX * PY):
            total = total + dots[g, slot]
        pltpu.make_async_copy(others, others, d_send.at[0]).wait()
        return [jnp.sum(total[i:i + 1], axis=1, keepdims=True) for i in range(total.shape[0])]

    def beside(field, i, value, s):
        return (field[i - 1], field[i + 1], pltpu.roll(value, s, 0), pltpu.roll(value, ROWS - s, 0),
                pltpu.roll(value, s, 1), pltpu.roll(value, NZ - s, 1))

    def coupled(coefs, field, i, value, s):
        near = beside(field, i, value, s)
        total = coefs[0, i] * near[0]
        for f in range(1, 6):
            total = total + coefs[f, i] * near[f]
        return total

    def prior_row(field, i):
        value = field[i]
        near = beside(field, i, value, 1)
        away = near[0] + near[1] + near[2] + near[3]
        away = away + jnp.where(lane >= 1, near[4], 0.0) + jnp.where(lane < NZ - 1, near[5], 0.0)
        return (6.5 * value - away)[0:NY]

    def swap(value, s, axis):
        index, size = (row, ROWS) if axis == 0 else (lane, NZ)
        return jnp.where((index & s) == 0, pltpu.roll(value, size - s, axis), pltpu.roll(value, s, axis))

    def block_sum(low, high, s):
        total = low + high
        total = total + swap(total, s, 1)
        return total + swap(total, s, 0)

    def pick_chunk(value):
        mine = ((row & 3) == 0) & ((row >> 2) == (lane & 3)) & (row < NY)
        return jnp.sum(jnp.where(mine, value, 0.0), axis=0, keepdims=True)

    def pick_ring(value, at):
        mine = ((row == NY) & ((lane & 3) == at)) | ((row == NY + H) & ((lane & 3) == 3 - at))
        return jnp.sum(jnp.where(mine, value, 0.0), axis=0, keepdims=True)

    def inside_yz(s):
        return (y_at >= s, y_at < GY - s, lane >= s, lane < NZ - s)

    def cell_inside(x):
        return jnp.where((x >= 0) & (x < PX * NX), ((y_at >= 0) & (y_at < GY)).astype(F32), 0.0) > 0.5

    own = lambda field: field.at[H:H + NX, 0:NY]
    loads = [pltpu.make_async_copy(source, target, in_sem.at[k]) for k, (source, target) in enumerate((
        (prior_ref, own(pr)), (logk_ref, own(lk)), (state_ref, own(st)), (cells_ref, cells_in), (prec_ref, prec_in),
        (grad_ref, grad)))]
    for load in loads:
        load.start()
    barrier = pltpu.get_barrier_semaphore()
    fields = [(lk, 0), (st, 1), (pr, 2), (src, 3), (z2.at[0], 4), (c0, 5), (z2.at[1], 6)]
    for field, slot in fields:
        halo_clear(field, yrecv.at[slot], NX, H)
    for slot in range(4):
        halo_clear(vl.at[slot], yrecv1.at[slot], NX // 2, H1)
    for field in (gp, zp1, vp1, zp2, vp2):
        def clear(i, field=field):
            field[i] = jnp.zeros((ROWS, NZ), F32)
        loop(1, RX - 1, clear)
    for i in (0, RX1 - 1):
        v1p[i] = jnp.zeros((ROWS, NZ), F32)
    for k in range(8):
        @pl.when(exists(*DIRS[k]))
        def _(k=k):
            pl.semaphore_signal(barrier, inc=1, device_id={"gx": px + DIRS[k][0], "gy": py + DIRS[k][1]},
                                device_id_type=MESH)

    def edges(field, slot):
        for i in range(NX):
            ystage[slot, 0, i] = field[H + i, 0:H]
            ystage[slot, 1, i] = field[H + i, NY - H:NY]
    loads[0].wait()
    edges(pr, 2)
    loads[1].wait()
    edges(lk, 0)
    loads[2].wait()
    edges(st, 1)
    across = jnp.where(px > 0, 1, 0) + jnp.where(px < PX - 1, 1, 0)
    along = jnp.where(py > 0, 1, 0) + jnp.where(py < PY - 1, 1, 0)
    pl.semaphore_wait(barrier, (across + 1) * (along + 1) - 1)

    send_prior, send_lk, send_st = fine(pr, 2, 1, 0), fine(lk, 0, H, 1), fine(st, 1, H, 2)
    halo_send(*send_prior, count=4)
    halo_send(*send_lk)
    halo_send(*send_st)

    loads[3].wait()
    loads[4].wait()
    cells = cells_in[...]
    at_xy = ((cells >> 15) - px * NX) * NY + ((cells >> 8) & (GY - 1)) - py * NY
    at_z = cells & (NZ - 1)
    hot_xy = lax.broadcasted_iota(jnp.int32, (NX * NY, SENSORS), 0) == at_xy
    hot_z = (lax.broadcasted_iota(jnp.int32, (NZ, SENSORS), 0) == at_z).astype(F32).astype(jnp.bfloat16)
    left = jnp.where(hot_xy, prec_in[...], 0.0)
    total = jnp.zeros((NX * NY, NZ), F32)
    for part in range(3):
        piece = left.astype(jnp.bfloat16)
        left = left - piece.astype(F32)
        total = total + lax.dot_general(piece, hot_z, (((1,), (1,)), ((), ())), preferred_element_type=F32)
    for i in range(NX):
        weight[i] = total[i * NY:(i + 1) * NY]

    loads[5].wait()
    halo_wait(*send_prior, count=4)

    def start_source(i):
        put(src, ystage.at[3], i + H, i, prior_row(pr, i + H) - grad[i])
    loop(0, NX, start_source, 8)
    send_src = fine(src, 3, H, 3)
    halo_send(*send_src)

    halo_wait(*send_lk)

    def start_cond(i):
        kk[i] = jnp.exp(lk[i])
    loop(0, RX, start_cond, 8)

    inner = inside_yz(1)

    def start_couplings(i):
        value = kk[i]
        x = px * NX + i - H
        near = beside(kk, i, value, 1)
        in_x = (x > 0, x < GX - 1)
        diag = None
        for f in range(6):
            ok = in_x[f] if f < 2 else inner[f - 2]
            a = 0.5 * (value + jnp.where(ok, near[f], value))
            ca[f, i] = jnp.where(ok, a, 0.0)
            diag = a if diag is None else diag + a
        wd[i] = jnp.where(cell_inside(x), OMEGA / diag, 0.0)
    loop(1, RX - 1, start_couplings, 14)

    def start_level1(i):
        c1[i] = block_sum(kk[2 * i], kk[2 * i + 1], 1) * 0.125
    loop(0, RX1, start_level1, 8)

    for i in range(2):
        chunk0[i:i + 1] = pick_chunk(block_sum(c1[H1 + 2 * i], c1[H1 + 2 * i + 1], 2) * 0.125)

    inner1 = inside_yz(2)

    def start_couplings1(i):
        value = c1[i]
        x = px * NX + 2 * i - H
        near = beside(c1, i, value, 2)
        in_x = (x > 0, x < GX - 2)
        diag = None
        for f in range(6):
            ok = in_x[f] if f < 2 else inner1[f - 2]
            a = value + jnp.where(ok, near[f], value)
            ca1[f, i] = jnp.where(ok, a, 0.0)
            diag = a if diag is None else diag + a
        wd1[i] = jnp.where(cell_inside(x), OMEGA / diag, 0.0)
    loop(1, RX1 - 1, start_couplings1, 6)

    halo_wait(*send_st)

    def start_state(i):
        value = st[i]
        x = px * NX + i - H
        near = beside(st, i, value, 1)
        in_x = (x > 0, x < GX - 1)
        diag = None
        for f in range(6):
            ok = in_x[f] if f < 2 else inner[f - 2]
            d = jnp.where(ok, 0.5 * (value - near[f]), value)
            cd[f, i] = jnp.where(ok, d, 0.0)
            diag = d if diag is None else diag + d
        sd[i] = diag
    loop(1, RX - 1, start_state, 14)


    def coarse_beside(values, d):
        v = values[d]
        zero = jnp.zeros_like(v)
        low = values[d - 1] if d > 0 else zero
        high = values[d + 1] if d < WIN - 1 else zero
        return (pltpu.roll(v, 1, 0), pltpu.roll(v, 7, 0),
                jnp.where(y_in > 0, pltpu.roll(v, 1, 1), pltpu.roll(low, NZ - 3, 1)),
                jnp.where(y_in < 3, pltpu.roll(v, NZ - 1, 1), pltpu.roll(high, 3, 1)),
                pltpu.roll(v, 4, 1), pltpu.roll(v, NZ - 4, 1))

    def coarse_couplings():
        values = [cond2[d] for d in range(WIN)]
        for d in range(WIN):
            place = py - REACH + d
            y = place * 4 + y_in
            inside = (row8 > 0, row8 < 7, y > 0, y < GY // 4 - 1, lane8 >= 4, lane8 < NZ - 4)
            diag = None
            for f, near in enumerate(coarse_beside(values, d)):
                a = 2.0 * (values[d] + jnp.where(inside[f], near, values[d]))
                ca2[f, d] = jnp.where(inside[f], a, 0.0)
                diag = a if diag is None else diag + a
            wd2[d] = jnp.where((place >= 0) & (place < PY), OMEGA / diag, 0.0)

    def coarse_solve():
        def sweep(s, values):
            out = []
            for d in range(WIN):
                total = rhs2[d]
                for f, near in enumerate(coarse_beside(values, d)):
                    total = total + ca2[f, d] * near
                out.append((1.0 - OMEGA) * values[d] + wd2[d] * total)
            return tuple(out)
        values = lax.fori_loop(1, COARSE_SWEEPS, sweep, tuple(wd2[d] * rhs2[d] for d in range(WIN)))
        for d in range(WIN):
            sol[d] = values[d]
        cell = jnp.where(row < NY, row >> 2, jnp.where(row < NY + H, 0, 3))
        for i in range(4):
            x = 2 * px - 1 + i
            at = jnp.clip(x, 0, 7)
            own, high, low = (sol[d, pl.ds(at, 1), :] for d in (REACH, REACH + 1, REACH - 1))
            spread = jnp.where(row < NY, own, jnp.where(row < NY + H, high, low))
            spread = jnp.where((lane & 3) == cell, spread, 0.0)
            spread = spread + swap(spread, 1, 1)
            spread = spread + swap(spread, 2, 1)
            p2[i] = jnp.where((x >= 0) & (x < 8), spread, 0.0)

    def contribute(g, z, v):
        def restrict(i):
            parts = [(1.0 - OMEGA) * z[at] + coupled(ca, v, at, v[at], 1) for at in (2 * i, 2 * i + 1)]
            total = block_sum(parts[0], parts[1], 1)
            bp[i] = total
            v1p[i] = wd1[i] * total
        loop(1, RX1 - 1, restrict, RX1 - 2)

        def level1_residual(i):
            if i == 0:
                return ca1[0, 1] * v1p[1]
            if i == RX1 - 1:
                return ca1[1, RX1 - 2] * v1p[RX1 - 2]
            return (1.0 - OMEGA) * bp[i] + coupled(ca1, v1p, i, v1p[i], 2)
        for j, (q, at) in enumerate(((1, 1), (0, 0), (0, 1), (1, 0))):
            total = block_sum(level1_residual(2 * j), level1_residual(2 * j + 1), 2)
            chunk[g - 1, q, at:at + 1] = pick_chunk(total)
            ringed = pick_ring(total, q)
            if q == 0:
                chunk[g - 1, 2, at:at + 1] = ringed
            else:
                outer = ringed if j == 0 else jnp.concatenate([ringed, outer], axis=0)
        chunk[g - 1, 2] = chunk[g - 1, 2] + outer

    def solve(source, n, reach, finish, first, during=lambda: None, after=lambda: None):
        def presmooth(i):
            vv[i] = wd[i] * source[i]
        loop(1, RX - 1, presmooth, 14)

        def restrict(i):
            parts = []
            for j in range(2):
                at = 2 * i + j
                parts.append((1.0 - OMEGA) * source[at] + coupled(ca, vv, at, vv[at], 1))
            total = block_sum(parts[0], parts[1], 1)
            b1[i] = total
            v1[i] = wd1[i] * total
        loop(1, RX1 - 1, restrict, 6)

        for i in range(NX // 2):
            put(vl.at[n], ystage1.at[n], H1 + i, i, v1[H1 + i, 0:NY])
        send_vl = coarse(n)
        halo_send(*send_vl)
        if first:
            gather_cond()
            coarse_couplings()
        during()
        gather_rhs(n + 1)
        after()
        coarse_solve()
        halo_wait(*send_vl)
        if first:
            gather_end(0, 0)
        gather_end(n + 1, 0)
        halo_done(*send_vl)

        for i in range(RX1):
            v1[i] = vl[n, i] + p2[i // 2]

        def postsmooth1(i):
            v = v1[i]
            r1[i] = (1.0 - OMEGA) * v + wd1[i] * (b1[i] + coupled(ca1, v1, i, v, 2))
        loop(1, RX1 - 1, postsmooth1, 6)

        def correct(i):
            for j in range(2):
                vv[2 * i + j] = vv[2 * i + j] + r1[i]
        loop(1, RX1 - 1, correct)

        def postsmooth(i):
            v = vv[i]
            finish(i, (1.0 - OMEGA) * v + wd[i] * (source[i] + coupled(ca, vv, i, v, 1)))
        loop(H - reach, H + NX + reach, postsmooth, 10)

    def hessian(r, n, keep, during, after, arrive):
        def own_scaled(i):
            gp[i, 0:NY] = kk[i, 0:NY] * r[i, 0:NY]
        loop(H, H + NX, own_scaled, 8)

        def own_sensitivity(i):
            value = gp[i]
            z = sd[i] * value + coupled(cd, gp, i, value, 1)
            zp1[i] = z
            vp1[i] = wd[i] * z
        loop(H - 1, H + NX + 1, own_sensitivity, 10)
        contribute(2 * n + 1, zp1, vp1)
        if n == 0:
            arrive()
            gather_send(0)
        gather_send(2 * n + 1)
        if n != 0:
            arrive()

        def scaled(i):
            gg[i] = kk[i] * r[i]
        loop(0, RX, scaled, 8)

        def sensitivity(i):
            value = gg[i]
            zz[i] = sd[i] * value + coupled(cd, gg, i, value, 1)
        loop(1, RX - 1, sensitivity, 14)

        second = z2.at[n]

        def weighted(i, value):
            wkeep[n, i - H] = value[0:NY]
            z = weight[i - H] * value[0:NY]
            put(second, ystage.at[4 + 2 * n], i, i - H, z)
            zp2[i, 0:NY] = z
            vp2[i, 0:NY] = wd[i, 0:NY] * z
        solve(zz, 2 * n, 0, weighted, n == 0)
        send_z2 = fine(second, 4 + 2 * n, H - 1, 1)
        halo_send(*send_z2)
        contribute(2 * n + 2, zp2, vp2)
        gather_send(2 * n + 2)
        halo_wait(*send_z2)
        halo_done(*send_z2)

        def adjoint(i, value):
            pp[i] = value
        solve(second, 2 * n + 1, 1, adjoint, False, during, after)

        def assemble(i):
            p = pp[i]
            misfit = kk[i] * (sd[i] * p - coupled(cd, pp, i, p, 1))
            keep(i, misfit[0:NY] + prior_row(r, i))
        loop(H, H + NX, assemble, 8)

    def arrive_first():
        halo_wait(*send_src)
        halo_done(*send_prior, count=4)
        halo_done(*send_lk)
        halo_done(*send_st)

    zero = jnp.zeros((NY, NZ), F32)
    sums = {}

    def first_products():
        total = [zero, zero]
        for i in range(NX):
            r, w = src[i + H, 0:NY], wkeep[0, i]
            total[0] = total[0] + r * r
            total[1] = total[1] + weight[i] * w * w + r * prior_row(src, i + H)
        dot_prepare(0, (total[0], total[1], zero))

    def keep_first(i, value):
        put(c0, ystage.at[5], i, i - H, value)
    hessian(src, 0, keep_first, first_products, lambda: dot_send(0), arrive_first)
    send_c0 = fine(c0, 5, H, 1)
    halo_send(*send_c0)

    def arrive_second():
        halo_wait(*send_c0)
        halo_done(*send_c0)

    def second_products():
        rr, rc = dot_wait(0)[:2]
        alpha = rr / rc
        sums.update(rr=rr, rc=rc, alpha=alpha)
        for i in range(H - 1, H + NX + 1):
            r1f[i] = src[i] - alpha * c0[i]
        total = [zero, zero, zero]
        for i in range(NX):
            r, w = r1f[i + H, 0:NY], wkeep[0, i] - alpha * wkeep[1, i]
            total[0] = total[0] + r * r
            total[1] = total[1] + weight[i] * w * w + r * prior_row(r1f, i + H)
            total[2] = total[2] + r * c0[i + H, 0:NY]
        dot_prepare(1, total)
        dot_send(1)

    def keep_second(i, value):
        kc[i - H] = value
    hessian(c0, 1, keep_second, second_products, lambda: None, arrive_second)

    norm, product, cross = dot_wait(1)
    alpha = sums["alpha"]
    ratio = norm / sums["rr"]
    beta = norm / (product + 2.0 * ratio * cross + ratio * ratio * sums["rc"])

    def finish(i):
        r, c, later = src[i + H, 0:NY], c0[i + H, 0:NY], r1f[i + H, 0:NY]
        curved = c - alpha * kc[i]
        step_ref[i] = alpha * r + beta * (later + ratio * r)
        resid_ref[i] = later - beta * (curved + ratio * c)
    loop(0, NX, finish)

    halo_done(*send_src)


def scratch():
    vmem = lambda *shape: pltpu.VMEM(shape, F32)
    fine = lambda *lead: vmem(*lead, RX, ROWS, NZ)
    level1 = lambda *lead: vmem(*lead, RX1, ROWS, NZ)
    dma = pltpu.SemaphoreType.DMA
    return [
        fine(), fine(), fine(), fine(), fine(), fine(2), level1(4),
        vmem(7, 2, NX, H, NZ), vmem(7, 2, RX, H, NZ), vmem(4, 2, NX // 2, H, NZ), vmem(4, 2, RX1, H, NZ),
        vmem(NX, NY, NZ), pltpu.VMEM((1, SENSORS), jnp.int32), vmem(1, SENSORS), fine(), vmem(2, NX, NY, NZ),
        fine(), fine(6), fine(), fine(6), fine(), fine(), fine(), fine(), vmem(1, 8, 128), fine(),
        level1(), level1(6), level1(), level1(), level1(), level1(), vmem(4, ROWS, NZ),
        fine(), fine(), fine(), fine(), fine(), level1(), level1(),
        vmem(WIN, PX, 2, NZ), vmem(4, WIN, PX, PIECES, 2, NZ), vmem(2, NZ), vmem(4, PIECES, 2, NZ), vmem(WIN, 8, NZ), vmem(6, WIN, 8, NZ), vmem(WIN, 8, NZ),
        vmem(WIN, 8, NZ), vmem(WIN, 8, NZ), vmem(NX, NY, NZ), vmem(NX, NY, NZ),
        vmem(2, PX * PY, 3, 128), vmem(2, 3, 128),
        dma((4, 8)), dma((4, 8)), dma((2, WIN)), dma((3, WIN)), dma((1,)), dma((2,)), dma((6,)),
    ]


def on_device(log_conductivity, state, gradient, prior_sample, sensor_cells, noise_precision):
    block = jax.ShapeDtypeStruct(log_conductivity.shape, F32)
    vmem = pl.BlockSpec(memory_space=pltpu.VMEM)
    return pl.pallas_call(
        kernel,
        out_shape=(block, block),
        in_specs=[pl.BlockSpec(memory_space=pltpu.HBM)] * 6,
        out_specs=(vmem, vmem),
        scratch_shapes=scratch(),
        compiler_params=pltpu.CompilerParams(
            collective_id=0, has_side_effects=True, vmem_limit_bytes=24 * 1024 * 1024),
    )(*(pltpu.with_memory_space_constraint(x, pltpu.HBM) for x in (
        log_conductivity, state, gradient, prior_sample,
        sensor_cells.reshape(1, SENSORS), noise_precision.reshape(1, SENSORS))))


def solution(mesh):
    field, sensors = P(("ens", "gx"), "gy", None), P(("ens", "gx", "gy"))
    return jax.shard_map(
        on_device,
        mesh=mesh,
        in_specs=(field, field, field, field, sensors, sensors),
        out_specs=(field, field),
        check_vma=False,
    )
```

```python
import jax
import jax.numpy as jnp
from jax import lax
from jax.experimental import pallas as pl
from jax.experimental.pallas import tpu as pltpu
from jax.sharding import PartitionSpec as P

MESH = pl.DeviceIdType.MESH
F32 = jnp.float32

NX, NY, NZ = 8, 16, 256
H, H1 = 4, 2
RX, RX1 = NX + 2 * H, NX // 2 + 2 * H1
ROWS = NY + 2 * H
PX, PY = 4, 8
GX, GY = NX * PX, NY * PY
REACH = 2
WIN = 2 * REACH + 1
COARSE_SWEEPS = 6
PIECES = 3
SENSORS = 512
OMEGA = 0.8
DIRS = ((1, 0), (-1, 0), (0, 1), (0, -1), (1, 1), (1, -1), (-1, 1), (-1, -1))
UNROLL = 2


def kernel(logk_ref, state_ref, grad_ref, prior_ref, cells_ref, prec_ref,
           step_ref, resid_ref,
           lk, st, pr, src, c0, z2, vl, ystage, yrecv, ystage1, yrecv1, grad, cells_in, prec_in, r1f, wkeep,
           kk, ca, wd, cd, sd, gg, zz, vv, cp, pp,
           c1, ca1, wd1, b1, v1, r1, p2,
           gp, zp1, vp1, zp2, vp2, bp, v1p, gat0, gat, chunk0, chunk, cond2, ca2, wd2, rhs2, sol, weight, kc, dots, dchunk,
           h_send, h_recv, g_send, g_recv, d_send, d_recv, in_sem):
    px = lax.axis_index("gx")
    py = lax.axis_index("gy")
    row = lax.broadcasted_iota(jnp.int32, (ROWS, NZ), 0)
    lane = lax.broadcasted_iota(jnp.int32, (ROWS, NZ), 1)
    row8 = lax.broadcasted_iota(jnp.int32, (8, NZ), 0)
    lane8 = lax.broadcasted_iota(jnp.int32, (8, NZ), 1)
    y_in = lane8 & 3
    y_at = py * NY + jnp.where(row < NY + H, row, row - ROWS)

    def loop(low, high, body, unroll=UNROLL):
        whole = (high - low) // unroll

        def step(k, carry):
            for j in range(unroll):
                body(low + k * unroll + j)
            return carry
        if whole > 1:
            lax.fori_loop(0, whole, step, 0)
        for i in range(low + whole * unroll if whole > 1 else low, high):
            body(i)

    def exists(dx, dy):
        return (px + dx >= 0) & (px + dx < PX) & (py + dy >= 0) & (py + dy < PY)

    def halo_copy(field, ys, yr, n, h, wx, k, send, recv, reverse):
        dx, dy = DIRS[k]
        if dy == 0:
            source = field.at[h + n - wx:h + n, 0:NY] if dx == 1 else field.at[h:h + wx, 0:NY]
            target = field.at[h - wx:h, 0:NY] if dx == 1 else field.at[h + n:h + n + wx, 0:NY]
        else:
            side = 1 if dy == 1 else 0
            if dx == 0:
                source, target = ys.at[side], yr.at[side, h:h + n]
            elif dx == 1:
                source, target = ys.at[side, n - h:n], yr.at[side, 0:h]
            else:
                source, target = ys.at[side, 0:h], yr.at[side, h + n:h + n + h]
        if reverse:
            dx, dy = -dx, -dy
        return pltpu.make_async_remote_copy(
            src_ref=source, dst_ref=target, send_sem=send.at[k], recv_sem=recv.at[k],
            device_id={"gx": px + dx, "gy": py + dy}, device_id_type=MESH)

    def halo_clear(field, yr, n, h):
        @pl.when(px == 0)
        def _():
            field[0:h, 0:NY] = jnp.zeros((h, NY, NZ), F32)
            yr[:, 0:h] = jnp.zeros((2, h, H, NZ), F32)

        @pl.when(px == PX - 1)
        def _():
            field[h + n:, 0:NY] = jnp.zeros((h, NY, NZ), F32)
            yr[:, h + n:] = jnp.zeros((2, h, H, NZ), F32)

        @pl.when(py == 0)
        def _():
            yr[1] = jnp.zeros((n + 2 * h, H, NZ), F32)

        @pl.when(py == PY - 1)
        def _():
            yr[0] = jnp.zeros((n + 2 * h, H, NZ), F32)

    def put(field, ys, i, j, value):
        field[i, 0:NY] = value
        ys[0, j] = value[0:H]
        ys[1, j] = value[NY - H:NY]

    def halo_send(field, ys, yr, n, h, wx, send, recv, count=8):
        for k in range(count):
            @pl.when(exists(*DIRS[k]))
            def _(k=k):
                halo_copy(field, ys, yr, n, h, wx, k, send, recv, False).start()

    def halo_wait(field, ys, yr, n, h, wx, send, recv, count=8):
        for k in range(count):
            @pl.when(exists(-DIRS[k][0], -DIRS[k][1]))
            def _(k=k):
                halo_copy(field, ys, yr, n, h, wx, k, send, recv, True).wait_recv()

        def place(i):
            field[i, NY:ROWS] = jnp.concatenate([yr[0, i], yr[1, i]], axis=0)
        loop(0, n + 2 * h, place, 4)

    def halo_done(field, ys, yr, n, h, wx, send, recv, count=8):
        for k in range(count):
            @pl.when(exists(*DIRS[k]))
            def _(k=k):
                halo_copy(field, ys, yr, n, h, wx, k, send, recv, False).wait_send()

    def fine(field, slot, wx, sems):
        return (field, ystage.at[slot], yrecv.at[slot], NX, H, wx, h_send.at[sems], h_recv.at[sems])

    def coarse(slot):
        return (vl.at[slot], ystage1.at[slot], yrecv1.at[slot], NX // 2, H1, H1, h_send.at[0], h_recv.at[0])

    PEERS = [(dx, dy) for dy in (0, 1, -1, 2, -2) for dx in (1, 3, 2, 0) if (dx, dy) != (0, 0)]

    REACHED = (0, 1, -1, 2, -2)

    def buffers(g):
        return (chunk0, gat0) if g == 0 else (chunk.at[g - 1], gat.at[g - 1])

    def sems(g):
        return (g_send.at[0], g_recv.at[0]) if g == 0 else (g_send.at[1], g_recv.at[1 + (g - 1) % 2])

    def gather_send(g):
        mine, all_ = buffers(g)
        sent, arrived = sems(g)
        for dx, dy in PEERS:
            @pl.when((py + dy >= 0) & (py + dy < PY))
            def _(dx=dx, dy=dy):
                pltpu.make_async_remote_copy(
                    src_ref=mine, dst_ref=all_.at[REACH - dy, px],
                    send_sem=sent.at[REACH + dy], recv_sem=arrived.at[REACH - dy],
                    device_id={"gx": lax.rem(px + dx, PX), "gy": py + dy}, device_id_type=MESH).start()
        all_[REACH, px] = mine[...]

    def gather_end(g, which):
        all_ = buffers(g)[1]
        for dy in REACHED:
            @pl.when((py + dy >= 0) & (py + dy < PY))
            def _(dy=dy):
                row_ = all_.at[REACH + dy, 0:PX - 1] if dy == 0 else all_.at[REACH + dy]
                pltpu.make_async_copy(row_, row_, sems(g)[which].at[REACH + dy]).wait()

    def valid(d):
        return (py - REACH + d >= 0) & (py - REACH + d < PY)

    def gather_cond():
        gather_end(0, 1)
        for d in range(WIN):
            whole = jnp.concatenate([gat0[d, p] for p in range(PX)], axis=0)
            cond2[d] = jnp.where(valid(d), whole, 0.0)

    def along_x(piece):
        moved = jnp.where((row8 & 1) == 0, pltpu.roll(piece, 2, 0), pltpu.roll(piece, 6, 0))
        return jnp.where((row8 > 0) & (row8 < 7), moved, 0.0)

    def gather_rhs(g):
        gather_end(g, 1)
        own, ring = [], []
        for d in range(WIN):
            piece = [jnp.concatenate([gat[g - 1, d, p, q] for p in range(PX)], axis=0) for q in range(PIECES)]
            corner = along_x(piece[2])
            corner = jnp.where(y_in == 0, pltpu.roll(corner, NZ - 1, 1), pltpu.roll(corner, 1, 1))
            own.append(jnp.where(valid(d), piece[0] + along_x(piece[1]), 0.0))
            ring.append(jnp.where(valid(d), piece[2] + corner, 0.0))
        zero8 = jnp.zeros((8, NZ), F32)
        for d in range(WIN):
            low = ring[d - 1] if d > 0 else zero8
            high = ring[d + 1] if d < WIN - 1 else zero8
            rhs2[d] = own[d] + jnp.where(y_in == 0, low, jnp.where(y_in == 3, high, 0.0))

    OTHERS = [(dx, dy) for dy in range(PY) for dx in range(PX) if (dx, dy) != (0, 0)]

    def dot_prepare(g, values):
        folded = [jnp.sum(v[:, 0:NZ // 2] + v[:, NZ // 2:NZ], axis=0, keepdims=True) for v in values]
        part = jnp.concatenate(folded, axis=0)
        dchunk[g] = part
        dots[g, px * PY + py] = part

    def dot_send(g):
        for dx, dy in OTHERS:
            pltpu.make_async_remote_copy(
                src_ref=dchunk.at[g], dst_ref=dots.at[g, px * PY + py], send_sem=d_send.at[0], recv_sem=d_recv.at[g],
                device_id={"gx": lax.rem(px + dx, PX), "gy": lax.rem(py + dy, PY)}, device_id_type=MESH).start()

    def dot_wait(g):
        others = dots.at[g, 0:PX * PY - 1]
        pltpu.make_async_copy(others, others, d_recv.at[g]).wait()
        total = dots[g, 0]
        for slot in range(1, PX * PY):
            total = total + dots[g, slot]
        pltpu.make_async_copy(others, others, d_send.at[0]).wait()
        return [jnp.sum(total[i:i + 1], axis=1, keepdims=True) for i in range(total.shape[0])]

    def beside(field, i, value, s):
        return (field[i - 1], field[i + 1], pltpu.roll(value, s, 0), pltpu.roll(value, ROWS - s, 0),
                pltpu.roll(value, s, 1), pltpu.roll(value, NZ - s, 1))

    def coupled(coefs, field, i, value, s):
        near = beside(field, i, value, s)
        total = coefs[0, i] * near[0]
        for f in range(1, 6):
            total = total + coefs[f, i] * near[f]
        return total

    def prior_row(field, i):
        value = field[i]
        near = beside(field, i, value, 1)
        away = near[0] + near[1] + near[2] + near[3]
        away = away + jnp.where(lane >= 1, near[4], 0.0) + jnp.where(lane < NZ - 1, near[5], 0.0)
        return (6.5 * value - away)[0:NY]

    def swap(value, s, axis):
        index, size = (row, ROWS) if axis == 0 else (lane, NZ)
        return jnp.where((index & s) == 0, pltpu.roll(value, size - s, axis), pltpu.roll(value, s, axis))

    def block_sum(low, high, s):
        total = low + high
        total = total + swap(total, s, 1)
        return total + swap(total, s, 0)

    def pick_chunk(value):
        mine = ((row & 3) == 0) & ((row >> 2) == (lane & 3)) & (row < NY)
        return jnp.sum(jnp.where(mine, value, 0.0), axis=0, keepdims=True)

    def pick_ring(value, at):
        mine = ((row == NY) & ((lane & 3) == at)) | ((row == NY + H) & ((lane & 3) == 3 - at))
        return jnp.sum(jnp.where(mine, value, 0.0), axis=0, keepdims=True)

    def inside_yz(s):
        return (y_at >= s, y_at < GY - s, lane >= s, lane < NZ - s)

    def cell_inside(x):
        return jnp.where((x >= 0) & (x < PX * NX), ((y_at >= 0) & (y_at < GY)).astype(F32), 0.0) > 0.5

    own = lambda field: field.at[H:H + NX, 0:NY]
    loads = [pltpu.make_async_copy(source, target, in_sem.at[k]) for k, (source, target) in enumerate((
        (prior_ref, own(pr)), (logk_ref, own(lk)), (state_ref, own(st)), (cells_ref, cells_in), (prec_ref, prec_in),
        (grad_ref, grad)))]
    for load in loads:
        load.start()
    barrier = pltpu.get_barrier_semaphore()
    for k in range(8):
        @pl.when(exists(*DIRS[k]))
        def _(k=k):
            pl.semaphore_signal(barrier, inc=1, device_id={"gx": px + DIRS[k][0], "gy": py + DIRS[k][1]},
                                device_id_type=MESH)
    fields = [(lk, 0), (st, 1), (pr, 2), (src, 3), (z2.at[0], 4), (c0, 5), (z2.at[1], 6)]
    for field, slot in fields:
        halo_clear(field, yrecv.at[slot], NX, H)
    for slot in range(4):
        halo_clear(vl.at[slot], yrecv1.at[slot], NX // 2, H1)
    for field in (gp, zp1, vp1, zp2, vp2):
        def clear(i, field=field):
            field[i] = jnp.zeros((ROWS, NZ), F32)
        loop(1, RX - 1, clear)
    for i in (0, RX1 - 1):
        v1p[i] = jnp.zeros((ROWS, NZ), F32)
    def edges(field, slot):
        for i in range(NX):
            ystage[slot, 0, i] = field[H + i, 0:H]
            ystage[slot, 1, i] = field[H + i, NY - H:NY]
    loads[0].wait()
    edges(pr, 2)
    loads[1].wait()
    edges(lk, 0)
    loads[2].wait()
    edges(st, 1)
    across = jnp.where(px > 0, 1, 0) + jnp.where(px < PX - 1, 1, 0)
    along = jnp.where(py > 0, 1, 0) + jnp.where(py < PY - 1, 1, 0)
    pl.semaphore_wait(barrier, (across + 1) * (along + 1) - 1)

    send_prior, send_lk, send_st = fine(pr, 2, 1, 0), fine(lk, 0, H, 1), fine(st, 1, H, 2)
    halo_send(*send_prior, count=4)
    halo_send(*send_lk)
    halo_send(*send_st)

    loads[3].wait()
    loads[4].wait()
    cells = cells_in[...]
    at_xy = ((cells >> 15) - px * NX) * NY + ((cells >> 8) & (GY - 1)) - py * NY
    at_z = cells & (NZ - 1)
    hot_xy = lax.broadcasted_iota(jnp.int32, (NX * NY, SENSORS), 0) == at_xy
    hot_z = (lax.broadcasted_iota(jnp.int32, (NZ, SENSORS), 0) == at_z).astype(F32).astype(jnp.bfloat16)
    left = jnp.where(hot_xy, prec_in[...], 0.0)
    total = jnp.zeros((NX * NY, NZ), F32)
    for part in range(3):
        piece = left.astype(jnp.bfloat16)
        left = left - piece.astype(F32)
        total = total + lax.dot_general(piece, hot_z, (((1,), (1,)), ((), ())), preferred_element_type=F32)
    for i in range(NX):
        weight[i] = total[i * NY:(i + 1) * NY]

    loads[5].wait()
    halo_wait(*send_prior, count=4)

    def start_source(i):
        put(src, ystage.at[3], i + H, i, prior_row(pr, i + H) - grad[i])
    loop(0, NX, start_source, 8)
    send_src = fine(src, 3, H, 3)
    halo_send(*send_src)

    halo_wait(*send_lk)

    def start_cond(i):
        kk[i] = jnp.exp(lk[i])
    loop(0, RX, start_cond, 8)

    inner = inside_yz(1)

    def start_couplings(i):
        value = kk[i]
        x = px * NX + i - H
        near = beside(kk, i, value, 1)
        in_x = (x > 0, x < GX - 1)
        diag = None
        for f in range(6):
            ok = in_x[f] if f < 2 else inner[f - 2]
            a = 0.5 * (value + jnp.where(ok, near[f], value))
            ca[f, i] = jnp.where(ok, a, 0.0)
            diag = a if diag is None else diag + a
        wd[i] = jnp.where(cell_inside(x), OMEGA / diag, 0.0)
    loop(1, RX - 1, start_couplings, 14)

    def start_level1(i):
        c1[i] = block_sum(kk[2 * i], kk[2 * i + 1], 1) * 0.125
    loop(0, RX1, start_level1, 8)

    for i in range(2):
        chunk0[i:i + 1] = pick_chunk(block_sum(c1[H1 + 2 * i], c1[H1 + 2 * i + 1], 2) * 0.125)

    inner1 = inside_yz(2)

    def start_couplings1(i):
        value = c1[i]
        x = px * NX + 2 * i - H
        near = beside(c1, i, value, 2)
        in_x = (x > 0, x < GX - 2)
        diag = None
        for f in range(6):
            ok = in_x[f] if f < 2 else inner1[f - 2]
            a = value + jnp.where(ok, near[f], value)
            ca1[f, i] = jnp.where(ok, a, 0.0)
            diag = a if diag is None else diag + a
        wd1[i] = jnp.where(cell_inside(x), OMEGA / diag, 0.0)
    loop(1, RX1 - 1, start_couplings1, 6)

    halo_wait(*send_st)

    def start_state(i):
        value = st[i]
        x = px * NX + i - H
        near = beside(st, i, value, 1)
        in_x = (x > 0, x < GX - 1)
        diag = None
        for f in range(6):
            ok = in_x[f] if f < 2 else inner[f - 2]
            d = jnp.where(ok, 0.5 * (value - near[f]), value)
            cd[f, i] = jnp.where(ok, d, 0.0)
            diag = d if diag is None else diag + d
        sd[i] = diag
    loop(1, RX - 1, start_state, 14)


    def coarse_beside(values, d):
        v = values[d]
        zero = jnp.zeros_like(v)
        low = values[d - 1] if d > 0 else zero
        high = values[d + 1] if d < WIN - 1 else zero
        return (pltpu.roll(v, 1, 0), pltpu.roll(v, 7, 0),
                jnp.where(y_in > 0, pltpu.roll(v, 1, 1), pltpu.roll(low, NZ - 3, 1)),
                jnp.where(y_in < 3, pltpu.roll(v, NZ - 1, 1), pltpu.roll(high, 3, 1)),
                pltpu.roll(v, 4, 1), pltpu.roll(v, NZ - 4, 1))

    def coarse_couplings():
        values = [cond2[d] for d in range(WIN)]
        for d in range(WIN):
            place = py - REACH + d
            y = place * 4 + y_in
            inside = (row8 > 0, row8 < 7, y > 0, y < GY // 4 - 1, lane8 >= 4, lane8 < NZ - 4)
            diag = None
            for f, near in enumerate(coarse_beside(values, d)):
                a = 2.0 * (values[d] + jnp.where(inside[f], near, values[d]))
                ca2[f, d] = jnp.where(inside[f], a, 0.0)
                diag = a if diag is None else diag + a
            wd2[d] = jnp.where((place >= 0) & (place < PY), OMEGA / diag, 0.0)

    def coarse_solve():
        def sweep(values, low, high):
            out = list(values)
            for d in range(low, high):
                total = rhs2[d]
                for f, near in enumerate(coarse_beside(values, d)):
                    total = total + ca2[f, d] * near
                out[d] = (1.0 - OMEGA) * values[d] + wd2[d] * total
            return out
        values = sweep([wd2[d] * rhs2[d] for d in range(WIN)], 0, WIN)
        for s in range(2, COARSE_SWEEPS):
            values = sweep(values, 1, WIN - 1)
        for d in range(1, WIN - 1):
            sol[d] = values[d]
        cell = jnp.where(row < NY, row >> 2, jnp.where(row < NY + H, 0, 3))
        for i in range(4):
            x = 2 * px - 1 + i
            at = jnp.clip(x, 0, 7)
            own, high, low = (sol[d, pl.ds(at, 1), :] for d in (REACH, REACH + 1, REACH - 1))
            spread = jnp.where(row < NY, own, jnp.where(row < NY + H, high, low))
            spread = jnp.where((lane & 3) == cell, spread, 0.0)
            spread = spread + swap(spread, 1, 1)
            spread = spread + swap(spread, 2, 1)
            p2[i] = jnp.where((x >= 0) & (x < 8), spread, 0.0)

    def contribute(g, z, v, out):
        def restrict(i):
            parts = [(1.0 - OMEGA) * z[at] + coupled(ca, v, at, v[at], 1) for at in (2 * i, 2 * i + 1)
                     if H - out <= at < H + NX + out]
            total = block_sum(parts[0], parts[-1] if len(parts) > 1 else 0.0, 1)
            bp[i] = total
            v1p[i] = wd1[i] * total
        loop(1, RX1 - 1, restrict, RX1 - 2)

        def level1_residual(i):
            if i == 0:
                return ca1[0, 1] * v1p[1]
            if i == RX1 - 1:
                return ca1[1, RX1 - 2] * v1p[RX1 - 2]
            return (1.0 - OMEGA) * bp[i] + coupled(ca1, v1p, i, v1p[i], 2)
        for j, (q, at) in enumerate(((1, 1), (0, 0), (0, 1), (1, 0))):
            total = block_sum(level1_residual(2 * j), level1_residual(2 * j + 1), 2)
            chunk[g - 1, q, at:at + 1] = pick_chunk(total)
            ringed = pick_ring(total, q)
            if q == 0:
                chunk[g - 1, 2, at:at + 1] = ringed
            else:
                outer = ringed if j == 0 else jnp.concatenate([ringed, outer], axis=0)
        chunk[g - 1, 2] = chunk[g - 1, 2] + outer

    def solve(source, n, reach, finish, first, after=lambda: None):
        def presmooth(i):
            vv[i] = wd[i] * source[i]
        loop(1, RX - 1, presmooth, 14)

        def restrict(i):
            parts = []
            for j in range(2):
                at = 2 * i + j
                parts.append((1.0 - OMEGA) * source[at] + coupled(ca, vv, at, vv[at], 1))
            total = block_sum(parts[0], parts[1], 1)
            b1[i] = total
            v1[i] = wd1[i] * total
        loop(1, RX1 - 1, restrict, 6)

        for i in range(NX // 2):
            put(vl.at[n], ystage1.at[n], H1 + i, i, v1[H1 + i, 0:NY])
        send_vl = coarse(n)
        halo_send(*send_vl)
        if first:
            gather_cond()
            coarse_couplings()
        gather_rhs(n + 1)
        after()
        coarse_solve()
        halo_wait(*send_vl)
        if first:
            gather_end(0, 0)
        gather_end(n + 1, 0)
        halo_done(*send_vl)

        for i in range(RX1):
            v1[i] = vl[n, i] + p2[i // 2]

        def postsmooth1(i):
            v = v1[i]
            r1[i] = (1.0 - OMEGA) * v + wd1[i] * (b1[i] + coupled(ca1, v1, i, v, 2))
        loop(1, RX1 - 1, postsmooth1, 6)

        def correct(i):
            for j in range(2):
                vv[2 * i + j] = vv[2 * i + j] + r1[i]
        loop(1, RX1 - 1, correct)

        def postsmooth(i):
            v = vv[i]
            finish(i, (1.0 - OMEGA) * v + wd[i] * (source[i] + coupled(ca, vv, i, v, 1)))
        loop(H - reach, H + NX + reach, postsmooth, 10)

    def hessian(r, n, keep, during, after, arrive):
        def own_scaled(i):
            gp[i, 0:NY] = kk[i, 0:NY] * r[i, 0:NY]
        loop(H, H + NX, own_scaled, 8)

        def own_sensitivity(i):
            value = gp[i]
            z = sd[i] * value + coupled(cd, gp, i, value, 1)
            zp1[i] = z
            vp1[i] = wd[i] * z
        loop(H - 1, H + NX + 1, own_sensitivity, 10)
        contribute(2 * n + 1, zp1, vp1, 2)
        if n == 0:
            arrive()
            gather_send(0)
        gather_send(2 * n + 1)
        if n != 0:
            arrive()

        def scaled(i):
            gg[i] = kk[i] * r[i]
        loop(0, RX, scaled, 8)

        def sensitivity(i):
            value = gg[i]
            zz[i] = sd[i] * value + coupled(cd, gg, i, value, 1)
        loop(1, RX - 1, sensitivity, 14)

        second = z2.at[n]

        def weighted(i, value):
            wkeep[n, i - H] = value[0:NY]
            z = weight[i - H] * value[0:NY]
            put(second, ystage.at[4 + 2 * n], i, i - H, z)
            zp2[i, 0:NY] = z
            vp2[i, 0:NY] = wd[i, 0:NY] * z
        solve(zz, 2 * n, 0, weighted, n == 0)
        send_z2 = fine(second, 4 + 2 * n, H - 1, 1)
        halo_send(*send_z2)
        contribute(2 * n + 2, zp2, vp2, 1)
        gather_send(2 * n + 2)
        during()
        halo_wait(*send_z2)
        halo_done(*send_z2)

        def adjoint(i, value):
            pp[i] = value
        solve(second, 2 * n + 1, 1, adjoint, False, after)

        def assemble(i):
            p = pp[i]
            misfit = kk[i] * (sd[i] * p - coupled(cd, pp, i, p, 1))
            keep(i, misfit[0:NY] + prior_row(r, i))
        loop(H, H + NX, assemble, 8)

    def arrive_first():
        halo_wait(*send_src)
        halo_done(*send_prior, count=4)
        halo_done(*send_lk)
        halo_done(*send_st)

    zero = jnp.zeros((NY, NZ), F32)
    sums = {}

    def first_products():
        total = [zero, zero]
        for i in range(NX):
            r, w = src[i + H, 0:NY], wkeep[0, i]
            total[0] = total[0] + r * r
            total[1] = total[1] + weight[i] * w * w + r * prior_row(src, i + H)
        dot_prepare(0, (total[0], total[1], zero))

    def keep_first(i, value):
        put(c0, ystage.at[5], i, i - H, value)
    hessian(src, 0, keep_first, first_products, lambda: dot_send(0), arrive_first)
    send_c0 = fine(c0, 5, H, 1)
    halo_send(*send_c0)

    def arrive_second():
        halo_wait(*send_c0)
        halo_done(*send_c0)

    def second_products():
        rr, rc = dot_wait(0)[:2]
        alpha = rr / rc
        sums.update(rr=rr, rc=rc, alpha=alpha)
        for i in range(H - 1, H + NX + 1):
            r1f[i] = src[i] - alpha * c0[i]
        total = [zero, zero, zero]
        for i in range(NX):
            r, w = r1f[i + H, 0:NY], wkeep[0, i] - alpha * wkeep[1, i]
            total[0] = total[0] + r * r
            total[1] = total[1] + weight[i] * w * w + r * prior_row(r1f, i + H)
            total[2] = total[2] + r * c0[i + H, 0:NY]
        dot_prepare(1, total)
        dot_send(1)

    def keep_second(i, value):
        kc[i - H] = value
    hessian(c0, 1, keep_second, second_products, lambda: None, arrive_second)

    norm, product, cross = dot_wait(1)
    alpha = sums["alpha"]
    ratio = norm / sums["rr"]
    beta = norm / (product + 2.0 * ratio * cross + ratio * ratio * sums["rc"])

    def finish(i):
        r, c, later = src[i + H, 0:NY], c0[i + H, 0:NY], r1f[i + H, 0:NY]
        curved = c - alpha * kc[i]
        step_ref[i] = alpha * r + beta * (later + ratio * r)
        resid_ref[i] = later - beta * (curved + ratio * c)
    loop(0, NX, finish)

    halo_done(*send_src)


def scratch():
    vmem = lambda *shape: pltpu.VMEM(shape, F32)
    fine = lambda *lead: vmem(*lead, RX, ROWS, NZ)
    level1 = lambda *lead: vmem(*lead, RX1, ROWS, NZ)
    dma = pltpu.SemaphoreType.DMA
    return [
        fine(), fine(), fine(), fine(), fine(), fine(2), level1(4),
        vmem(7, 2, NX, H, NZ), vmem(7, 2, RX, H, NZ), vmem(4, 2, NX // 2, H, NZ), vmem(4, 2, RX1, H, NZ),
        vmem(NX, NY, NZ), pltpu.VMEM((1, SENSORS), jnp.int32), vmem(1, SENSORS), fine(), vmem(2, NX, NY, NZ),
        fine(), fine(6), fine(), fine(6), fine(), fine(), fine(), fine(), vmem(1, 8, 128), fine(),
        level1(), level1(6), level1(), level1(), level1(), level1(), vmem(4, ROWS, NZ),
        fine(), fine(), fine(), fine(), fine(), level1(), level1(),
        vmem(WIN, PX, 2, NZ), vmem(4, WIN, PX, PIECES, 2, NZ), vmem(2, NZ), vmem(4, PIECES, 2, NZ), vmem(WIN, 8, NZ), vmem(6, WIN, 8, NZ), vmem(WIN, 8, NZ),
        vmem(WIN, 8, NZ), vmem(WIN, 8, NZ), vmem(NX, NY, NZ), vmem(NX, NY, NZ),
        vmem(2, PX * PY, 3, 128), vmem(2, 3, 128),
        dma((4, 8)), dma((4, 8)), dma((2, WIN)), dma((3, WIN)), dma((1,)), dma((2,)), dma((6,)),
    ]


def on_device(log_conductivity, state, gradient, prior_sample, sensor_cells, noise_precision):
    block = jax.ShapeDtypeStruct(log_conductivity.shape, F32)
    vmem = pl.BlockSpec(memory_space=pltpu.VMEM)
    return pl.pallas_call(
        kernel,
        out_shape=(block, block),
        in_specs=[pl.BlockSpec(memory_space=pltpu.HBM)] * 6,
        out_specs=(vmem, vmem),
        scratch_shapes=scratch(),
        compiler_params=pltpu.CompilerParams(
            collective_id=0, has_side_effects=True, vmem_limit_bytes=24 * 1024 * 1024),
    )(*(pltpu.with_memory_space_constraint(x, pltpu.HBM) for x in (
        log_conductivity, state, gradient, prior_sample,
        sensor_cells.reshape(1, SENSORS), noise_precision.reshape(1, SENSORS))))


def solution(mesh):
    field, sensors = P(("ens", "gx"), "gy", None), P(("ens", "gx", "gy"))
    return jax.shard_map(
        on_device,
        mesh=mesh,
        in_specs=(field, field, field, field, sensors, sensors),
        out_specs=(field, field),
        check_vma=False,
    )
```

```python
import jax
import jax.numpy as jnp
from jax import lax
from jax.experimental import pallas as pl
from jax.experimental.pallas import tpu as pltpu
from jax.sharding import PartitionSpec as P

MESH = pl.DeviceIdType.MESH
F32 = jnp.float32

NX, NY, NZ = 8, 16, 256
H, H1 = 4, 2
RX, RX1 = NX + 2 * H, NX // 2 + 2 * H1
ROWS = NY + 2 * H
PX, PY = 4, 8
GX, GY = NX * PX, NY * PY
REACH = 2
WIN = 2 * REACH + 1
COARSE_SWEEPS = 6
PIECES = 3
SENSORS = 512
OMEGA = 0.8
DIRS = ((1, 0), (-1, 0), (0, 1), (0, -1), (1, 1), (1, -1), (-1, 1), (-1, -1))
UNROLL = 2


def kernel(logk_ref, state_ref, grad_ref, prior_ref, cells_ref, prec_ref,
           step_ref, resid_ref,
           lk, st, pr, src, c0, z2, wdx, ystage, yrecv, ystage1, yrecv1, grad, cells_in, prec_in, r1f, wkeep,
           kk, ca, wd, cd, sd, gg, zz, vv, cp, pp,
           c1, ca1, wd1, b1, v1, r1, p2,
           gp, zp1, vp1, zp2, vp2, bp, v1p, xp, yp, xr, yr2, cr, gat0, gat, chunk0, chunk, cond2, ca2, wd2, rhs2, sol, weight, kc, dots, dchunk,
           h_send, h_recv, g_send, g_recv, d_send, d_recv, in_sem):
    px = lax.axis_index("gx")
    py = lax.axis_index("gy")
    row = lax.broadcasted_iota(jnp.int32, (ROWS, NZ), 0)
    lane = lax.broadcasted_iota(jnp.int32, (ROWS, NZ), 1)
    row8 = lax.broadcasted_iota(jnp.int32, (8, NZ), 0)
    lane8 = lax.broadcasted_iota(jnp.int32, (8, NZ), 1)
    y_in = lane8 & 3
    y_at = py * NY + jnp.where(row < NY + H, row, row - ROWS)

    def loop(low, high, body, unroll=UNROLL):
        whole = (high - low) // unroll

        def step(k, carry):
            for j in range(unroll):
                body(low + k * unroll + j)
            return carry
        if whole > 1:
            lax.fori_loop(0, whole, step, 0)
        for i in range(low + whole * unroll if whole > 1 else low, high):
            body(i)

    def exists(dx, dy):
        return (px + dx >= 0) & (px + dx < PX) & (py + dy >= 0) & (py + dy < PY)

    def halo_copy(field, ys, yr, n, h, wx, k, send, recv, reverse):
        dx, dy = DIRS[k]
        if dy == 0:
            source = field.at[h + n - wx:h + n, 0:NY] if dx == 1 else field.at[h:h + wx, 0:NY]
            target = field.at[h - wx:h, 0:NY] if dx == 1 else field.at[h + n:h + n + wx, 0:NY]
        else:
            side = 1 if dy == 1 else 0
            if dx == 0:
                source, target = ys.at[side], yr.at[side, h:h + n]
            elif dx == 1:
                source, target = ys.at[side, n - wx:n], yr.at[side, h - wx:h]
            else:
                source, target = ys.at[side, 0:wx], yr.at[side, h + n:h + n + wx]
        if reverse:
            dx, dy = -dx, -dy
        return pltpu.make_async_remote_copy(
            src_ref=source, dst_ref=target, send_sem=send.at[k], recv_sem=recv.at[k],
            device_id={"gx": px + dx, "gy": py + dy}, device_id_type=MESH)

    def halo_clear(field, yr, n, h):
        @pl.when(px == 0)
        def _():
            field[0:h, 0:NY] = jnp.zeros((h, NY, NZ), F32)
            yr[:, 0:h] = jnp.zeros((2, h, H, NZ), F32)

        @pl.when(px == PX - 1)
        def _():
            field[h + n:, 0:NY] = jnp.zeros((h, NY, NZ), F32)
            yr[:, h + n:] = jnp.zeros((2, h, H, NZ), F32)

        @pl.when(py == 0)
        def _():
            yr[1] = jnp.zeros((n + 2 * h, H, NZ), F32)

        @pl.when(py == PY - 1)
        def _():
            yr[0] = jnp.zeros((n + 2 * h, H, NZ), F32)

    def put(field, ys, i, j, value):
        field[i, 0:NY] = value
        ys[0, j] = value[0:H]
        ys[1, j] = value[NY - H:NY]

    def halo_send(field, ys, yr, n, h, wx, send, recv, count=8):
        for k in range(count):
            @pl.when(exists(*DIRS[k]))
            def _(k=k):
                halo_copy(field, ys, yr, n, h, wx, k, send, recv, False).start()

    def halo_wait(field, ys, yr, n, h, wx, send, recv, count=8):
        for k in range(count):
            @pl.when(exists(-DIRS[k][0], -DIRS[k][1]))
            def _(k=k):
                halo_copy(field, ys, yr, n, h, wx, k, send, recv, True).wait_recv()

        def place(i):
            field[i, NY:ROWS] = jnp.concatenate([yr[0, i], yr[1, i]], axis=0)
        loop(h - wx, n + h + wx, place, 4)

    def halo_done(field, ys, yr, n, h, wx, send, recv, count=8):
        for k in range(count):
            @pl.when(exists(*DIRS[k]))
            def _(k=k):
                halo_copy(field, ys, yr, n, h, wx, k, send, recv, False).wait_send()

    def fine(field, slot, wx, sems):
        return (field, ystage.at[slot], yrecv.at[slot], NX, H, wx, h_send.at[sems], h_recv.at[sems])

    send_wd = (wdx, ystage1, yrecv1, NX // 2, H1, H1, h_send.at[4], h_recv.at[4])

    def pack(first, second, third):
        r = lax.broadcasted_iota(jnp.int32, first.shape, 0) & 1
        l = lax.broadcasted_iota(jnp.int32, first.shape, 1) & 1
        return jnp.where(r == 0, jnp.where(l == 0, first, second), third)

    def unpack(packed):
        n = packed.shape[0]
        r = lax.broadcasted_iota(jnp.int32, packed.shape, 0) & 1
        l = lax.broadcasted_iota(jnp.int32, packed.shape, 1) & 1
        even = jnp.where(r == 0, packed, pltpu.roll(packed, 1, 0))
        return (jnp.where(l == 0, even, pltpu.roll(even, 1, 1)), jnp.where(l == 1, even, pltpu.roll(even, NZ - 1, 1)),
                jnp.where(r == 1, packed, pltpu.roll(packed, n - 1, 0)))

    def share_copy(n, k, reverse):
        dx, dy = DIRS[k]
        side_x, side_y = int(dx == 1), int(dy == 1)
        if dy == 0:
            source, target = xp.at[n, side_x], xr.at[n, 1 - side_x]
        elif dx == 0:
            source, target = yp.at[n, side_y], yr2.at[n, 1 - side_y]
        else:
            source, target = yp.at[n, side_y, side_x], cr.at[n, 1 - side_x, 1 - side_y]
        if reverse:
            dx, dy = -dx, -dy
        sems = 2 * (n % 2)
        return pltpu.make_async_remote_copy(
            src_ref=source, dst_ref=target, send_sem=h_send.at[sems, k], recv_sem=h_recv.at[sems, k],
            device_id={"gx": px + dx, "gy": py + dy}, device_id_type=MESH)

    def share_clear():
        for at, edge in ((0, 0), (1, PX - 1)):
            @pl.when(px == edge)
            def _(at=at):
                for n in range(4):
                    xr[n, at] = jnp.zeros((ROWS, NZ), F32)
                    cr[n, at] = jnp.zeros((2, 8, NZ), F32)
        for at, edge in ((0, 0), (1, PY - 1)):
            @pl.when(py == edge)
            def _(at=at):
                for n in range(4):
                    yr2[n, at] = jnp.zeros((2, 8, NZ), F32)
                    for x in range(2):
                        cr[n, x, at] = jnp.zeros((8, NZ), F32)

    def share_send(n):
        for half in range(2):
            layers = [bp[1 + 3 * half + j] for j in range(3)]
            xp[n, half] = pack(*layers)
            yp[n, 1, half] = pack(*(jnp.where(row8 >= 4, v[8:16], v[16:24]) for v in layers))
            yp[n, 0, half] = pack(*(jnp.where(row8 >= 4, v[16:24], v[0:8]) for v in layers))
        for k in range(8):
            @pl.when(exists(*DIRS[k]))
            def _(k=k):
                share_copy(n, k, False).start()

    def share_wait(n):
        for k in range(8):
            @pl.when(exists(-DIRS[k][0], -DIRS[k][1]))
            def _(k=k):
                share_copy(n, k, True).wait_recv()
        zero = jnp.zeros((8, NZ), F32)

        def placed(v, side):
            upper, lower = jnp.where(row8 >= 4, v, 0.0), jnp.where(row8 < 4, v, 0.0)
            return jnp.concatenate([lower, zero, upper] if side == 0 else [zero, upper, lower], axis=0)
        total = [bp[i] if 0 < i < RX1 - 1 else None for i in range(RX1)]

        def add(i, v):
            total[i] = v if total[i] is None else total[i] + v
        for half, start in ((0, 1), (1, 4)):
            for side in range(2):
                for j, v in enumerate(unpack(yr2[n, side, half])):
                    add(start + j, placed(v, side))
        for side_x, start in ((0, 0), (1, 5)):
            for j, v in enumerate(unpack(xr[n, side_x])):
                add(start + j, v)
            for side_y in range(2):
                for j, v in enumerate(unpack(cr[n, side_x, side_y])):
                    add(start + j, placed(v, side_y))
        for i in range(RX1):
            b1[i] = total[i]
            v1[i] = wdx[i] * total[i]

    def share_done(n):
        for k in range(8):
            @pl.when(exists(*DIRS[k]))
            def _(k=k):
                share_copy(n, k, False).wait_send()

    PEERS = [(dx, dy) for dy in (0, 1, -1, 2, -2) for dx in (1, 3, 2, 0) if (dx, dy) != (0, 0)]

    REACHED = (0, 1, -1, 2, -2)

    def buffers(g):
        return (chunk0, gat0) if g == 0 else (chunk.at[g - 1], gat.at[g - 1])

    def sems(g):
        return (g_send.at[0], g_recv.at[0]) if g == 0 else (g_send.at[1], g_recv.at[1 + (g - 1) % 2])

    def gather_send(g):
        mine, all_ = buffers(g)
        sent, arrived = sems(g)
        for dx, dy in PEERS:
            @pl.when((py + dy >= 0) & (py + dy < PY))
            def _(dx=dx, dy=dy):
                pltpu.make_async_remote_copy(
                    src_ref=mine, dst_ref=all_.at[REACH - dy, px],
                    send_sem=sent.at[REACH + dy], recv_sem=arrived.at[REACH - dy],
                    device_id={"gx": lax.rem(px + dx, PX), "gy": py + dy}, device_id_type=MESH).start()
        all_[REACH, px] = mine[...]

    def gather_end(g, which):
        all_ = buffers(g)[1]
        for dy in REACHED:
            @pl.when((py + dy >= 0) & (py + dy < PY))
            def _(dy=dy):
                row_ = all_.at[REACH + dy, 0:PX - 1] if dy == 0 else all_.at[REACH + dy]
                pltpu.make_async_copy(row_, row_, sems(g)[which].at[REACH + dy]).wait()

    def valid(d):
        return (py - REACH + d >= 0) & (py - REACH + d < PY)

    def gather_cond():
        gather_end(0, 1)
        for d in range(WIN):
            whole = jnp.concatenate([gat0[d, p] for p in range(PX)], axis=0)
            cond2[d] = jnp.where(valid(d), whole, 0.0)

    def along_x(piece):
        moved = jnp.where((row8 & 1) == 0, pltpu.roll(piece, 2, 0), pltpu.roll(piece, 6, 0))
        return jnp.where((row8 > 0) & (row8 < 7), moved, 0.0)

    def gather_rhs(g):
        gather_end(g, 1)
        own, ring = [], []
        for d in range(WIN):
            piece = [jnp.concatenate([gat[g - 1, d, p, q] for p in range(PX)], axis=0) for q in range(PIECES)]
            corner = along_x(piece[2])
            corner = jnp.where(y_in == 0, pltpu.roll(corner, NZ - 1, 1), pltpu.roll(corner, 1, 1))
            own.append(jnp.where(valid(d), piece[0] + along_x(piece[1]), 0.0))
            ring.append(jnp.where(valid(d), piece[2] + corner, 0.0))
        zero8 = jnp.zeros((8, NZ), F32)
        for d in range(WIN):
            low = ring[d - 1] if d > 0 else zero8
            high = ring[d + 1] if d < WIN - 1 else zero8
            rhs2[d] = own[d] + jnp.where(y_in == 0, low, jnp.where(y_in == 3, high, 0.0))

    OTHERS = [(dx, dy) for dy in range(PY) for dx in range(PX) if (dx, dy) != (0, 0)]

    def dot_prepare(g, values):
        folded = [jnp.sum(v[:, 0:NZ // 2] + v[:, NZ // 2:NZ], axis=0, keepdims=True) for v in values]
        part = jnp.concatenate(folded, axis=0)
        dchunk[g] = part
        dots[g, px * PY + py] = part

    def dot_send(g):
        for dx, dy in OTHERS:
            pltpu.make_async_remote_copy(
                src_ref=dchunk.at[g], dst_ref=dots.at[g, px * PY + py], send_sem=d_send.at[0], recv_sem=d_recv.at[g],
                device_id={"gx": lax.rem(px + dx, PX), "gy": lax.rem(py + dy, PY)}, device_id_type=MESH).start()

    def dot_wait(g):
        others = dots.at[g, 0:PX * PY - 1]
        pltpu.make_async_copy(others, others, d_recv.at[g]).wait()
        total = dots[g, 0]
        for slot in range(1, PX * PY):
            total = total + dots[g, slot]
        pltpu.make_async_copy(others, others, d_send.at[0]).wait()
        return [jnp.sum(total[i:i + 1], axis=1, keepdims=True) for i in range(total.shape[0])]

    def beside(field, i, value, s):
        return (field[i - 1], field[i + 1], pltpu.roll(value, s, 0), pltpu.roll(value, ROWS - s, 0),
                pltpu.roll(value, s, 1), pltpu.roll(value, NZ - s, 1))

    def coupled(coefs, field, i, value, s):
        near = beside(field, i, value, s)
        total = coefs[0, i] * near[0]
        for f in range(1, 6):
            total = total + coefs[f, i] * near[f]
        return total

    def prior_row(field, i):
        value = field[i]
        near = beside(field, i, value, 1)
        away = near[0] + near[1] + near[2] + near[3]
        away = away + jnp.where(lane >= 1, near[4], 0.0) + jnp.where(lane < NZ - 1, near[5], 0.0)
        return (6.5 * value - away)[0:NY]

    def swap(value, s, axis):
        index, size = (row, ROWS) if axis == 0 else (lane, NZ)
        return jnp.where((index & s) == 0, pltpu.roll(value, size - s, axis), pltpu.roll(value, s, axis))

    def block_sum(low, high, s):
        total = low + high
        total = total + swap(total, s, 1)
        return total + swap(total, s, 0)

    def pick_chunk(value):
        mine = ((row & 3) == 0) & ((row >> 2) == (lane & 3)) & (row < NY)
        return jnp.sum(jnp.where(mine, value, 0.0), axis=0, keepdims=True)

    def pick_ring(value, at):
        mine = ((row == NY) & ((lane & 3) == at)) | ((row == NY + H) & ((lane & 3) == 3 - at))
        return jnp.sum(jnp.where(mine, value, 0.0), axis=0, keepdims=True)

    def inside_yz(s):
        return (y_at >= s, y_at < GY - s, lane >= s, lane < NZ - s)

    def cell_inside(x):
        return jnp.where((x >= 0) & (x < PX * NX), ((y_at >= 0) & (y_at < GY)).astype(F32), 0.0) > 0.5

    own = lambda field: field.at[H:H + NX, 0:NY]
    loads = [pltpu.make_async_copy(source, target, in_sem.at[k]) for k, (source, target) in enumerate((
        (prior_ref, own(pr)), (logk_ref, own(lk)), (state_ref, own(st)), (cells_ref, cells_in), (prec_ref, prec_in),
        (grad_ref, grad)))]
    for load in loads:
        load.start()
    barrier = pltpu.get_barrier_semaphore()
    for k in range(8):
        @pl.when(exists(*DIRS[k]))
        def _(k=k):
            pl.semaphore_signal(barrier, inc=1, device_id={"gx": px + DIRS[k][0], "gy": py + DIRS[k][1]},
                                device_id_type=MESH)
    fields = [(lk, 0), (st, 1), (pr, 2), (src, 3), (z2.at[0], 4), (c0, 5), (z2.at[1], 6)]
    for field, slot in fields:
        halo_clear(field, yrecv.at[slot], NX, H)
    halo_clear(wdx, yrecv1, NX // 2, H1)
    share_clear()
    for field in (gp, zp1, vp1, zp2, vp2):
        def clear(i, field=field):
            field[i] = jnp.zeros((ROWS, NZ), F32)
        loop(1, RX - 1, clear)
    for i in (0, RX1 - 1):
        v1p[i] = jnp.zeros((ROWS, NZ), F32)
    def edges(field, slot):
        for i in range(NX):
            ystage[slot, 0, i] = field[H + i, 0:H]
            ystage[slot, 1, i] = field[H + i, NY - H:NY]
    loads[0].wait()
    edges(pr, 2)
    loads[1].wait()
    edges(lk, 0)
    loads[2].wait()
    edges(st, 1)
    across = jnp.where(px > 0, 1, 0) + jnp.where(px < PX - 1, 1, 0)
    along = jnp.where(py > 0, 1, 0) + jnp.where(py < PY - 1, 1, 0)
    pl.semaphore_wait(barrier, (across + 1) * (along + 1) - 1)

    send_prior, send_lk, send_st = fine(pr, 2, 1, 0), fine(lk, 0, H, 1), fine(st, 1, 2, 2)
    halo_send(*send_prior, count=4)
    halo_send(*send_lk)
    halo_send(*send_st)

    loads[3].wait()
    loads[4].wait()
    cells = cells_in[...]
    at_xy = ((cells >> 15) - px * NX) * NY + ((cells >> 8) & (GY - 1)) - py * NY
    at_z = cells & (NZ - 1)
    hot_xy = lax.broadcasted_iota(jnp.int32, (NX * NY, SENSORS), 0) == at_xy
    hot_z = (lax.broadcasted_iota(jnp.int32, (NZ, SENSORS), 0) == at_z).astype(F32).astype(jnp.bfloat16)
    left = jnp.where(hot_xy, prec_in[...], 0.0)
    total = jnp.zeros((NX * NY, NZ), F32)
    for part in range(3):
        piece = left.astype(jnp.bfloat16)
        left = left - piece.astype(F32)
        total = total + lax.dot_general(piece, hot_z, (((1,), (1,)), ((), ())), preferred_element_type=F32)
    for i in range(NX):
        weight[i] = total[i * NY:(i + 1) * NY]

    loads[5].wait()
    halo_wait(*send_prior, count=4)

    def start_source(i):
        put(src, ystage.at[3], i + H, i, prior_row(pr, i + H) - grad[i])
    loop(0, NX, start_source, 8)
    send_src = fine(src, 3, 2, 3)
    halo_send(*send_src)

    halo_wait(*send_lk)

    def start_cond(i):
        kk[i] = jnp.exp(lk[i])
    loop(0, RX, start_cond, 8)

    inner = inside_yz(1)

    def start_couplings(i):
        value = kk[i]
        x = px * NX + i - H
        near = beside(kk, i, value, 1)
        in_x = (x > 0, x < GX - 1)
        diag = None
        for f in range(6):
            ok = in_x[f] if f < 2 else inner[f - 2]
            a = 0.5 * (value + jnp.where(ok, near[f], value))
            ca[f, i] = jnp.where(ok, a, 0.0)
            diag = a if diag is None else diag + a
        wd[i] = jnp.where(cell_inside(x), OMEGA / diag, 0.0)
    loop(2, RX - 2, start_couplings, 12)

    def start_level1(i):
        c1[i] = block_sum(kk[2 * i], kk[2 * i + 1], 1) * 0.125
    loop(0, RX1, start_level1, 8)

    for i in range(2):
        chunk0[i:i + 1] = pick_chunk(block_sum(c1[H1 + 2 * i], c1[H1 + 2 * i + 1], 2) * 0.125)

    inner1 = inside_yz(2)

    def start_couplings1(i):
        value = c1[i]
        x = px * NX + 2 * i - H
        near = beside(c1, i, value, 2)
        in_x = (x > 0, x < GX - 2)
        diag = None
        for f in range(6):
            ok = in_x[f] if f < 2 else inner1[f - 2]
            a = value + jnp.where(ok, near[f], value)
            ca1[f, i] = jnp.where(ok, a, 0.0)
            diag = a if diag is None else diag + a
        wd1[i] = jnp.where(cell_inside(x), OMEGA / diag, 0.0)
    loop(1, RX1 - 1, start_couplings1, 6)
    for i in range(NX // 2):
        put(wdx, ystage1, H1 + i, i, wd1[H1 + i, 0:NY])
    halo_send(*send_wd)

    halo_wait(*send_st)

    def start_state(i):
        value = st[i]
        x = px * NX + i - H
        near = beside(st, i, value, 1)
        in_x = (x > 0, x < GX - 1)
        diag = None
        for f in range(6):
            ok = in_x[f] if f < 2 else inner[f - 2]
            d = jnp.where(ok, 0.5 * (value - near[f]), value)
            cd[f, i] = jnp.where(ok, d, 0.0)
            diag = d if diag is None else diag + d
        sd[i] = diag
    loop(3, RX - 3, start_state, 10)


    def coarse_beside(values, d):
        v = values[d]
        zero = jnp.zeros_like(v)
        low = values[d - 1] if d > 0 else zero
        high = values[d + 1] if d < WIN - 1 else zero
        return (pltpu.roll(v, 1, 0), pltpu.roll(v, 7, 0),
                jnp.where(y_in > 0, pltpu.roll(v, 1, 1), pltpu.roll(low, NZ - 3, 1)),
                jnp.where(y_in < 3, pltpu.roll(v, NZ - 1, 1), pltpu.roll(high, 3, 1)),
                pltpu.roll(v, 4, 1), pltpu.roll(v, NZ - 4, 1))

    def coarse_couplings():
        values = [cond2[d] for d in range(WIN)]
        for d in range(WIN):
            place = py - REACH + d
            y = place * 4 + y_in
            inside = (row8 > 0, row8 < 7, y > 0, y < GY // 4 - 1, lane8 >= 4, lane8 < NZ - 4)
            diag = None
            for f, near in enumerate(coarse_beside(values, d)):
                a = 2.0 * (values[d] + jnp.where(inside[f], near, values[d]))
                ca2[f, d] = jnp.where(inside[f], a, 0.0)
                diag = a if diag is None else diag + a
            wd2[d] = jnp.where((place >= 0) & (place < PY), OMEGA / diag, 0.0)

    def coarse_solve():
        def sweep(values, low, high):
            out = list(values)
            for d in range(low, high):
                total = rhs2[d]
                for f, near in enumerate(coarse_beside(values, d)):
                    total = total + ca2[f, d] * near
                out[d] = (1.0 - OMEGA) * values[d] + wd2[d] * total
            return out
        values = sweep([wd2[d] * rhs2[d] for d in range(WIN)], 0, WIN)
        for s in range(2, COARSE_SWEEPS):
            values = sweep(values, 1, WIN - 1)
        for d in range(1, WIN - 1):
            sol[d] = values[d]
        cell = jnp.where(row < NY, row >> 2, jnp.where(row < NY + H, 0, 3))
        for i in range(4):
            x = 2 * px - 1 + i
            at = jnp.clip(x, 0, 7)
            own, high, low = (sol[d, pl.ds(at, 1), :] for d in (REACH, REACH + 1, REACH - 1))
            spread = jnp.where(row < NY, own, jnp.where(row < NY + H, high, low))
            spread = jnp.where((lane & 3) == cell, spread, 0.0)
            spread = spread + swap(spread, 1, 1)
            spread = spread + swap(spread, 2, 1)
            p2[i] = jnp.where((x >= 0) & (x < 8), spread, 0.0)

    def contribute(g, z, v, out):
        def restrict(i):
            parts = [(1.0 - OMEGA) * z[at] + coupled(ca, v, at, v[at], 1) for at in (2 * i, 2 * i + 1)
                     if H - out <= at < H + NX + out]
            total = block_sum(parts[0], parts[-1] if len(parts) > 1 else 0.0, 1)
            bp[i] = total
            v1p[i] = wd1[i] * total
        loop(1, RX1 - 1, restrict, RX1 - 2)

        def level1_residual(i):
            if i == 0:
                return ca1[0, 1] * v1p[1]
            if i == RX1 - 1:
                return ca1[1, RX1 - 2] * v1p[RX1 - 2]
            return (1.0 - OMEGA) * bp[i] + coupled(ca1, v1p, i, v1p[i], 2)
        for j, (q, at) in enumerate(((1, 1), (0, 0), (0, 1), (1, 0))):
            total = block_sum(level1_residual(2 * j), level1_residual(2 * j + 1), 2)
            chunk[g - 1, q, at:at + 1] = pick_chunk(total)
            ringed = pick_ring(total, q)
            if q == 0:
                chunk[g - 1, 2, at:at + 1] = ringed
            else:
                outer = ringed if j == 0 else jnp.concatenate([ringed, outer], axis=0)
        chunk[g - 1, 2] = chunk[g - 1, 2] + outer

    def solve(source, n, reach, finish, first, after=lambda: None):
        def presmooth(i):
            vv[i] = wd[i] * source[i]
        loop(H - 1 - reach, H + NX + 1 + reach, presmooth, NX + 2 + 2 * reach)
        if first:
            halo_wait(*send_wd)
        share_wait(n)
        if first:
            gather_cond()
            coarse_couplings()
        gather_rhs(n + 1)
        after()
        coarse_solve()
        if first:
            gather_end(0, 0)
            halo_done(*send_wd)
        gather_end(n + 1, 0)
        share_done(n)

        for i in range(RX1):
            v1[i] = v1[i] + p2[i // 2]

        def postsmooth1(i):
            v = v1[i]
            r1[i] = (1.0 - OMEGA) * v + wd1[i] * (b1[i] + coupled(ca1, v1, i, v, 2))
        loop(1, RX1 - 1, postsmooth1, 6)

        def correct(i):
            for j in range(2):
                vv[2 * i + j] = vv[2 * i + j] + r1[i]
        loop(1, RX1 - 1, correct)

        def postsmooth(i):
            v = vv[i]
            finish(i, (1.0 - OMEGA) * v + wd[i] * (source[i] + coupled(ca, vv, i, v, 1)))
        loop(H - reach, H + NX + reach, postsmooth, 10)

    def hessian(r, n, keep, during, after, arrive):
        def own_scaled(i):
            gp[i, 0:NY] = kk[i, 0:NY] * r[i, 0:NY]
        loop(H, H + NX, own_scaled, 8)

        def own_sensitivity(i):
            value = gp[i]
            z = sd[i] * value + coupled(cd, gp, i, value, 1)
            zp1[i] = z
            vp1[i] = wd[i] * z
        loop(H - 1, H + NX + 1, own_sensitivity, 10)
        contribute(2 * n + 1, zp1, vp1, 2)
        if n == 0:
            arrive()
            gather_send(0)
        gather_send(2 * n + 1)
        share_send(2 * n)
        if n != 0:
            arrive()

        def scaled(i):
            gg[i] = kk[i] * r[i]
        loop(2, RX - 2, scaled, 12)

        def sensitivity(i):
            value = gg[i]
            zz[i] = sd[i] * value + coupled(cd, gg, i, value, 1)
        loop(3, RX - 3, sensitivity, 10)

        second = z2.at[n]

        def weighted(i, value):
            wkeep[n, i - H] = value[0:NY]
            z = weight[i - H] * value[0:NY]
            put(second, ystage.at[4 + 2 * n], i, i - H, z)
            zp2[i, 0:NY] = z
            vp2[i, 0:NY] = wd[i, 0:NY] * z
        solve(zz, 2 * n, 0, weighted, n == 0)
        send_z2 = fine(second, 4 + 2 * n, 2, 1)
        halo_send(*send_z2)
        contribute(2 * n + 2, zp2, vp2, 1)
        gather_send(2 * n + 2)
        share_send(2 * n + 1)
        during()
        halo_wait(*send_z2)
        halo_done(*send_z2)

        def adjoint(i, value):
            pp[i] = value
        solve(second, 2 * n + 1, 1, adjoint, False, after)

        def assemble(i):
            p = pp[i]
            misfit = kk[i] * (sd[i] * p - coupled(cd, pp, i, p, 1))
            keep(i, misfit[0:NY] + prior_row(r, i))
        loop(H, H + NX, assemble, 8)

    def arrive_first():
        halo_wait(*send_src)
        halo_done(*send_prior, count=4)
        halo_done(*send_lk)
        halo_done(*send_st)

    zero = jnp.zeros((NY, NZ), F32)
    sums = {}

    def first_products():
        total = [zero, zero]
        for i in range(NX):
            r, w = src[i + H, 0:NY], wkeep[0, i]
            total[0] = total[0] + r * r
            total[1] = total[1] + weight[i] * w * w + r * prior_row(src, i + H)
        dot_prepare(0, (total[0], total[1], zero))

    def keep_first(i, value):
        put(c0, ystage.at[5], i, i - H, value)
    hessian(src, 0, keep_first, first_products, lambda: dot_send(0), arrive_first)
    halo_done(*send_src)
    send_c0 = fine(c0, 5, 2, 3)
    halo_send(*send_c0)

    def arrive_second():
        halo_wait(*send_c0)
        halo_done(*send_c0)

    def second_products():
        rr, rc = dot_wait(0)[:2]
        alpha = rr / rc
        sums.update(rr=rr, rc=rc, alpha=alpha)
        for i in range(H - 1, H + NX + 1):
            r1f[i] = src[i] - alpha * c0[i]
        total = [zero, zero, zero]
        for i in range(NX):
            r, w = r1f[i + H, 0:NY], wkeep[0, i] - alpha * wkeep[1, i]
            total[0] = total[0] + r * r
            total[1] = total[1] + weight[i] * w * w + r * prior_row(r1f, i + H)
            total[2] = total[2] + r * c0[i + H, 0:NY]
        dot_prepare(1, total)
        dot_send(1)

    def keep_second(i, value):
        kc[i - H] = value
    hessian(c0, 1, keep_second, second_products, lambda: None, arrive_second)

    norm, product, cross = dot_wait(1)
    alpha = sums["alpha"]
    ratio = norm / sums["rr"]
    beta = norm / (product + 2.0 * ratio * cross + ratio * ratio * sums["rc"])

    def finish(i):
        r, c, later = src[i + H, 0:NY], c0[i + H, 0:NY], r1f[i + H, 0:NY]
        curved = c - alpha * kc[i]
        step_ref[i] = alpha * r + beta * (later + ratio * r)
        resid_ref[i] = later - beta * (curved + ratio * c)
    loop(0, NX, finish)


def scratch():
    vmem = lambda *shape: pltpu.VMEM(shape, F32)
    fine = lambda *lead: vmem(*lead, RX, ROWS, NZ)
    level1 = lambda *lead: vmem(*lead, RX1, ROWS, NZ)
    dma = pltpu.SemaphoreType.DMA
    return [
        fine(), fine(), fine(), fine(), fine(), fine(2), level1(),
        vmem(7, 2, NX, H, NZ), vmem(7, 2, RX, H, NZ), vmem(2, NX // 2, H, NZ), vmem(2, RX1, H, NZ),
        vmem(NX, NY, NZ), pltpu.VMEM((1, SENSORS), jnp.int32), vmem(1, SENSORS), fine(), vmem(2, NX, NY, NZ),
        fine(), fine(6), fine(), fine(6), fine(), fine(), fine(), fine(), vmem(1, 8, 128), fine(),
        level1(), level1(6), level1(), level1(), level1(), level1(), vmem(4, ROWS, NZ),
        fine(), fine(), fine(), fine(), fine(), level1(), level1(),
        vmem(4, 2, ROWS, NZ), vmem(4, 2, 2, 8, NZ), vmem(4, 2, ROWS, NZ), vmem(4, 2, 2, 8, NZ), vmem(4, 2, 2, 8, NZ),
        vmem(WIN, PX, 2, NZ), vmem(4, WIN, PX, PIECES, 2, NZ), vmem(2, NZ), vmem(4, PIECES, 2, NZ), vmem(WIN, 8, NZ), vmem(6, WIN, 8, NZ), vmem(WIN, 8, NZ),
        vmem(WIN, 8, NZ), vmem(WIN, 8, NZ), vmem(NX, NY, NZ), vmem(NX, NY, NZ),
        vmem(2, PX * PY, 3, 128), vmem(2, 3, 128),
        dma((5, 8)), dma((5, 8)), dma((2, WIN)), dma((3, WIN)), dma((1,)), dma((2,)), dma((6,)),
    ]


def on_device(log_conductivity, state, gradient, prior_sample, sensor_cells, noise_precision):
    block = jax.ShapeDtypeStruct(log_conductivity.shape, F32)
    vmem = pl.BlockSpec(memory_space=pltpu.VMEM)
    return pl.pallas_call(
        kernel,
        out_shape=(block, block),
        in_specs=[pl.BlockSpec(memory_space=pltpu.HBM)] * 6,
        out_specs=(vmem, vmem),
        scratch_shapes=scratch(),
        compiler_params=pltpu.CompilerParams(
            collective_id=0, has_side_effects=True, vmem_limit_bytes=24 * 1024 * 1024),
    )(*(pltpu.with_memory_space_constraint(x, pltpu.HBM) for x in (
        log_conductivity, state, gradient, prior_sample,
        sensor_cells.reshape(1, SENSORS), noise_precision.reshape(1, SENSORS))))


def solution(mesh):
    field, sensors = P(("ens", "gx"), "gy", None), P(("ens", "gx", "gy"))
    return jax.shard_map(
        on_device,
        mesh=mesh,
        in_specs=(field, field, field, field, sensors, sensors),
        out_specs=(field, field),
        check_vma=False,
    )
```

```python
import jax
import jax.numpy as jnp
from jax import lax
from jax.experimental import pallas as pl
from jax.experimental.pallas import tpu as pltpu
from jax.sharding import PartitionSpec as P

MESH = pl.DeviceIdType.MESH
F32 = jnp.float32

NX, NY, NZ = 8, 16, 256
H, H1 = 4, 2
RX, RX1 = NX + 2 * H, NX // 2 + 2 * H1
ROWS = NY + 2 * H
PX, PY = 4, 8
GX, GY = NX * PX, NY * PY
REACH = 2
WIN = 2 * REACH + 1
COARSE_SWEEPS = 6
PIECES = 3
SENSORS = 512
OMEGA = 0.8
DIRS = ((1, 0), (-1, 0), (0, 1), (0, -1), (1, 1), (1, -1), (-1, 1), (-1, -1))
UNROLL = 2


def kernel(logk_ref, state_ref, grad_ref, prior_ref, cells_ref, prec_ref,
           step_ref, resid_ref,
           lk, st, pr, src, c0, z2, wdx, ystage, yrecv, ystage1, yrecv1, grad, cells_in, prec_in, r1f, wkeep, partial,
           kk, ca, wd, cd, sd, gg, zz, vv, cp, pp,
           c1, ca1, wd1, b1, v1, r1, p2,
           gp, zp1, vp1, zp2, vp2, bp, v1p, xp, yp, xr, yr2, cr, gat0, gat, chunk0, chunk, cond2, ca2, wd2, rhs2, sol, weight, kc, dots, dchunk,
           h_send, h_recv, g_send, g_recv, d_send, d_recv, in_sem):
    px = lax.axis_index("gx")
    py = lax.axis_index("gy")
    row = lax.broadcasted_iota(jnp.int32, (ROWS, NZ), 0)
    lane = lax.broadcasted_iota(jnp.int32, (ROWS, NZ), 1)
    row8 = lax.broadcasted_iota(jnp.int32, (8, NZ), 0)
    lane8 = lax.broadcasted_iota(jnp.int32, (8, NZ), 1)
    y_in = lane8 & 3
    y_at = py * NY + jnp.where(row < NY + H, row, row - ROWS)

    def loop(low, high, body, unroll=UNROLL):
        whole = (high - low) // unroll

        def step(k, carry):
            for j in range(unroll):
                body(low + k * unroll + j)
            return carry
        if whole > 1:
            lax.fori_loop(0, whole, step, 0)
        for i in range(low + whole * unroll if whole > 1 else low, high):
            body(i)

    def exists(dx, dy):
        return (px + dx >= 0) & (px + dx < PX) & (py + dy >= 0) & (py + dy < PY)

    def halo_copy(field, ys, yr, n, h, wx, k, send, recv, reverse):
        dx, dy = DIRS[k]
        if dy == 0:
            source = field.at[h + n - wx:h + n, 0:NY] if dx == 1 else field.at[h:h + wx, 0:NY]
            target = field.at[h - wx:h, 0:NY] if dx == 1 else field.at[h + n:h + n + wx, 0:NY]
        else:
            side = 1 if dy == 1 else 0
            if dx == 0:
                source, target = ys.at[side], yr.at[side, h:h + n]
            elif dx == 1:
                source, target = ys.at[side, n - wx:n], yr.at[side, h - wx:h]
            else:
                source, target = ys.at[side, 0:wx], yr.at[side, h + n:h + n + wx]
        if reverse:
            dx, dy = -dx, -dy
        return pltpu.make_async_remote_copy(
            src_ref=source, dst_ref=target, send_sem=send.at[k], recv_sem=recv.at[k],
            device_id={"gx": px + dx, "gy": py + dy}, device_id_type=MESH)

    def halo_clear(field, yr, n, h):
        @pl.when(px == 0)
        def _():
            field[0:h, 0:NY] = jnp.zeros((h, NY, NZ), F32)
            yr[:, 0:h] = jnp.zeros((2, h, H, NZ), F32)

        @pl.when(px == PX - 1)
        def _():
            field[h + n:, 0:NY] = jnp.zeros((h, NY, NZ), F32)
            yr[:, h + n:] = jnp.zeros((2, h, H, NZ), F32)

        @pl.when(py == 0)
        def _():
            yr[1] = jnp.zeros((n + 2 * h, H, NZ), F32)

        @pl.when(py == PY - 1)
        def _():
            yr[0] = jnp.zeros((n + 2 * h, H, NZ), F32)

    def put(field, ys, i, j, value):
        field[i, 0:NY] = value
        ys[0, j] = value[0:H]
        ys[1, j] = value[NY - H:NY]

    def halo_send(field, ys, yr, n, h, wx, send, recv, count=8):
        for k in range(count):
            @pl.when(exists(*DIRS[k]))
            def _(k=k):
                halo_copy(field, ys, yr, n, h, wx, k, send, recv, False).start()

    def halo_wait(field, ys, yr, n, h, wx, send, recv, count=8):
        for k in range(count):
            @pl.when(exists(-DIRS[k][0], -DIRS[k][1]))
            def _(k=k):
                halo_copy(field, ys, yr, n, h, wx, k, send, recv, True).wait_recv()

        def place(i):
            field[i, NY:ROWS] = jnp.concatenate([yr[0, i], yr[1, i]], axis=0)
        loop(h - wx, n + h + wx, place, 4)

    def halo_done(field, ys, yr, n, h, wx, send, recv, count=8):
        for k in range(count):
            @pl.when(exists(*DIRS[k]))
            def _(k=k):
                halo_copy(field, ys, yr, n, h, wx, k, send, recv, False).wait_send()

    def fine(field, slot, wx, sems):
        return (field, ystage.at[slot], yrecv.at[slot], NX, H, wx, h_send.at[sems], h_recv.at[sems])

    send_wd = (wdx, ystage1, yrecv1, NX // 2, H1, H1, h_send.at[4], h_recv.at[4])

    def pack(first, second, third):
        r = lax.broadcasted_iota(jnp.int32, first.shape, 0) & 1
        l = lax.broadcasted_iota(jnp.int32, first.shape, 1) & 1
        return jnp.where(r == 0, jnp.where(l == 0, first, second), third)

    def unpack(packed):
        n = packed.shape[0]
        r = lax.broadcasted_iota(jnp.int32, packed.shape, 0) & 1
        l = lax.broadcasted_iota(jnp.int32, packed.shape, 1) & 1
        even = jnp.where(r == 0, packed, pltpu.roll(packed, 1, 0))
        return (jnp.where(l == 0, even, pltpu.roll(even, 1, 1)), jnp.where(l == 1, even, pltpu.roll(even, NZ - 1, 1)),
                jnp.where(r == 1, packed, pltpu.roll(packed, n - 1, 0)))

    def share_copy(n, k, reverse):
        dx, dy = DIRS[k]
        side_x, side_y = int(dx == 1), int(dy == 1)
        if dy == 0:
            source, target = xp.at[n, side_x], xr.at[n, 1 - side_x]
        elif dx == 0:
            source, target = yp.at[n, side_y], yr2.at[n, 1 - side_y]
        else:
            source, target = yp.at[n, side_y, side_x], cr.at[n, 1 - side_x, 1 - side_y]
        if reverse:
            dx, dy = -dx, -dy
        sems = 2 * (n % 2)
        return pltpu.make_async_remote_copy(
            src_ref=source, dst_ref=target, send_sem=h_send.at[sems, k], recv_sem=h_recv.at[sems, k],
            device_id={"gx": px + dx, "gy": py + dy}, device_id_type=MESH)

    def share_clear():
        for at, edge in ((0, 0), (1, PX - 1)):
            @pl.when(px == edge)
            def _(at=at):
                for n in range(4):
                    xr[n, at] = jnp.zeros((ROWS, NZ), F32)
                    cr[n, at] = jnp.zeros((2, 8, NZ), F32)
        for at, edge in ((0, 0), (1, PY - 1)):
            @pl.when(py == edge)
            def _(at=at):
                for n in range(4):
                    yr2[n, at] = jnp.zeros((2, 8, NZ), F32)
                    for x in range(2):
                        cr[n, x, at] = jnp.zeros((8, NZ), F32)

    def share_send(n):
        for half in range(2):
            layers = [bp[1 + 3 * half + j] for j in range(3)]
            xp[n, half] = pack(*layers)
            yp[n, 1, half] = pack(*(jnp.where(row8 >= 4, v[8:16], v[16:24]) for v in layers))
            yp[n, 0, half] = pack(*(jnp.where(row8 >= 4, v[16:24], v[0:8]) for v in layers))
        for k in range(8):
            @pl.when(exists(*DIRS[k]))
            def _(k=k):
                share_copy(n, k, False).start()

    def share_wait(n):
        for k in range(8):
            @pl.when(exists(-DIRS[k][0], -DIRS[k][1]))
            def _(k=k):
                share_copy(n, k, True).wait_recv()
        zero = jnp.zeros((8, NZ), F32)

        def placed(v, side):
            upper, lower = jnp.where(row8 >= 4, v, 0.0), jnp.where(row8 < 4, v, 0.0)
            return jnp.concatenate([lower, zero, upper] if side == 0 else [zero, upper, lower], axis=0)
        total = [bp[i] if 0 < i < RX1 - 1 else None for i in range(RX1)]

        def add(i, v):
            total[i] = v if total[i] is None else total[i] + v
        for half, start in ((0, 1), (1, 4)):
            for side in range(2):
                for j, v in enumerate(unpack(yr2[n, side, half])):
                    add(start + j, placed(v, side))
        for side_x, start in ((0, 0), (1, 5)):
            for j, v in enumerate(unpack(xr[n, side_x])):
                add(start + j, v)
            for side_y in range(2):
                for j, v in enumerate(unpack(cr[n, side_x, side_y])):
                    add(start + j, placed(v, side_y))
        for i in range(RX1):
            b1[i] = total[i]
            v1[i] = wdx[i] * total[i]

    def share_done(n):
        for k in range(8):
            @pl.when(exists(*DIRS[k]))
            def _(k=k):
                share_copy(n, k, False).wait_send()

    PEERS = [(dx, dy) for dy in (2, -2, 1, -1, 0) for dx in (2, 1, 3, 0) if (dx, dy) != (0, 0)]

    REACHED = (0, 1, -1, 2, -2)

    def buffers(g):
        return (chunk0, gat0) if g == 0 else (chunk.at[g - 1], gat.at[g - 1])

    def sems(g):
        return (g_send.at[0], g_recv.at[0]) if g == 0 else (g_send.at[1], g_recv.at[1 + (g - 1) % 2])

    def gather_send(g):
        mine, all_ = buffers(g)
        sent, arrived = sems(g)
        for dx, dy in PEERS:
            @pl.when((py + dy >= 0) & (py + dy < PY))
            def _(dx=dx, dy=dy):
                pltpu.make_async_remote_copy(
                    src_ref=mine, dst_ref=all_.at[REACH - dy, px],
                    send_sem=sent.at[REACH + dy], recv_sem=arrived.at[REACH - dy],
                    device_id={"gx": lax.rem(px + dx, PX), "gy": py + dy}, device_id_type=MESH).start()
        all_[REACH, px] = mine[...]

    def gather_end(g, which):
        all_ = buffers(g)[1]
        for dy in REACHED:
            @pl.when((py + dy >= 0) & (py + dy < PY))
            def _(dy=dy):
                row_ = all_.at[REACH + dy, 0:PX - 1] if dy == 0 else all_.at[REACH + dy]
                pltpu.make_async_copy(row_, row_, sems(g)[which].at[REACH + dy]).wait()

    def valid(d):
        return (py - REACH + d >= 0) & (py - REACH + d < PY)

    def gather_cond():
        gather_end(0, 1)
        for d in range(WIN):
            whole = jnp.concatenate([gat0[d, p] for p in range(PX)], axis=0)
            cond2[d] = jnp.where(valid(d), whole, 0.0)

    def along_x(piece):
        moved = jnp.where((row8 & 1) == 0, pltpu.roll(piece, 2, 0), pltpu.roll(piece, 6, 0))
        return jnp.where((row8 > 0) & (row8 < 7), moved, 0.0)

    def gather_rhs(g):
        gather_end(g, 1)
        own, ring = [], []
        for d in range(WIN):
            piece = [jnp.concatenate([gat[g - 1, d, p, q] for p in range(PX)], axis=0) for q in range(PIECES)]
            corner = along_x(piece[2])
            corner = jnp.where(y_in == 0, pltpu.roll(corner, NZ - 1, 1), pltpu.roll(corner, 1, 1))
            own.append(jnp.where(valid(d), piece[0] + along_x(piece[1]), 0.0))
            ring.append(jnp.where(valid(d), piece[2] + corner, 0.0))
        zero8 = jnp.zeros((8, NZ), F32)
        for d in range(WIN):
            low = ring[d - 1] if d > 0 else zero8
            high = ring[d + 1] if d < WIN - 1 else zero8
            rhs2[d] = own[d] + jnp.where(y_in == 0, low, jnp.where(y_in == 3, high, 0.0))

    OTHERS = [(dx, dy) for dy in (4, 3, 5, 2, 6, 1, 7, 0) for dx in (2, 1, 3, 0) if (dx, dy) != (0, 0)]

    def dot_prepare(g, values):
        folded = [jnp.sum(v[:, 0:NZ // 2] + v[:, NZ // 2:NZ], axis=0, keepdims=True) for v in values]
        part = jnp.concatenate(folded, axis=0)
        dchunk[g] = part
        dots[g, px * PY + py] = part

    def dot_send(g):
        for dx, dy in OTHERS:
            pltpu.make_async_remote_copy(
                src_ref=dchunk.at[g], dst_ref=dots.at[g, px * PY + py], send_sem=d_send.at[0], recv_sem=d_recv.at[g],
                device_id={"gx": lax.rem(px + dx, PX), "gy": lax.rem(py + dy, PY)}, device_id_type=MESH).start()

    def dot_wait(g):
        others = dots.at[g, 0:PX * PY - 1]
        pltpu.make_async_copy(others, others, d_recv.at[g]).wait()
        total = dots[g, 0]
        for slot in range(1, PX * PY):
            total = total + dots[g, slot]
        pltpu.make_async_copy(others, others, d_send.at[0]).wait()
        return [jnp.sum(total[i:i + 1], axis=1, keepdims=True) for i in range(total.shape[0])]

    def beside(field, i, value, s):
        return (field[i - 1], field[i + 1], pltpu.roll(value, s, 0), pltpu.roll(value, ROWS - s, 0),
                pltpu.roll(value, s, 1), pltpu.roll(value, NZ - s, 1))

    def coupled(coefs, field, i, value, s):
        near = beside(field, i, value, s)
        total = coefs[0, i] * near[0]
        for f in range(1, 6):
            total = total + coefs[f, i] * near[f]
        return total

    def prior_row(field, i):
        value = field[i]
        near = beside(field, i, value, 1)
        away = near[0] + near[1] + near[2] + near[3]
        away = away + jnp.where(lane >= 1, near[4], 0.0) + jnp.where(lane < NZ - 1, near[5], 0.0)
        return (6.5 * value - away)[0:NY]

    def swap(value, s, axis):
        index, size = (row, ROWS) if axis == 0 else (lane, NZ)
        return jnp.where((index & s) == 0, pltpu.roll(value, size - s, axis), pltpu.roll(value, s, axis))

    def block_sum(low, high, s):
        total = low + high
        total = total + swap(total, s, 1)
        return total + swap(total, s, 0)

    def pick_chunk(value):
        mine = ((row & 3) == 0) & ((row >> 2) == (lane & 3)) & (row < NY)
        return jnp.sum(jnp.where(mine, value, 0.0), axis=0, keepdims=True)

    def pick_ring(value, at):
        mine = ((row == NY) & ((lane & 3) == at)) | ((row == NY + H) & ((lane & 3) == 3 - at))
        return jnp.sum(jnp.where(mine, value, 0.0), axis=0, keepdims=True)

    def inside_yz(s):
        return (y_at >= s, y_at < GY - s, lane >= s, lane < NZ - s)

    def cell_inside(x):
        return jnp.where((x >= 0) & (x < PX * NX), ((y_at >= 0) & (y_at < GY)).astype(F32), 0.0) > 0.5

    own = lambda field: field.at[H:H + NX, 0:NY]
    loads = [pltpu.make_async_copy(source, target, in_sem.at[k]) for k, (source, target) in enumerate((
        (prior_ref, own(pr)), (logk_ref, own(lk)), (state_ref, own(st)), (cells_ref, cells_in), (prec_ref, prec_in),
        (grad_ref, grad)))]
    for load in loads:
        load.start()
    barrier = pltpu.get_barrier_semaphore()
    for k in range(8):
        @pl.when(exists(*DIRS[k]))
        def _(k=k):
            pl.semaphore_signal(barrier, inc=1, device_id={"gx": px + DIRS[k][0], "gy": py + DIRS[k][1]},
                                device_id_type=MESH)
    fields = [(lk, 0), (st, 1), (pr, 2), (src, 3), (z2.at[0], 4), (c0, 5), (z2.at[1], 6)]
    for field, slot in fields:
        halo_clear(field, yrecv.at[slot], NX, H)
    halo_clear(wdx, yrecv1, NX // 2, H1)
    share_clear()
    for field in (gp, zp1, vp1, zp2, vp2):
        def clear(i, field=field):
            field[i] = jnp.zeros((ROWS, NZ), F32)
        loop(1, RX - 1, clear)
    for i in (0, RX1 - 1):
        v1p[i] = jnp.zeros((ROWS, NZ), F32)
    def edges(field, slot):
        for i in range(NX):
            ystage[slot, 0, i] = field[H + i, 0:H]
            ystage[slot, 1, i] = field[H + i, NY - H:NY]
    loads[0].wait()
    edges(pr, 2)
    loads[1].wait()
    edges(lk, 0)
    loads[2].wait()
    edges(st, 1)
    across = jnp.where(px > 0, 1, 0) + jnp.where(px < PX - 1, 1, 0)
    along = jnp.where(py > 0, 1, 0) + jnp.where(py < PY - 1, 1, 0)
    pl.semaphore_wait(barrier, (across + 1) * (along + 1) - 1)

    send_prior, send_lk, send_st = fine(pr, 2, 1, 0), fine(lk, 0, H, 1), fine(st, 1, 2, 2)
    halo_send(*send_prior, count=4)
    halo_send(*send_lk)
    halo_send(*send_st)

    loads[3].wait()
    loads[4].wait()
    cells = cells_in[...]
    at_xy = ((cells >> 15) - px * NX) * NY + ((cells >> 8) & (GY - 1)) - py * NY
    at_z = cells & (NZ - 1)
    hot_xy = lax.broadcasted_iota(jnp.int32, (NX * NY, SENSORS), 0) == at_xy
    hot_z = (lax.broadcasted_iota(jnp.int32, (NZ, SENSORS), 0) == at_z).astype(F32).astype(jnp.bfloat16)
    left = jnp.where(hot_xy, prec_in[...], 0.0)
    total = jnp.zeros((NX * NY, NZ), F32)
    for part in range(3):
        piece = left.astype(jnp.bfloat16)
        left = left - piece.astype(F32)
        total = total + lax.dot_general(piece, hot_z, (((1,), (1,)), ((), ())), preferred_element_type=F32)
    for i in range(NX):
        weight[i] = total[i * NY:(i + 1) * NY]

    loads[5].wait()
    halo_wait(*send_prior, count=4)

    def start_source(i):
        put(src, ystage.at[3], i + H, i, prior_row(pr, i + H) - grad[i])
    loop(0, NX, start_source, 8)
    send_src = fine(src, 3, 2, 3)
    halo_send(*send_src)

    halo_wait(*send_lk)

    def start_cond(i):
        kk[i] = jnp.exp(lk[i])
    loop(0, RX, start_cond, 8)

    inner = inside_yz(1)

    def start_couplings(i):
        value = kk[i]
        x = px * NX + i - H
        near = beside(kk, i, value, 1)
        in_x = (x > 0, x < GX - 1)
        diag = None
        for f in range(6):
            ok = in_x[f] if f < 2 else inner[f - 2]
            a = 0.5 * (value + jnp.where(ok, near[f], value))
            ca[f, i] = jnp.where(ok, a, 0.0)
            diag = a if diag is None else diag + a
        wd[i] = jnp.where(cell_inside(x), OMEGA / diag, 0.0)
    loop(2, RX - 2, start_couplings, 12)

    def start_level1(i):
        c1[i] = block_sum(kk[2 * i], kk[2 * i + 1], 1) * 0.125
    loop(0, RX1, start_level1, 8)

    for i in range(2):
        chunk0[i:i + 1] = pick_chunk(block_sum(c1[H1 + 2 * i], c1[H1 + 2 * i + 1], 2) * 0.125)

    inner1 = inside_yz(2)

    def start_couplings1(i):
        value = c1[i]
        x = px * NX + 2 * i - H
        near = beside(c1, i, value, 2)
        in_x = (x > 0, x < GX - 2)
        diag = None
        for f in range(6):
            ok = in_x[f] if f < 2 else inner1[f - 2]
            a = value + jnp.where(ok, near[f], value)
            ca1[f, i] = jnp.where(ok, a, 0.0)
            diag = a if diag is None else diag + a
        wd1[i] = jnp.where(cell_inside(x), OMEGA / diag, 0.0)
    loop(1, RX1 - 1, start_couplings1, 6)
    for i in range(NX // 2):
        put(wdx, ystage1, H1 + i, i, wd1[H1 + i, 0:NY])
    halo_send(*send_wd)

    halo_wait(*send_st)

    def start_state(i):
        value = st[i]
        x = px * NX + i - H
        near = beside(st, i, value, 1)
        in_x = (x > 0, x < GX - 1)
        diag = None
        for f in range(6):
            ok = in_x[f] if f < 2 else inner[f - 2]
            d = jnp.where(ok, 0.5 * (value - near[f]), value)
            cd[f, i] = jnp.where(ok, d, 0.0)
            diag = d if diag is None else diag + d
        sd[i] = diag
    loop(3, RX - 3, start_state, 10)


    def coarse_beside(values, d):
        v = values[d]
        zero = jnp.zeros_like(v)
        low = values[d - 1] if d > 0 else zero
        high = values[d + 1] if d < WIN - 1 else zero
        return (pltpu.roll(v, 1, 0), pltpu.roll(v, 7, 0),
                jnp.where(y_in > 0, pltpu.roll(v, 1, 1), pltpu.roll(low, NZ - 3, 1)),
                jnp.where(y_in < 3, pltpu.roll(v, NZ - 1, 1), pltpu.roll(high, 3, 1)),
                pltpu.roll(v, 4, 1), pltpu.roll(v, NZ - 4, 1))

    def coarse_couplings():
        values = [cond2[d] for d in range(WIN)]
        for d in range(WIN):
            place = py - REACH + d
            y = place * 4 + y_in
            inside = (row8 > 0, row8 < 7, y > 0, y < GY // 4 - 1, lane8 >= 4, lane8 < NZ - 4)
            diag = None
            for f, near in enumerate(coarse_beside(values, d)):
                a = 2.0 * (values[d] + jnp.where(inside[f], near, values[d]))
                ca2[f, d] = jnp.where(inside[f], a, 0.0)
                diag = a if diag is None else diag + a
            wd2[d] = jnp.where((place >= 0) & (place < PY), OMEGA / diag, 0.0)

    def coarse_solve():
        def sweep(values, low, high):
            out = list(values)
            for d in range(low, high):
                total = rhs2[d]
                for f, near in enumerate(coarse_beside(values, d)):
                    total = total + ca2[f, d] * near
                out[d] = (1.0 - OMEGA) * values[d] + wd2[d] * total
            return out
        values = sweep([wd2[d] * rhs2[d] for d in range(WIN)], 0, WIN)
        for s in range(2, COARSE_SWEEPS):
            values = sweep(values, 1, WIN - 1)
        for d in range(1, WIN - 1):
            sol[d] = values[d]
        cell = jnp.where(row < NY, row >> 2, jnp.where(row < NY + H, 0, 3))
        for i in range(4):
            x = 2 * px - 1 + i
            at = jnp.clip(x, 0, 7)
            own, high, low = (sol[d, pl.ds(at, 1), :] for d in (REACH, REACH + 1, REACH - 1))
            spread = jnp.where(row < NY, own, jnp.where(row < NY + H, high, low))
            spread = jnp.where((lane & 3) == cell, spread, 0.0)
            spread = spread + swap(spread, 1, 1)
            spread = spread + swap(spread, 2, 1)
            p2[i] = jnp.where((x >= 0) & (x < 8), spread, 0.0)

    def contribute(g, z, v, out):
        def restrict(i):
            parts = [(1.0 - OMEGA) * z[at] + coupled(ca, v, at, v[at], 1) for at in (2 * i, 2 * i + 1)
                     if H - out <= at < H + NX + out]
            total = block_sum(parts[0], parts[-1] if len(parts) > 1 else 0.0, 1)
            bp[i] = total
            v1p[i] = wd1[i] * total
        loop(1, RX1 - 1, restrict, RX1 - 2)

        def level1_residual(i):
            if i == 0:
                return ca1[0, 1] * v1p[1]
            if i == RX1 - 1:
                return ca1[1, RX1 - 2] * v1p[RX1 - 2]
            return (1.0 - OMEGA) * bp[i] + coupled(ca1, v1p, i, v1p[i], 2)
        for j, (q, at) in enumerate(((1, 1), (0, 0), (0, 1), (1, 0))):
            total = block_sum(level1_residual(2 * j), level1_residual(2 * j + 1), 2)
            chunk[g - 1, q, at:at + 1] = pick_chunk(total)
            ringed = pick_ring(total, q)
            if q == 0:
                chunk[g - 1, 2, at:at + 1] = ringed
            else:
                outer = ringed if j == 0 else jnp.concatenate([ringed, outer], axis=0)
        chunk[g - 1, 2] = chunk[g - 1, 2] + outer

    def solve(source, n, reach, finish, first, after=lambda: None):
        def presmooth(i):
            vv[i] = wd[i] * source[i]
        loop(H - 1 - reach, H + NX + 1 + reach, presmooth, NX + 2 + 2 * reach)
        if first:
            halo_wait(*send_wd)
        share_wait(n)
        if first:
            gather_cond()
            coarse_couplings()
        if n == 2:
            after()
        gather_rhs(n + 1)
        if n == 1:
            after()
        coarse_solve()
        if first:
            gather_end(0, 0)
            halo_done(*send_wd)
        gather_end(n + 1, 0)
        share_done(n)

        for i in range(RX1):
            v1[i] = v1[i] + p2[i // 2]

        def postsmooth1(i):
            v = v1[i]
            r1[i] = (1.0 - OMEGA) * v + wd1[i] * (b1[i] + coupled(ca1, v1, i, v, 2))
        loop(1, RX1 - 1, postsmooth1, 6)

        def correct(i):
            for j in range(2):
                vv[2 * i + j] = vv[2 * i + j] + r1[i]
        loop(1, RX1 - 1, correct)

        def postsmooth(i):
            v = vv[i]
            finish(i, (1.0 - OMEGA) * v + wd[i] * (source[i] + coupled(ca, vv, i, v, 1)))
        loop(H - reach, H + NX + reach, postsmooth, 10)

    def hessian(r, n, keep, during, after, arrive, between=lambda: None):
        def own_scaled(i):
            gp[i, 0:NY] = kk[i, 0:NY] * r[i, 0:NY]
        loop(H, H + NX, own_scaled, 8)

        def own_sensitivity(i):
            value = gp[i]
            z = sd[i] * value + coupled(cd, gp, i, value, 1)
            zp1[i] = z
            vp1[i] = wd[i] * z
        loop(H - 1, H + NX + 1, own_sensitivity, 10)
        contribute(2 * n + 1, zp1, vp1, 2)
        if n == 0:
            arrive()
            gather_send(0)
        gather_send(2 * n + 1)
        share_send(2 * n)
        if n != 0:
            arrive()

        def scaled(i):
            gg[i] = kk[i] * r[i]
        loop(2, RX - 2, scaled, 12)

        def sensitivity(i):
            value = gg[i]
            zz[i] = sd[i] * value + coupled(cd, gg, i, value, 1)
        loop(3, RX - 3, sensitivity, 10)

        second = z2.at[n]

        def weighted(i, value):
            wkeep[n, i - H] = value[0:NY]
            z = weight[i - H] * value[0:NY]
            put(second, ystage.at[4 + 2 * n], i, i - H, z)
            zp2[i, 0:NY] = z
            vp2[i, 0:NY] = wd[i, 0:NY] * z
        solve(zz, 2 * n, 0, weighted, n == 0, between)
        send_z2 = fine(second, 4 + 2 * n, 2, 1)
        halo_send(*send_z2)
        if n == 1:
            during()
        contribute(2 * n + 2, zp2, vp2, 1)
        gather_send(2 * n + 2)
        share_send(2 * n + 1)
        if n == 0:
            during()
        halo_wait(*send_z2)
        halo_done(*send_z2)

        def adjoint(i, value):
            pp[i] = value
        solve(second, 2 * n + 1, 1, adjoint, False, after)

        def assemble(i):
            p = pp[i]
            misfit = kk[i] * (sd[i] * p - coupled(cd, pp, i, p, 1))
            keep(i, misfit[0:NY] + prior_row(r, i))
        loop(H, H + NX, assemble, 8)

    def arrive_first():
        halo_wait(*send_src)
        halo_done(*send_prior, count=4)
        halo_done(*send_lk)
        halo_done(*send_st)

    zero = jnp.zeros((NY, NZ), F32)
    sums = {}

    def first_products():
        total = [zero, zero]
        for i in range(NX):
            r, w = src[i + H, 0:NY], wkeep[0, i]
            total[0] = total[0] + r * r
            total[1] = total[1] + weight[i] * w * w + r * prior_row(src, i + H)
        dot_prepare(0, (total[0], total[1], zero))

    def keep_first(i, value):
        put(c0, ystage.at[5], i, i - H, value)
    hessian(src, 0, keep_first, first_products, lambda: dot_send(0), arrive_first)
    halo_done(*send_src)
    send_c0 = fine(c0, 5, 2, 3)
    halo_send(*send_c0)

    def arrive_second():
        halo_wait(*send_c0)
        halo_done(*send_c0)

    def second_start():
        rr, rc = dot_wait(0)[:2]
        alpha = rr / rc
        sums.update(rr=rr, rc=rc, alpha=alpha)
        for i in range(H - 1, H + NX + 1):
            r1f[i] = src[i] - alpha * c0[i]
        total = [zero, zero, zero]
        for i in range(NX):
            r = r1f[i + H, 0:NY]
            total[0] = total[0] + r * r
            total[1] = total[1] + r * prior_row(r1f, i + H)
            total[2] = total[2] + r * c0[i + H, 0:NY]
        for j in range(3):
            partial[j] = total[j]

    def second_products():
        weighted = zero
        for i in range(NX):
            w = wkeep[0, i] - sums["alpha"] * wkeep[1, i]
            weighted = weighted + weight[i] * w * w
        dot_prepare(1, (partial[0], partial[1] + weighted, partial[2]))
        dot_send(1)

    def keep_second(i, value):
        kc[i - H] = value
    hessian(c0, 1, keep_second, second_products, lambda: None, arrive_second, second_start)

    norm, product, cross = dot_wait(1)
    alpha = sums["alpha"]
    ratio = norm / sums["rr"]
    beta = norm / (product + 2.0 * ratio * cross + ratio * ratio * sums["rc"])

    def finish(i):
        r, c, later = src[i + H, 0:NY], c0[i + H, 0:NY], r1f[i + H, 0:NY]
        curved = c - alpha * kc[i]
        step_ref[i] = alpha * r + beta * (later + ratio * r)
        resid_ref[i] = later - beta * (curved + ratio * c)
    loop(0, NX, finish)


def scratch():
    vmem = lambda *shape: pltpu.VMEM(shape, F32)
    fine = lambda *lead: vmem(*lead, RX, ROWS, NZ)
    level1 = lambda *lead: vmem(*lead, RX1, ROWS, NZ)
    dma = pltpu.SemaphoreType.DMA
    return [
        fine(), fine(), fine(), fine(), fine(), fine(2), level1(),
        vmem(7, 2, NX, H, NZ), vmem(7, 2, RX, H, NZ), vmem(2, NX // 2, H, NZ), vmem(2, RX1, H, NZ),
        vmem(NX, NY, NZ), pltpu.VMEM((1, SENSORS), jnp.int32), vmem(1, SENSORS), fine(), vmem(2, NX, NY, NZ), vmem(3, NY, NZ),
        fine(), fine(6), fine(), fine(6), fine(), fine(), fine(), fine(), vmem(1, 8, 128), fine(),
        level1(), level1(6), level1(), level1(), level1(), level1(), vmem(4, ROWS, NZ),
        fine(), fine(), fine(), fine(), fine(), level1(), level1(),
        vmem(4, 2, ROWS, NZ), vmem(4, 2, 2, 8, NZ), vmem(4, 2, ROWS, NZ), vmem(4, 2, 2, 8, NZ), vmem(4, 2, 2, 8, NZ),
        vmem(WIN, PX, 2, NZ), vmem(4, WIN, PX, PIECES, 2, NZ), vmem(2, NZ), vmem(4, PIECES, 2, NZ), vmem(WIN, 8, NZ), vmem(6, WIN, 8, NZ), vmem(WIN, 8, NZ),
        vmem(WIN, 8, NZ), vmem(WIN, 8, NZ), vmem(NX, NY, NZ), vmem(NX, NY, NZ),
        vmem(2, PX * PY, 3, 128), vmem(2, 3, 128),
        dma((5, 8)), dma((5, 8)), dma((2, WIN)), dma((3, WIN)), dma((1,)), dma((2,)), dma((6,)),
    ]


def on_device(log_conductivity, state, gradient, prior_sample, sensor_cells, noise_precision):
    block = jax.ShapeDtypeStruct(log_conductivity.shape, F32)
    vmem = pl.BlockSpec(memory_space=pltpu.VMEM)
    return pl.pallas_call(
        kernel,
        out_shape=(block, block),
        in_specs=[pl.BlockSpec(memory_space=pltpu.HBM)] * 6,
        out_specs=(vmem, vmem),
        scratch_shapes=scratch(),
        compiler_params=pltpu.CompilerParams(
            collective_id=0, has_side_effects=True, vmem_limit_bytes=24 * 1024 * 1024),
    )(*(pltpu.with_memory_space_constraint(x, pltpu.HBM) for x in (
        log_conductivity, state, gradient, prior_sample,
        sensor_cells.reshape(1, SENSORS), noise_precision.reshape(1, SENSORS))))


def solution(mesh):
    field, sensors = P(("ens", "gx"), "gy", None), P(("ens", "gx", "gy"))
    return jax.shard_map(
        on_device,
        mesh=mesh,
        in_specs=(field, field, field, field, sensors, sensors),
        out_specs=(field, field),
        check_vma=False,
    )
```

```python
import jax
import jax.numpy as jnp
from jax import lax
from jax.experimental import pallas as pl
from jax.experimental.pallas import tpu as pltpu
from jax.sharding import PartitionSpec as P

MESH = pl.DeviceIdType.MESH
F32 = jnp.float32

NX, NY, NZ = 8, 16, 256
H, H1 = 4, 2
RX, RX1 = NX + 2 * H, NX // 2 + 2 * H1
ROWS = NY + 2 * H
PX, PY = 4, 8
GX, GY = NX * PX, NY * PY
REACH = 2
WIN = 2 * REACH + 1
COARSE_SWEEPS = 6
PIECES = 3
SENSORS = 512
OMEGA = 0.8
DIRS = ((1, 0), (-1, 0), (0, 1), (0, -1), (1, 1), (1, -1), (-1, 1), (-1, -1))
UNROLL = 2


def kernel(logk_ref, state_ref, grad_ref, prior_ref, cells_ref, prec_ref,
           step_ref, resid_ref,
           lk, st, pr, src, c0, z2, wdx, ystage, yrecv, ystage1, yrecv1, grad, cells_in, prec_in, r1f, wkeep, partial,
           kk, ca, wd, cd, sd, gg, zz, vv, cp, pp,
           c1, ca1, wd1, b1, v1, p2,
           gp, zp1, vp1, zp2, vp2, bp, v1p, xp, yp, xr, yr2, cr, gat0, gat, chunk0, chunk, cond2, ca2, wd2, rhs2, sol, weight, kc, dots, dchunk,
           h_send, h_recv, g_send, g_recv, d_send, d_recv, in_sem):
    px = lax.axis_index("gx")
    py = lax.axis_index("gy")
    row = lax.broadcasted_iota(jnp.int32, (ROWS, NZ), 0)
    lane = lax.broadcasted_iota(jnp.int32, (ROWS, NZ), 1)
    row8 = lax.broadcasted_iota(jnp.int32, (8, NZ), 0)
    lane8 = lax.broadcasted_iota(jnp.int32, (8, NZ), 1)
    y_in = lane8 & 3
    y_at = py * NY + jnp.where(row < NY + H, row, row - ROWS)

    def loop(low, high, body, unroll=UNROLL):
        whole = (high - low) // unroll

        def step(k, carry):
            for j in range(unroll):
                body(low + k * unroll + j)
            return carry
        if whole > 1:
            lax.fori_loop(0, whole, step, 0)
        for i in range(low + whole * unroll if whole > 1 else low, high):
            body(i)

    def exists(dx, dy):
        return (px + dx >= 0) & (px + dx < PX) & (py + dy >= 0) & (py + dy < PY)

    def halo_copy(field, ys, yr, n, h, wx, k, send, recv, reverse):
        dx, dy = DIRS[k]
        if dy == 0:
            source = field.at[h + n - wx:h + n, 0:NY] if dx == 1 else field.at[h:h + wx, 0:NY]
            target = field.at[h - wx:h, 0:NY] if dx == 1 else field.at[h + n:h + n + wx, 0:NY]
        else:
            side = 1 if dy == 1 else 0
            if dx == 0:
                source, target = ys.at[side], yr.at[side, h:h + n]
            elif dx == 1:
                source, target = ys.at[side, n - wx:n], yr.at[side, h - wx:h]
            else:
                source, target = ys.at[side, 0:wx], yr.at[side, h + n:h + n + wx]
        if reverse:
            dx, dy = -dx, -dy
        return pltpu.make_async_remote_copy(
            src_ref=source, dst_ref=target, send_sem=send.at[k], recv_sem=recv.at[k],
            device_id={"gx": px + dx, "gy": py + dy}, device_id_type=MESH)

    def halo_clear(field, yr, n, h):
        @pl.when(px == 0)
        def _():
            field[0:h, 0:NY] = jnp.zeros((h, NY, NZ), F32)
            yr[:, 0:h] = jnp.zeros((2, h, H, NZ), F32)

        @pl.when(px == PX - 1)
        def _():
            field[h + n:, 0:NY] = jnp.zeros((h, NY, NZ), F32)
            yr[:, h + n:] = jnp.zeros((2, h, H, NZ), F32)

        @pl.when(py == 0)
        def _():
            yr[1] = jnp.zeros((n + 2 * h, H, NZ), F32)

        @pl.when(py == PY - 1)
        def _():
            yr[0] = jnp.zeros((n + 2 * h, H, NZ), F32)

    def put(field, ys, i, j, value):
        field[i, 0:NY] = value
        ys[0, j] = value[0:H]
        ys[1, j] = value[NY - H:NY]

    def halo_send(field, ys, yr, n, h, wx, send, recv, count=8, first=0):
        for k in reversed(range(first, count)):
            @pl.when(exists(*DIRS[k]))
            def _(k=k):
                halo_copy(field, ys, yr, n, h, wx, k, send, recv, False).start()

    def halo_wait(field, ys, yr, n, h, wx, send, recv, count=8):
        for k in range(count):
            @pl.when(exists(-DIRS[k][0], -DIRS[k][1]))
            def _(k=k):
                halo_copy(field, ys, yr, n, h, wx, k, send, recv, True).wait_recv()

        def place(i):
            field[i, NY:ROWS] = jnp.concatenate([yr[0, i], yr[1, i]], axis=0)
        loop(h - wx, n + h + wx, place, 4)

    def halo_done(field, ys, yr, n, h, wx, send, recv, count=8):
        for k in range(count):
            @pl.when(exists(*DIRS[k]))
            def _(k=k):
                halo_copy(field, ys, yr, n, h, wx, k, send, recv, False).wait_send()

    def fine(field, slot, wx, sems):
        return (field, ystage.at[slot], yrecv.at[slot], NX, H, wx, h_send.at[sems % 3], h_recv.at[sems])

    send_wd = (wdx, ystage1, yrecv1, NX // 2, H1, H1, h_send.at[1], h_recv.at[4])

    def pack(first, second, third):
        r = lax.broadcasted_iota(jnp.int32, first.shape, 0) & 1
        l = lax.broadcasted_iota(jnp.int32, first.shape, 1) & 1
        return jnp.where(r == 0, jnp.where(l == 0, first, second), third)

    def unpack(packed):
        n = packed.shape[0]
        r = lax.broadcasted_iota(jnp.int32, packed.shape, 0) & 1
        l = lax.broadcasted_iota(jnp.int32, packed.shape, 1) & 1
        even = jnp.where(r == 0, packed, pltpu.roll(packed, 1, 0))
        return (jnp.where(l == 0, even, pltpu.roll(even, 1, 1)), jnp.where(l == 1, even, pltpu.roll(even, NZ - 1, 1)),
                jnp.where(r == 1, packed, pltpu.roll(packed, n - 1, 0)))

    def share_copy(n, k, reverse):
        dx, dy = DIRS[k]
        side_x, side_y = int(dx == 1), int(dy == 1)
        if dy == 0:
            source, target = xp.at[n, side_x], xr.at[n, 1 - side_x]
        elif dx == 0:
            source, target = yp.at[n, side_y], yr2.at[n, 1 - side_y]
        else:
            source, target = yp.at[n, side_y, side_x], cr.at[n, 1 - side_x, 1 - side_y]
        if reverse:
            dx, dy = -dx, -dy
        sems = 2 * (n % 2)
        return pltpu.make_async_remote_copy(
            src_ref=source, dst_ref=target, send_sem=h_send.at[sems, k], recv_sem=h_recv.at[sems, k],
            device_id={"gx": px + dx, "gy": py + dy}, device_id_type=MESH)

    def share_clear():
        for at, edge in ((0, 0), (1, PX - 1)):
            @pl.when(px == edge)
            def _(at=at):
                for n in range(4):
                    xr[n, at] = jnp.zeros((ROWS, NZ), F32)
                    cr[n, at] = jnp.zeros((2, 8, NZ), F32)
        for at, edge in ((0, 0), (1, PY - 1)):
            @pl.when(py == edge)
            def _(at=at):
                for n in range(4):
                    yr2[n, at] = jnp.zeros((2, 8, NZ), F32)
                    for x in range(2):
                        cr[n, x, at] = jnp.zeros((8, NZ), F32)

    def share_send(n):
        for half in range(2):
            layers = [bp[1 + 3 * half + j] for j in range(3)]
            xp[n, half] = pack(*layers)
            yp[n, 1, half] = pack(*(jnp.where(row8 >= 4, v[8:16], v[16:24]) for v in layers))
            yp[n, 0, half] = pack(*(jnp.where(row8 >= 4, v[16:24], v[0:8]) for v in layers))
        for k in reversed(range(8)):
            @pl.when(exists(*DIRS[k]))
            def _(k=k):
                share_copy(n, k, False).start()

    def share_wait(n):
        for k in range(8):
            @pl.when(exists(-DIRS[k][0], -DIRS[k][1]))
            def _(k=k):
                share_copy(n, k, True).wait_recv()
        zero = jnp.zeros((8, NZ), F32)

        def placed(v, side):
            upper, lower = jnp.where(row8 >= 4, v, 0.0), jnp.where(row8 < 4, v, 0.0)
            return jnp.concatenate([lower, zero, upper] if side == 0 else [zero, upper, lower], axis=0)
        total = [bp[i] if 0 < i < RX1 - 1 else None for i in range(RX1)]

        def add(i, v):
            total[i] = v if total[i] is None else total[i] + v
        for half, start in ((0, 1), (1, 4)):
            for side in range(2):
                for j, v in enumerate(unpack(yr2[n, side, half])):
                    add(start + j, placed(v, side))
        for side_x, start in ((0, 0), (1, 5)):
            for j, v in enumerate(unpack(xr[n, side_x])):
                add(start + j, v)
            for side_y in range(2):
                for j, v in enumerate(unpack(cr[n, side_x, side_y])):
                    add(start + j, placed(v, side_y))
        for i in range(RX1):
            b1[i] = total[i]
            v1[i] = wdx[i] * total[i]

    def share_done(n):
        for k in range(8):
            @pl.when(exists(*DIRS[k]))
            def _(k=k):
                share_copy(n, k, False).wait_send()

    PEERS = [(dx, dy) for dy in (2, -2, 1, -1, 0) for dx in (2, 1, 3, 0) if (dx, dy) != (0, 0)]

    REACHED = (0, 1, -1, 2, -2)

    def buffers(g):
        return (chunk0, gat0) if g == 0 else (chunk.at[g - 1], gat.at[g - 1])

    def sems(g):
        return (g_send.at[0], g_recv.at[0]) if g == 0 else (g_send.at[1], g_recv.at[1 + (g - 1) % 2])

    def gather_send(g, which="all"):
        mine, all_ = buffers(g)
        sent, arrived = sems(g)
        for dx, dy in PEERS:
            there = (py + dy >= 0) & (py + dy < PY)
            if which != "all":
                apart = px == {3: 0, 1: PX - 1}.get(dx, -1)
                there = there & (apart if which == "apart" else jnp.logical_not(apart))

            @pl.when(there)
            def _(dx=dx, dy=dy):
                pltpu.make_async_remote_copy(
                    src_ref=mine, dst_ref=all_.at[REACH - dy, px],
                    send_sem=sent.at[REACH + dy], recv_sem=arrived.at[REACH - dy],
                    device_id={"gx": lax.rem(px + dx, PX), "gy": py + dy}, device_id_type=MESH).start()
        if which != "apart":
            all_[REACH, px] = mine[...]

    def gather_end(g, which):
        all_ = buffers(g)[1]
        for dy in REACHED:
            @pl.when((py + dy >= 0) & (py + dy < PY))
            def _(dy=dy):
                row_ = all_.at[REACH + dy, 0:PX - 1] if dy == 0 else all_.at[REACH + dy]
                pltpu.make_async_copy(row_, row_, sems(g)[which].at[REACH + dy]).wait()

    def valid(d):
        return (py - REACH + d >= 0) & (py - REACH + d < PY)

    def gather_cond():
        gather_end(0, 1)
        for d in range(WIN):
            whole = jnp.concatenate([gat0[d, p] for p in range(PX)], axis=0)
            cond2[d] = jnp.where(valid(d), whole, 0.0)

    def along_x(piece):
        moved = jnp.where((row8 & 1) == 0, pltpu.roll(piece, 2, 0), pltpu.roll(piece, 6, 0))
        return jnp.where((row8 > 0) & (row8 < 7), moved, 0.0)

    def gather_rhs(g):
        gather_end(g, 1)
        own, ring = [], []
        for d in range(WIN):
            piece = [jnp.concatenate([gat[g - 1, d, p, q] for p in range(PX)], axis=0) for q in range(PIECES)]
            corner = along_x(piece[2])
            corner = jnp.where(y_in == 0, pltpu.roll(corner, NZ - 1, 1), pltpu.roll(corner, 1, 1))
            own.append(jnp.where(valid(d), piece[0] + along_x(piece[1]), 0.0))
            ring.append(jnp.where(valid(d), piece[2] + corner, 0.0))
        zero8 = jnp.zeros((8, NZ), F32)
        for d in range(WIN):
            low = ring[d - 1] if d > 0 else zero8
            high = ring[d + 1] if d < WIN - 1 else zero8
            rhs2[d] = own[d] + jnp.where(y_in == 0, low, jnp.where(y_in == 3, high, 0.0))

    OTHERS = [(dx, dy) for dy in (4, 3, 5, 2, 6, 1, 7, 0) for dx in (2, 1, 3, 0) if (dx, dy) != (0, 0)]

    def dot_prepare(g, values):
        folded = [jnp.sum(v[:, 0:NZ // 2] + v[:, NZ // 2:NZ], axis=0, keepdims=True) for v in values]
        part = jnp.concatenate(folded, axis=0)
        dchunk[g] = part
        dots[g, px * PY + py] = part

    def dot_send(g):
        for dx, dy in OTHERS:
            pltpu.make_async_remote_copy(
                src_ref=dchunk.at[g], dst_ref=dots.at[g, px * PY + py], send_sem=d_send.at[0], recv_sem=d_recv.at[g],
                device_id={"gx": lax.rem(px + dx, PX), "gy": lax.rem(py + dy, PY)}, device_id_type=MESH).start()

    def dot_wait(g):
        others = dots.at[g, 0:PX * PY - 1]
        pltpu.make_async_copy(others, others, d_recv.at[g]).wait()
        total = dots[g, 0]
        for slot in range(1, PX * PY):
            total = total + dots[g, slot]
        pltpu.make_async_copy(others, others, d_send.at[0]).wait()
        return [jnp.sum(total[i:i + 1], axis=1, keepdims=True) for i in range(total.shape[0])]

    def beside(field, i, value, s):
        return (field[i - 1], field[i + 1], pltpu.roll(value, s, 0), pltpu.roll(value, ROWS - s, 0),
                pltpu.roll(value, s, 1), pltpu.roll(value, NZ - s, 1))

    def coupled(coefs, field, i, value, s):
        near = beside(field, i, value, s)
        total = coefs[0, i] * near[0]
        for f in range(1, 6):
            total = total + coefs[f, i] * near[f]
        return total

    def prior_row(field, i):
        value = field[i]
        near = beside(field, i, value, 1)
        away = near[0] + near[1] + near[2] + near[3]
        away = away + jnp.where(lane >= 1, near[4], 0.0) + jnp.where(lane < NZ - 1, near[5], 0.0)
        return (6.5 * value - away)[0:NY]

    def swap(value, s, axis):
        index, size = (row, ROWS) if axis == 0 else (lane, NZ)
        return jnp.where((index & s) == 0, pltpu.roll(value, size - s, axis), pltpu.roll(value, s, axis))

    def block_sum(low, high, s):
        total = low + high
        total = total + swap(total, s, 1)
        return total + swap(total, s, 0)

    def pick_chunk(value):
        mine = ((row & 3) == 0) & ((row >> 2) == (lane & 3)) & (row < NY)
        return jnp.sum(jnp.where(mine, value, 0.0), axis=0, keepdims=True)

    def pick_ring(value, at):
        mine = ((row == NY) & ((lane & 3) == at)) | ((row == NY + H) & ((lane & 3) == 3 - at))
        return jnp.sum(jnp.where(mine, value, 0.0), axis=0, keepdims=True)

    def inside_yz(s):
        return (y_at >= s, y_at < GY - s, lane >= s, lane < NZ - s)

    def cell_inside(x):
        return jnp.where((x >= 0) & (x < PX * NX), ((y_at >= 0) & (y_at < GY)).astype(F32), 0.0) > 0.5

    own = lambda field: field.at[H:H + NX, 0:NY]
    loads = [pltpu.make_async_copy(source, target, in_sem.at[k]) for k, (source, target) in enumerate((
        (prior_ref, own(pr)), (logk_ref, own(lk)), (state_ref, own(st)), (cells_ref, cells_in), (prec_ref, prec_in),
        (grad_ref, grad)))]
    for load in loads:
        load.start()
    barrier = pltpu.get_barrier_semaphore()
    for k in range(8):
        @pl.when(exists(*DIRS[k]))
        def _(k=k):
            pl.semaphore_signal(barrier, inc=1, device_id={"gx": px + DIRS[k][0], "gy": py + DIRS[k][1]},
                                device_id_type=MESH)
    fields = [(lk, 0), (st, 1), (pr, 2), (src, 3), (z2.at[0], 4), (c0, 5), (z2.at[1], 6)]
    for field, slot in fields:
        halo_clear(field, yrecv.at[slot], NX, H)
    halo_clear(wdx, yrecv1, NX // 2, H1)
    share_clear()
    for field in (gp, zp1, vp1, zp2, vp2):
        def clear(i, field=field):
            field[i] = jnp.zeros((ROWS, NZ), F32)
        loop(1, RX - 1, clear)
    for i in (0, RX1 - 1):
        v1p[i] = jnp.zeros((ROWS, NZ), F32)
    def edges(field, slot):
        for i in range(NX):
            ystage[slot, 0, i] = field[H + i, 0:H]
            ystage[slot, 1, i] = field[H + i, NY - H:NY]
    loads[0].wait()
    edges(pr, 2)
    loads[1].wait()
    edges(lk, 0)
    loads[2].wait()
    edges(st, 1)
    across = jnp.where(px > 0, 1, 0) + jnp.where(px < PX - 1, 1, 0)
    along = jnp.where(py > 0, 1, 0) + jnp.where(py < PY - 1, 1, 0)
    pl.semaphore_wait(barrier, (across + 1) * (along + 1) - 1)

    send_prior, send_lk, send_st = fine(pr, 2, 1, 0), fine(lk, 0, H, 1), fine(st, 1, 2, 2)
    halo_send(*send_prior, count=4)
    halo_send(*send_lk, first=4)
    halo_send(*send_st, first=4)
    halo_send(*send_lk, count=4)
    halo_send(*send_st, count=4)

    loads[3].wait()
    loads[4].wait()
    cells = cells_in[...]
    at_xy = ((cells >> 15) - px * NX) * NY + ((cells >> 8) & (GY - 1)) - py * NY
    at_z = cells & (NZ - 1)
    hot_xy = lax.broadcasted_iota(jnp.int32, (NX * NY, SENSORS), 0) == at_xy
    hot_z = (lax.broadcasted_iota(jnp.int32, (NZ, SENSORS), 0) == at_z).astype(F32).astype(jnp.bfloat16)
    left = jnp.where(hot_xy, prec_in[...], 0.0)
    total = jnp.zeros((NX * NY, NZ), F32)
    for part in range(3):
        piece = left.astype(jnp.bfloat16)
        left = left - piece.astype(F32)
        total = total + lax.dot_general(piece, hot_z, (((1,), (1,)), ((), ())), preferred_element_type=F32)
    for i in range(NX):
        weight[i] = total[i * NY:(i + 1) * NY]

    loads[5].wait()
    halo_wait(*send_prior, count=4)

    def start_source(i):
        put(src, ystage.at[3], i + H, i, prior_row(pr, i + H) - grad[i])
    loop(0, NX, start_source, 8)
    halo_done(*send_prior, count=4)
    send_src = fine(src, 3, 2, 3)
    halo_send(*send_src)

    halo_wait(*send_lk)

    def start_cond(i):
        kk[i] = jnp.exp(lk[i])
    loop(0, RX, start_cond, 8)

    inner = inside_yz(1)

    def start_couplings(i):
        value = kk[i]
        x = px * NX + i - H
        near = beside(kk, i, value, 1)
        in_x = (x > 0, x < GX - 1)
        diag = None
        for f in range(6):
            ok = in_x[f] if f < 2 else inner[f - 2]
            a = 0.5 * (value + jnp.where(ok, near[f], value))
            ca[f, i] = jnp.where(ok, a, 0.0)
            diag = a if diag is None else diag + a
        wd[i] = jnp.where(cell_inside(x), OMEGA / diag, 0.0)
    loop(2, RX - 2, start_couplings, 12)

    def start_level1(i):
        c1[i] = block_sum(kk[2 * i], kk[2 * i + 1], 1) * 0.125
    loop(0, RX1, start_level1, 8)

    for i in range(2):
        chunk0[i:i + 1] = pick_chunk(block_sum(c1[H1 + 2 * i], c1[H1 + 2 * i + 1], 2) * 0.125)

    gather_send(0, "near")

    inner1 = inside_yz(2)

    def start_couplings1(i):
        value = c1[i]
        x = px * NX + 2 * i - H
        near = beside(c1, i, value, 2)
        in_x = (x > 0, x < GX - 2)
        diag = None
        for f in range(6):
            ok = in_x[f] if f < 2 else inner1[f - 2]
            a = value + jnp.where(ok, near[f], value)
            ca1[f, i] = jnp.where(ok, a, 0.0)
            diag = a if diag is None else diag + a
        wd1[i] = jnp.where(cell_inside(x), OMEGA / diag, 0.0)
    loop(1, RX1 - 1, start_couplings1, 6)
    for i in range(NX // 2):
        put(wdx, ystage1, H1 + i, i, wd1[H1 + i, 0:NY])
    halo_done(*send_lk)
    halo_send(*send_wd)

    halo_wait(*send_st)

    def start_state(i):
        value = st[i]
        x = px * NX + i - H
        near = beside(st, i, value, 1)
        in_x = (x > 0, x < GX - 1)
        diag = None
        for f in range(6):
            ok = in_x[f] if f < 2 else inner[f - 2]
            d = jnp.where(ok, 0.5 * (value - near[f]), value)
            cd[f, i] = jnp.where(ok, d, 0.0)
            diag = d if diag is None else diag + d
        sd[i] = diag
    loop(3, RX - 3, start_state, 10)


    def coarse_beside(values, d):
        v = values[d]
        zero = jnp.zeros_like(v)
        low = values[d - 1] if d > 0 else zero
        high = values[d + 1] if d < WIN - 1 else zero
        return (pltpu.roll(v, 1, 0), pltpu.roll(v, 7, 0),
                jnp.where(y_in > 0, pltpu.roll(v, 1, 1), pltpu.roll(low, NZ - 3, 1)),
                jnp.where(y_in < 3, pltpu.roll(v, NZ - 1, 1), pltpu.roll(high, 3, 1)),
                pltpu.roll(v, 4, 1), pltpu.roll(v, NZ - 4, 1))

    def coarse_couplings():
        values = [cond2[d] for d in range(WIN)]
        for d in range(WIN):
            place = py - REACH + d
            y = place * 4 + y_in
            inside = (row8 > 0, row8 < 7, y > 0, y < GY // 4 - 1, lane8 >= 4, lane8 < NZ - 4)
            diag = None
            for f, near in enumerate(coarse_beside(values, d)):
                a = 2.0 * (values[d] + jnp.where(inside[f], near, values[d]))
                ca2[f, d] = jnp.where(inside[f], a, 0.0)
                diag = a if diag is None else diag + a
            wd2[d] = jnp.where((place >= 0) & (place < PY), OMEGA / diag, 0.0)

    def coarse_solve():
        def sweep(values, low, high):
            out = list(values)
            for d in range(low, high):
                total = rhs2[d]
                for f, near in enumerate(coarse_beside(values, d)):
                    total = total + ca2[f, d] * near
                out[d] = (1.0 - OMEGA) * values[d] + wd2[d] * total
            return out
        values = sweep([wd2[d] * rhs2[d] for d in range(WIN)], 0, WIN)
        for s in range(2, COARSE_SWEEPS):
            values = sweep(values, 1, WIN - 1)
        for d in range(1, WIN - 1):
            sol[d] = values[d]
        cell = jnp.where(row < NY, row >> 2, jnp.where(row < NY + H, 0, 3))
        for i in range(4):
            x = 2 * px - 1 + i
            at = jnp.clip(x, 0, 7)
            own, high, low = (sol[d, pl.ds(at, 1), :] for d in (REACH, REACH + 1, REACH - 1))
            spread = jnp.where(row < NY, own, jnp.where(row < NY + H, high, low))
            spread = jnp.where((lane & 3) == cell, spread, 0.0)
            spread = spread + swap(spread, 1, 1)
            spread = spread + swap(spread, 2, 1)
            p2[i] = jnp.where((x >= 0) & (x < 8), spread, 0.0)

    def contribute(g, z, v, out):
        def restrict(i):
            parts = [(1.0 - OMEGA) * z[at] + coupled(ca, v, at, v[at], 1) for at in (2 * i, 2 * i + 1)
                     if H - out <= at < H + NX + out]
            total = block_sum(parts[0], parts[-1] if len(parts) > 1 else 0.0, 1)
            bp[i] = total
            v1p[i] = wd1[i] * total
        loop(1, RX1 - 1, restrict, RX1 - 2)

        def level1_residual(i):
            if i == 0:
                return ca1[0, 1] * v1p[1]
            if i == RX1 - 1:
                return ca1[1, RX1 - 2] * v1p[RX1 - 2]
            return (1.0 - OMEGA) * bp[i] + coupled(ca1, v1p, i, v1p[i], 2)
        for j, (q, at) in enumerate(((1, 1), (0, 0), (0, 1), (1, 0))):
            total = block_sum(level1_residual(2 * j), level1_residual(2 * j + 1), 2)
            chunk[g - 1, q, at:at + 1] = pick_chunk(total)
            ringed = pick_ring(total, q)
            if q == 0:
                chunk[g - 1, 2, at:at + 1] = ringed
            else:
                outer = ringed if j == 0 else jnp.concatenate([ringed, outer], axis=0)
        chunk[g - 1, 2] = chunk[g - 1, 2] + outer

    def solve(source, n, reach, finish, first, after=lambda: None):
        def presmooth(i):
            vv[i] = wd[i] * source[i]
        loop(H - 1 - reach, H + NX + 1 + reach, presmooth, NX + 2 + 2 * reach)
        if first:
            halo_wait(*send_wd)
        share_wait(n)
        if first:
            gather_cond()
            coarse_couplings()
        if n == 2:
            after()
        gather_rhs(n + 1)
        if n == 1:
            after()
        coarse_solve()
        if first:
            gather_end(0, 0)
            halo_done(*send_wd)
        gather_end(n + 1, 0)
        share_done(n)

        for i in range(RX1):
            v1[i] = v1[i] + p2[i // 2]

        def postsmooth1(i):
            v = v1[i]
            better = (1.0 - OMEGA) * v + wd1[i] * (b1[i] + coupled(ca1, v1, i, v, 2))
            for j in range(2):
                if H - 1 - reach <= 2 * i + j < H + NX + 1 + reach:
                    vv[2 * i + j] = vv[2 * i + j] + better
        loop(1, RX1 - 1, postsmooth1, 6)

        def postsmooth(i):
            v = vv[i]
            finish(i, (1.0 - OMEGA) * v + wd[i] * (source[i] + coupled(ca, vv, i, v, 1)))
        loop(H - reach, H + NX + reach, postsmooth, 10)

    def hessian(r, n, keep, during, after, arrive, between=lambda: None):
        def own_scaled(i):
            gp[i, 0:NY] = kk[i, 0:NY] * r[i, 0:NY]
        loop(H, H + NX, own_scaled, 8)

        def own_sensitivity(i):
            value = gp[i]
            z = sd[i] * value + coupled(cd, gp, i, value, 1)
            zp1[i] = z
            vp1[i] = wd[i] * z
        loop(H - 1, H + NX + 1, own_sensitivity, 10)
        contribute(2 * n + 1, zp1, vp1, 2)
        if n == 0:
            arrive()
            gather_send(0, "apart")
        gather_send(2 * n + 1)
        share_send(2 * n)
        if n != 0:
            arrive()

        def scaled(i):
            gg[i] = kk[i] * r[i]
        loop(2, RX - 2, scaled, 12)

        def sensitivity(i):
            value = gg[i]
            zz[i] = sd[i] * value + coupled(cd, gg, i, value, 1)
        loop(3, RX - 3, sensitivity, 10)

        second = z2.at[n]

        def weighted(i, value):
            wkeep[n, i - H] = value[0:NY]
            z = weight[i - H] * value[0:NY]
            put(second, ystage.at[4 + 2 * n], i, i - H, z)
            zp2[i, 0:NY] = z
            vp2[i, 0:NY] = wd[i, 0:NY] * z
        solve(zz, 2 * n, 0, weighted, n == 0, between)
        send_z2 = fine(second, 4 + 2 * n, 2, 1)
        halo_send(*send_z2)
        if n == 1:
            during()
        contribute(2 * n + 2, zp2, vp2, 1)
        gather_send(2 * n + 2)
        share_send(2 * n + 1)
        if n == 0:
            during()
        halo_wait(*send_z2)
        halo_done(*send_z2)

        def adjoint(i, value):
            pp[i] = value
        solve(second, 2 * n + 1, 1, adjoint, False, after)

        def assemble(i):
            p = pp[i]
            misfit = kk[i] * (sd[i] * p - coupled(cd, pp, i, p, 1))
            keep(i, misfit[0:NY] + prior_row(r, i))
        loop(H, H + NX, assemble, 8)

    def arrive_first():
        halo_wait(*send_src)
        halo_done(*send_src)
        halo_done(*send_st)

    zero = jnp.zeros((NY, NZ), F32)
    sums = {}

    def first_products():
        total = [zero, zero]
        for i in range(NX):
            r, w = src[i + H, 0:NY], wkeep[0, i]
            total[0] = total[0] + r * r
            total[1] = total[1] + weight[i] * w * w + r * prior_row(src, i + H)
        dot_prepare(0, (total[0], total[1], zero))

    def keep_first(i, value):
        put(c0, ystage.at[5], i, i - H, value)
    hessian(src, 0, keep_first, first_products, lambda: dot_send(0), arrive_first)
    send_c0 = fine(c0, 5, 2, 3)
    halo_send(*send_c0)

    def arrive_second():
        halo_wait(*send_c0)
        halo_done(*send_c0)

    def second_start():
        rr, rc = dot_wait(0)[:2]
        alpha = rr / rc
        sums.update(rr=rr, rc=rc, alpha=alpha)
        for i in range(H - 1, H + NX + 1):
            r1f[i] = src[i] - alpha * c0[i]
        total = [zero, zero, zero]
        for i in range(NX):
            r = r1f[i + H, 0:NY]
            total[0] = total[0] + r * r
            total[1] = total[1] + r * prior_row(r1f, i + H)
            total[2] = total[2] + r * c0[i + H, 0:NY]
        for j in range(3):
            partial[j] = total[j]

    def second_products():
        weighted = zero
        for i in range(NX):
            w = wkeep[0, i] - sums["alpha"] * wkeep[1, i]
            weighted = weighted + weight[i] * w * w
        dot_prepare(1, (partial[0], partial[1] + weighted, partial[2]))
        dot_send(1)

    def keep_second(i, value):
        kc[i - H] = value
    hessian(c0, 1, keep_second, second_products, lambda: None, arrive_second, second_start)

    norm, product, cross = dot_wait(1)
    alpha = sums["alpha"]
    ratio = norm / sums["rr"]
    beta = norm / (product + 2.0 * ratio * cross + ratio * ratio * sums["rc"])

    def finish(i):
        r, c, later = src[i + H, 0:NY], c0[i + H, 0:NY], r1f[i + H, 0:NY]
        curved = c - alpha * kc[i]
        step_ref[i] = alpha * r + beta * (later + ratio * r)
        resid_ref[i] = later - beta * (curved + ratio * c)
    loop(0, NX, finish)


def scratch():
    vmem = lambda *shape: pltpu.VMEM(shape, F32)
    fine = lambda *lead: vmem(*lead, RX, ROWS, NZ)
    level1 = lambda *lead: vmem(*lead, RX1, ROWS, NZ)
    dma = pltpu.SemaphoreType.DMA
    return [
        fine(), fine(), fine(), fine(), fine(), fine(2), level1(),
        vmem(7, 2, NX, H, NZ), vmem(7, 2, RX, H, NZ), vmem(2, NX // 2, H, NZ), vmem(2, RX1, H, NZ),
        vmem(NX, NY, NZ), pltpu.VMEM((1, SENSORS), jnp.int32), vmem(1, SENSORS), fine(), vmem(2, NX, NY, NZ), vmem(3, NY, NZ),
        fine(), fine(6), fine(), fine(6), fine(), fine(), fine(), fine(), vmem(1, 8, 128), fine(),
        level1(), level1(6), level1(), level1(), level1(), vmem(4, ROWS, NZ),
        fine(), fine(), fine(), fine(), fine(), level1(), level1(),
        vmem(4, 2, ROWS, NZ), vmem(4, 2, 2, 8, NZ), vmem(4, 2, ROWS, NZ), vmem(4, 2, 2, 8, NZ), vmem(4, 2, 2, 8, NZ),
        vmem(WIN, PX, 2, NZ), vmem(4, WIN, PX, PIECES, 2, NZ), vmem(2, NZ), vmem(4, PIECES, 2, NZ), vmem(WIN, 8, NZ), vmem(6, WIN, 8, NZ), vmem(WIN, 8, NZ),
        vmem(WIN, 8, NZ), vmem(WIN, 8, NZ), vmem(NX, NY, NZ), vmem(NX, NY, NZ),
        vmem(2, PX * PY, 3, 128), vmem(2, 3, 128),
        dma((3, 8)), dma((5, 8)), dma((2, WIN)), dma((3, WIN)), dma((1,)), dma((2,)), dma((6,)),
    ]


def on_device(log_conductivity, state, gradient, prior_sample, sensor_cells, noise_precision):
    block = jax.ShapeDtypeStruct(log_conductivity.shape, F32)
    vmem = pl.BlockSpec(memory_space=pltpu.VMEM)
    return pl.pallas_call(
        kernel,
        out_shape=(block, block),
        in_specs=[pl.BlockSpec(memory_space=pltpu.HBM)] * 6,
        out_specs=(vmem, vmem),
        scratch_shapes=scratch(),
        compiler_params=pltpu.CompilerParams(
            collective_id=0, has_side_effects=True, vmem_limit_bytes=24 * 1024 * 1024),
    )(*(pltpu.with_memory_space_constraint(x, pltpu.HBM) for x in (
        log_conductivity, state, gradient, prior_sample,
        sensor_cells.reshape(1, SENSORS), noise_precision.reshape(1, SENSORS))))


def solution(mesh):
    field, sensors = P(("ens", "gx"), "gy", None), P(("ens", "gx", "gy"))
    return jax.shard_map(
        on_device,
        mesh=mesh,
        in_specs=(field, field, field, field, sensors, sensors),
        out_specs=(field, field),
        check_vma=False,
    )
```

```python
import jax
import jax.numpy as jnp
from jax import lax
from jax.experimental import pallas as pl
from jax.experimental.pallas import tpu as pltpu
from jax.sharding import PartitionSpec as P

MESH = pl.DeviceIdType.MESH
F32 = jnp.float32

NX, NY, NZ = 8, 16, 256
H, H1 = 4, 2
RX, RX1 = NX + 2 * H, NX // 2 + 2 * H1
ROWS = NY + 2 * H
PX, PY = 4, 8
GX, GY = NX * PX, NY * PY
REACH = 2
WIN = 2 * REACH + 1
COARSE_SWEEPS = 6
PIECES = 3
SENSORS = 512
OMEGA = 0.8
DIRS = ((1, 0), (-1, 0), (0, 1), (0, -1), (1, 1), (1, -1), (-1, 1), (-1, -1))
UNROLL = 2


def kernel(logk_ref, state_ref, grad_ref, prior_ref, cells_ref, prec_ref,
           step_ref, resid_ref,
           lk, st, pr, src, c0, z2, wdx, ystage, yrecv, ystage1, yrecv1, grad, cells_in, prec_in, r1f, wkeep, partial,
           kk, ca, wd, cd, sd, gg, zz, vv, cp, pp,
           c1, ca1, wd1, b1, v1, p2,
           gp, zp1, vp1, zp2, vp2, bp, v1p, xp, yp, xr, yr2, cr, gat0, gat, chunk0, chunk, cond2, ca2, wd2, rhs2, sol, weight, kc, dots, dchunk,
           h_send, h_recv, g_send, g_recv, d_send, d_recv, in_sem):
    px = lax.axis_index("gx")
    py = lax.axis_index("gy")
    row = lax.broadcasted_iota(jnp.int32, (ROWS, NZ), 0)
    lane = lax.broadcasted_iota(jnp.int32, (ROWS, NZ), 1)
    row8 = lax.broadcasted_iota(jnp.int32, (8, NZ), 0)
    lane8 = lax.broadcasted_iota(jnp.int32, (8, NZ), 1)
    y_in = lane8 & 3
    y_at = py * NY + jnp.where(row < NY + H, row, row - ROWS)

    def loop(low, high, body, unroll=UNROLL):
        whole = (high - low) // unroll

        def step(k, carry):
            for j in range(unroll):
                body(low + k * unroll + j)
            return carry
        if whole > 1:
            lax.fori_loop(0, whole, step, 0)
        for i in range(low + whole * unroll if whole > 1 else low, high):
            body(i)

    def exists(dx, dy):
        return (px + dx >= 0) & (px + dx < PX) & (py + dy >= 0) & (py + dy < PY)

    def halo_copy(field, ys, yr, n, h, wx, k, send, recv, reverse):
        dx, dy = DIRS[k]
        if dy == 0:
            source = field.at[h + n - wx:h + n, 0:NY] if dx == 1 else field.at[h:h + wx, 0:NY]
            target = field.at[h - wx:h, 0:NY] if dx == 1 else field.at[h + n:h + n + wx, 0:NY]
        else:
            side = 1 if dy == 1 else 0
            if dx == 0:
                source, target = ys.at[side], yr.at[side, h:h + n]
            elif dx == 1:
                source, target = ys.at[side, n - wx:n], yr.at[side, h - wx:h]
            else:
                source, target = ys.at[side, 0:wx], yr.at[side, h + n:h + n + wx]
        if reverse:
            dx, dy = -dx, -dy
        return pltpu.make_async_remote_copy(
            src_ref=source, dst_ref=target, send_sem=send.at[k], recv_sem=recv.at[k],
            device_id={"gx": px + dx, "gy": py + dy}, device_id_type=MESH)

    def halo_clear(field, yr, n, h):
        @pl.when(px == 0)
        def _():
            field[0:h, 0:NY] = jnp.zeros((h, NY, NZ), F32)
            yr[:, 0:h] = jnp.zeros((2, h, H, NZ), F32)

        @pl.when(px == PX - 1)
        def _():
            field[h + n:, 0:NY] = jnp.zeros((h, NY, NZ), F32)
            yr[:, h + n:] = jnp.zeros((2, h, H, NZ), F32)

        @pl.when(py == 0)
        def _():
            yr[1] = jnp.zeros((n + 2 * h, H, NZ), F32)

        @pl.when(py == PY - 1)
        def _():
            yr[0] = jnp.zeros((n + 2 * h, H, NZ), F32)

    def put(field, ys, i, j, value):
        field[i, 0:NY] = value
        ys[0, j] = value[0:H]
        ys[1, j] = value[NY - H:NY]

    def halo_send(field, ys, yr, n, h, wx, send, recv, count=8, first=0):
        for k in reversed(range(first, count)):
            @pl.when(exists(*DIRS[k]))
            def _(k=k):
                halo_copy(field, ys, yr, n, h, wx, k, send, recv, False).start()

    def halo_wait(field, ys, yr, n, h, wx, send, recv, count=8):
        for k in range(count):
            @pl.when(exists(-DIRS[k][0], -DIRS[k][1]))
            def _(k=k):
                halo_copy(field, ys, yr, n, h, wx, k, send, recv, True).wait_recv()

        def place(i):
            field[i, NY:ROWS] = jnp.concatenate([yr[0, i], yr[1, i]], axis=0)
        loop(h - wx, n + h + wx, place, 4)

    def halo_done(field, ys, yr, n, h, wx, send, recv, count=8):
        for k in range(count):
            @pl.when(exists(*DIRS[k]))
            def _(k=k):
                halo_copy(field, ys, yr, n, h, wx, k, send, recv, False).wait_send()

    def fine(field, slot, wx, sems):
        return (field, ystage.at[slot], yrecv.at[slot], NX, H, wx, h_send.at[sems % 3], h_recv.at[sems])

    send_wd = (wdx, ystage1, yrecv1, NX // 2, H1, H1, h_send.at[1], h_recv.at[4])

    def pack(first, second, third):
        r = lax.broadcasted_iota(jnp.int32, first.shape, 0) & 1
        l = lax.broadcasted_iota(jnp.int32, first.shape, 1) & 1
        return jnp.where(r == 0, jnp.where(l == 0, first, second), third)

    def unpack(packed):
        n = packed.shape[0]
        r = lax.broadcasted_iota(jnp.int32, packed.shape, 0) & 1
        l = lax.broadcasted_iota(jnp.int32, packed.shape, 1) & 1
        even = jnp.where(r == 0, packed, pltpu.roll(packed, 1, 0))
        return (jnp.where(l == 0, even, pltpu.roll(even, 1, 1)), jnp.where(l == 1, even, pltpu.roll(even, NZ - 1, 1)),
                jnp.where(r == 1, packed, pltpu.roll(packed, n - 1, 0)))

    def share_copy(n, k, reverse):
        dx, dy = DIRS[k]
        side_x, side_y = int(dx == 1), int(dy == 1)
        if dy == 0:
            source, target = xp.at[n, side_x], xr.at[n, 1 - side_x]
        elif dx == 0:
            source, target = yp.at[n, side_y], yr2.at[n, 1 - side_y]
        else:
            source, target = yp.at[n, side_y, side_x], cr.at[n, 1 - side_x, 1 - side_y]
        if reverse:
            dx, dy = -dx, -dy
        sems = 2 * (n % 2)
        return pltpu.make_async_remote_copy(
            src_ref=source, dst_ref=target, send_sem=h_send.at[sems, k], recv_sem=h_recv.at[sems, k],
            device_id={"gx": px + dx, "gy": py + dy}, device_id_type=MESH)

    def share_clear():
        for at, edge in ((0, 0), (1, PX - 1)):
            @pl.when(px == edge)
            def _(at=at):
                for n in range(4):
                    xr[n, at] = jnp.zeros((ROWS, NZ), F32)
                    cr[n, at] = jnp.zeros((2, 8, NZ), F32)
        for at, edge in ((0, 0), (1, PY - 1)):
            @pl.when(py == edge)
            def _(at=at):
                for n in range(4):
                    yr2[n, at] = jnp.zeros((2, 8, NZ), F32)
                    for x in range(2):
                        cr[n, x, at] = jnp.zeros((8, NZ), F32)

    def share_send(n):
        for half in range(2):
            layers = [bp[1 + 3 * half + j] for j in range(3)]
            xp[n, half] = pack(*layers)
            yp[n, 1, half] = pack(*(jnp.where(row8 >= 4, v[8:16], v[16:24]) for v in layers))
            yp[n, 0, half] = pack(*(jnp.where(row8 >= 4, v[16:24], v[0:8]) for v in layers))
        for k in reversed(range(8)):
            @pl.when(exists(*DIRS[k]))
            def _(k=k):
                share_copy(n, k, False).start()

    def share_wait(n):
        for k in range(8):
            @pl.when(exists(-DIRS[k][0], -DIRS[k][1]))
            def _(k=k):
                share_copy(n, k, True).wait_recv()
        zero = jnp.zeros((8, NZ), F32)

        def placed(v, side):
            upper, lower = jnp.where(row8 >= 4, v, 0.0), jnp.where(row8 < 4, v, 0.0)
            return jnp.concatenate([lower, zero, upper] if side == 0 else [zero, upper, lower], axis=0)
        total = [bp[i] if 0 < i < RX1 - 1 else None for i in range(RX1)]

        def add(i, v):
            total[i] = v if total[i] is None else total[i] + v
        for half, start in ((0, 1), (1, 4)):
            for side in range(2):
                for j, v in enumerate(unpack(yr2[n, side, half])):
                    add(start + j, placed(v, side))
        for side_x, start in ((0, 0), (1, 5)):
            for j, v in enumerate(unpack(xr[n, side_x])):
                add(start + j, v)
            for side_y in range(2):
                for j, v in enumerate(unpack(cr[n, side_x, side_y])):
                    add(start + j, placed(v, side_y))
        for i in range(RX1):
            b1[i] = total[i]
            v1[i] = wdx[i] * total[i]

    def share_done(n):
        for k in range(8):
            @pl.when(exists(*DIRS[k]))
            def _(k=k):
                share_copy(n, k, False).wait_send()

    PEERS = [(dx, dy) for dy in (2, -2, 1, -1, 0) for dx in (2, 1, 3, 0) if (dx, dy) != (0, 0)]

    REACHED = (0, 1, -1, 2, -2)

    def buffers(g):
        return (chunk0, gat0) if g == 0 else (chunk.at[g - 1], gat.at[g - 1])

    def sems(g):
        return (g_send.at[0], g_recv.at[0]) if g == 0 else (g_send.at[1], g_recv.at[1 + (g - 1) % 2])

    def gather_send(g, which="all"):
        mine, all_ = buffers(g)
        sent, arrived = sems(g)
        for dx, dy in PEERS:
            there = (py + dy >= 0) & (py + dy < PY)
            if which != "all":
                apart = px == {3: 0, 1: PX - 1}.get(dx, -1)
                there = there & (apart if which == "apart" else jnp.logical_not(apart))

            @pl.when(there)
            def _(dx=dx, dy=dy):
                pltpu.make_async_remote_copy(
                    src_ref=mine, dst_ref=all_.at[REACH - dy, px],
                    send_sem=sent.at[REACH + dy], recv_sem=arrived.at[REACH - dy],
                    device_id={"gx": lax.rem(px + dx, PX), "gy": py + dy}, device_id_type=MESH).start()
        if which != "apart":
            all_[REACH, px] = mine[...]

    def gather_end(g, which):
        all_ = buffers(g)[1]
        for dy in REACHED:
            @pl.when((py + dy >= 0) & (py + dy < PY))
            def _(dy=dy):
                row_ = all_.at[REACH + dy, 0:PX - 1] if dy == 0 else all_.at[REACH + dy]
                pltpu.make_async_copy(row_, row_, sems(g)[which].at[REACH + dy]).wait()

    def valid(d):
        return (py - REACH + d >= 0) & (py - REACH + d < PY)

    def gather_cond():
        gather_end(0, 1)
        for d in range(WIN):
            whole = jnp.concatenate([gat0[d, p] for p in range(PX)], axis=0)
            cond2[d] = jnp.where(valid(d), whole, 0.0)

    def along_x(piece):
        moved = jnp.where((row8 & 1) == 0, pltpu.roll(piece, 2, 0), pltpu.roll(piece, 6, 0))
        return jnp.where((row8 > 0) & (row8 < 7), moved, 0.0)

    def gather_rhs(g):
        gather_end(g, 1)
        own, ring = [], []
        for d in range(WIN):
            piece = [jnp.concatenate([gat[g - 1, d, p, q] for p in range(PX)], axis=0) for q in range(PIECES)]
            corner = along_x(piece[2])
            corner = jnp.where(y_in == 0, pltpu.roll(corner, NZ - 1, 1), pltpu.roll(corner, 1, 1))
            own.append(jnp.where(valid(d), piece[0] + along_x(piece[1]), 0.0))
            ring.append(jnp.where(valid(d), piece[2] + corner, 0.0))
        zero8 = jnp.zeros((8, NZ), F32)
        for d in range(WIN):
            low = ring[d - 1] if d > 0 else zero8
            high = ring[d + 1] if d < WIN - 1 else zero8
            rhs2[d] = own[d] + jnp.where(y_in == 0, low, jnp.where(y_in == 3, high, 0.0))

    OTHERS = [(dx, dy) for dy in (4, 3, 5, 2, 6, 1, 7, 0) for dx in (2, 1, 3, 0) if (dx, dy) != (0, 0)]

    def dot_prepare(g, values):
        folded = [jnp.sum(v[:, 0:NZ // 2] + v[:, NZ // 2:NZ], axis=0, keepdims=True) for v in values]
        part = jnp.concatenate(folded, axis=0)
        dchunk[g] = part
        dots[g, px * PY + py] = part

    def dot_send(g):
        for dx, dy in OTHERS:
            pltpu.make_async_remote_copy(
                src_ref=dchunk.at[g], dst_ref=dots.at[g, px * PY + py], send_sem=d_send.at[0], recv_sem=d_recv.at[g],
                device_id={"gx": lax.rem(px + dx, PX), "gy": lax.rem(py + dy, PY)}, device_id_type=MESH).start()

    def dot_wait(g):
        others = dots.at[g, 0:PX * PY - 1]
        pltpu.make_async_copy(others, others, d_recv.at[g]).wait()
        total = dots[g, 0]
        for slot in range(1, PX * PY):
            total = total + dots[g, slot]
        pltpu.make_async_copy(others, others, d_send.at[0]).wait()
        return [jnp.sum(total[i:i + 1], axis=1, keepdims=True) for i in range(total.shape[0])]

    def beside(field, i, value, s):
        return (field[i - 1], field[i + 1], pltpu.roll(value, s, 0), pltpu.roll(value, ROWS - s, 0),
                pltpu.roll(value, s, 1), pltpu.roll(value, NZ - s, 1))

    def coupled(coefs, field, i, value, s):
        near = beside(field, i, value, s)
        total = coefs[0, i] * near[0]
        for f in range(1, 6):
            total = total + coefs[f, i] * near[f]
        return total

    def prior_row(field, i):
        value = field[i]
        near = beside(field, i, value, 1)
        away = near[0] + near[1] + near[2] + near[3]
        away = away + jnp.where(lane >= 1, near[4], 0.0) + jnp.where(lane < NZ - 1, near[5], 0.0)
        return (6.5 * value - away)[0:NY]

    def swap(value, s, axis):
        index, size = (row, ROWS) if axis == 0 else (lane, NZ)
        return jnp.where((index & s) == 0, pltpu.roll(value, size - s, axis), pltpu.roll(value, s, axis))

    def block_sum(low, high, s):
        total = low + high
        total = total + swap(total, s, 1)
        return total + swap(total, s, 0)

    def pick_chunk(value):
        mine = ((row & 3) == 0) & ((row >> 2) == (lane & 3)) & (row < NY)
        return jnp.sum(jnp.where(mine, value, 0.0), axis=0, keepdims=True)

    def pick_ring(value, at):
        mine = ((row == NY) & ((lane & 3) == at)) | ((row == NY + H) & ((lane & 3) == 3 - at))
        return jnp.sum(jnp.where(mine, value, 0.0), axis=0, keepdims=True)

    def inside_yz(s):
        return (y_at >= s, y_at < GY - s, lane >= s, lane < NZ - s)

    def cell_inside(x):
        return jnp.where((x >= 0) & (x < PX * NX), ((y_at >= 0) & (y_at < GY)).astype(F32), 0.0) > 0.5

    own = lambda field: field.at[H:H + NX, 0:NY]
    loads = [pltpu.make_async_copy(source, target, in_sem.at[k]) for k, (source, target) in enumerate((
        (prior_ref, own(pr)), (logk_ref, own(lk)), (state_ref, own(st)), (cells_ref, cells_in), (prec_ref, prec_in),
        (grad_ref, grad)))]
    for load in loads:
        load.start()
    barrier = pltpu.get_barrier_semaphore()
    for k in range(8):
        @pl.when(exists(*DIRS[k]))
        def _(k=k):
            pl.semaphore_signal(barrier, inc=1, device_id={"gx": px + DIRS[k][0], "gy": py + DIRS[k][1]},
                                device_id_type=MESH)
    fields = [(lk, 0), (st, 1), (pr, 2), (src, 3), (z2.at[0], 4), (c0, 5), (z2.at[1], 6)]
    for field, slot in fields:
        halo_clear(field, yrecv.at[slot], NX, H)
    halo_clear(wdx, yrecv1, NX // 2, H1)
    share_clear()
    for field in (gp, zp1, vp1, zp2, vp2):
        def clear(i, field=field):
            field[i] = jnp.zeros((ROWS, NZ), F32)
        loop(1, RX - 1, clear)
    for i in (0, RX1 - 1):
        v1p[i] = jnp.zeros((ROWS, NZ), F32)
    def edges(field, slot):
        for i in range(NX):
            ystage[slot, 0, i] = field[H + i, 0:H]
            ystage[slot, 1, i] = field[H + i, NY - H:NY]
    loads[0].wait()
    edges(pr, 2)
    loads[1].wait()
    edges(lk, 0)
    loads[2].wait()
    edges(st, 1)
    across = jnp.where(px > 0, 1, 0) + jnp.where(px < PX - 1, 1, 0)
    along = jnp.where(py > 0, 1, 0) + jnp.where(py < PY - 1, 1, 0)
    pl.semaphore_wait(barrier, (across + 1) * (along + 1) - 1)

    send_prior, send_lk, send_st = fine(pr, 2, 1, 0), fine(lk, 0, H, 1), fine(st, 1, 2, 2)
    halo_send(*send_prior, count=4)
    halo_send(*send_lk, first=4)
    halo_send(*send_st, first=4)
    halo_send(*send_lk, count=4)
    halo_send(*send_st, count=4)

    loads[3].wait()
    loads[4].wait()
    cells = cells_in[...]
    at_xy = ((cells >> 15) - px * NX) * NY + ((cells >> 8) & (GY - 1)) - py * NY
    at_z = cells & (NZ - 1)
    hot_xy = lax.broadcasted_iota(jnp.int32, (NX * NY, SENSORS), 0) == at_xy
    hot_z = (lax.broadcasted_iota(jnp.int32, (NZ, SENSORS), 0) == at_z).astype(F32).astype(jnp.bfloat16)
    left = jnp.where(hot_xy, prec_in[...], 0.0)
    total = jnp.zeros((NX * NY, NZ), F32)
    for part in range(3):
        piece = left.astype(jnp.bfloat16)
        left = left - piece.astype(F32)
        total = total + lax.dot_general(piece, hot_z, (((1,), (1,)), ((), ())), preferred_element_type=F32)
    for i in range(NX):
        weight[i] = total[i * NY:(i + 1) * NY]

    loads[5].wait()
    halo_wait(*send_prior, count=4)

    def start_source(i):
        put(src, ystage.at[3], i + H, i, prior_row(pr, i + H) - grad[i])
    loop(0, NX, start_source, 8)
    halo_done(*send_prior, count=4)
    send_src = fine(src, 3, 2, 3)
    halo_send(*send_src)

    halo_wait(*send_lk)

    def start_cond(i):
        kk[i] = jnp.exp(lk[i])
    loop(0, RX, start_cond, 8)

    inner = inside_yz(1)

    def start_couplings(i):
        value = kk[i]
        x = px * NX + i - H
        near = beside(kk, i, value, 1)
        in_x = (x > 0, x < GX - 1)
        diag = None
        for f in range(6):
            ok = in_x[f] if f < 2 else inner[f - 2]
            a = 0.5 * (value + jnp.where(ok, near[f], value))
            ca[f, i] = jnp.where(ok, a, 0.0)
            diag = a if diag is None else diag + a
        wd[i] = jnp.where(cell_inside(x), OMEGA / diag, 0.0)
    loop(2, RX - 2, start_couplings, 12)

    def start_level1(i):
        c1[i] = block_sum(kk[2 * i], kk[2 * i + 1], 1) * 0.125
    loop(0, RX1, start_level1, 8)

    for i in range(2):
        chunk0[i:i + 1] = pick_chunk(block_sum(c1[H1 + 2 * i], c1[H1 + 2 * i + 1], 2) * 0.125)

    gather_send(0, "near")

    inner1 = inside_yz(2)

    def start_couplings1(i):
        value = c1[i]
        x = px * NX + 2 * i - H
        near = beside(c1, i, value, 2)
        in_x = (x > 0, x < GX - 2)
        diag = None
        for f in range(6):
            ok = in_x[f] if f < 2 else inner1[f - 2]
            a = value + jnp.where(ok, near[f], value)
            ca1[f, i] = jnp.where(ok, a, 0.0)
            diag = a if diag is None else diag + a
        wd1[i] = jnp.where(cell_inside(x), OMEGA / diag, 0.0)
    loop(1, RX1 - 1, start_couplings1, 6)
    for i in range(NX // 2):
        put(wdx, ystage1, H1 + i, i, wd1[H1 + i, 0:NY])
    halo_done(*send_lk)
    halo_send(*send_wd)

    halo_wait(*send_st)

    def start_state(i):
        value = st[i]
        x = px * NX + i - H
        near = beside(st, i, value, 1)
        in_x = (x > 0, x < GX - 1)
        diag = None
        for f in range(6):
            ok = in_x[f] if f < 2 else inner[f - 2]
            d = jnp.where(ok, 0.5 * (value - near[f]), value)
            cd[f, i] = jnp.where(ok, d, 0.0)
            diag = d if diag is None else diag + d
        sd[i] = diag
    loop(3, RX - 3, start_state, 10)


    def coarse_beside(values, d):
        v = values[d]
        zero = jnp.zeros_like(v)
        low = values[d - 1] if d > 0 else zero
        high = values[d + 1] if d < WIN - 1 else zero
        return (pltpu.roll(v, 1, 0), pltpu.roll(v, 7, 0),
                jnp.where(y_in > 0, pltpu.roll(v, 1, 1), pltpu.roll(low, NZ - 3, 1)),
                jnp.where(y_in < 3, pltpu.roll(v, NZ - 1, 1), pltpu.roll(high, 3, 1)),
                pltpu.roll(v, 4, 1), pltpu.roll(v, NZ - 4, 1))

    def coarse_couplings():
        values = [cond2[d] for d in range(WIN)]
        for d in range(WIN):
            place = py - REACH + d
            y = place * 4 + y_in
            inside = (row8 > 0, row8 < 7, y > 0, y < GY // 4 - 1, lane8 >= 4, lane8 < NZ - 4)
            diag = None
            for f, near in enumerate(coarse_beside(values, d)):
                a = 2.0 * (values[d] + jnp.where(inside[f], near, values[d]))
                ca2[f, d] = jnp.where(inside[f], a, 0.0)
                diag = a if diag is None else diag + a
            wd2[d] = jnp.where((place >= 0) & (place < PY), OMEGA / diag, 0.0)

    def coarse_solve():
        def sweep(values, low, high):
            out = list(values)
            for d in range(low, high):
                total = rhs2[d]
                for f, near in enumerate(coarse_beside(values, d)):
                    total = total + ca2[f, d] * near
                out[d] = (1.0 - OMEGA) * values[d] + wd2[d] * total
            return out
        values = sweep([wd2[d] * rhs2[d] for d in range(WIN)], 0, WIN)
        for s in range(2, COARSE_SWEEPS):
            values = sweep(values, 1, WIN - 1)
        for d in range(1, WIN - 1):
            sol[d] = values[d]
        cell = jnp.where(row < NY, row >> 2, jnp.where(row < NY + H, 0, 3))
        for i in range(4):
            x = 2 * px - 1 + i
            at = jnp.clip(x, 0, 7)
            own, high, low = (sol[d, pl.ds(at, 1), :] for d in (REACH, REACH + 1, REACH - 1))
            spread = jnp.where(row < NY, own, jnp.where(row < NY + H, high, low))
            spread = jnp.where((lane & 3) == cell, spread, 0.0)
            spread = spread + swap(spread, 1, 1)
            spread = spread + swap(spread, 2, 1)
            p2[i] = jnp.where((x >= 0) & (x < 8), spread, 0.0)

    def contribute(g, z, v, out):
        def restrict(i):
            parts = [(1.0 - OMEGA) * z[at] + coupled(ca, v, at, v[at], 1) for at in (2 * i, 2 * i + 1)
                     if H - out <= at < H + NX + out]
            total = block_sum(parts[0], parts[-1] if len(parts) > 1 else 0.0, 1)
            bp[i] = total
            v1p[i] = wd1[i] * total
        loop(1, RX1 - 1, restrict, RX1 - 2)

        def level1_residual(i):
            if i == 0:
                return ca1[0, 1] * v1p[1]
            if i == RX1 - 1:
                return ca1[1, RX1 - 2] * v1p[RX1 - 2]
            return (1.0 - OMEGA) * bp[i] + coupled(ca1, v1p, i, v1p[i], 2)
        for j, (q, at) in enumerate(((1, 1), (0, 0), (0, 1), (1, 0))):
            total = block_sum(level1_residual(2 * j), level1_residual(2 * j + 1), 2)
            chunk[g - 1, q, at:at + 1] = pick_chunk(total)
            ringed = pick_ring(total, q)
            if q == 0:
                chunk[g - 1, 2, at:at + 1] = ringed
            else:
                outer = ringed if j == 0 else jnp.concatenate([ringed, outer], axis=0)
        chunk[g - 1, 2] = chunk[g - 1, 2] + outer

    def solve(source, n, reach, finish, first, after=lambda: None):
        def presmooth(i):
            vv[i] = wd[i] * source[i]
        loop(H - 1 - reach, H + NX + 1 + reach, presmooth, NX + 2 + 2 * reach)
        if first:
            halo_wait(*send_wd)
        share_wait(n)
        if first:
            gather_cond()
            coarse_couplings()
        if n == 2:
            after()
        gather_rhs(n + 1)
        if n == 1:
            after()
        coarse_solve()
        if first:
            gather_end(0, 0)
            halo_done(*send_wd)
        gather_end(n + 1, 0)
        share_done(n)

        for i in range(RX1):
            v1[i] = v1[i] + p2[i // 2]

        def postsmooth1(i):
            v = v1[i]
            better = (1.0 - OMEGA) * v + wd1[i] * (b1[i] + coupled(ca1, v1, i, v, 2))
            for j in range(2):
                if H - 1 - reach <= 2 * i + j < H + NX + 1 + reach:
                    vv[2 * i + j] = vv[2 * i + j] + better
        loop(1, RX1 - 1, postsmooth1, 6)

        def postsmooth(i):
            v = vv[i]
            finish(i, (1.0 - OMEGA) * v + wd[i] * (source[i] + coupled(ca, vv, i, v, 1)))
        loop(H - reach, H + NX + reach, postsmooth, 10)

    def hessian(r, n, keep, during, after, arrive, between=lambda: None):
        def own_scaled(i):
            gp[i, 0:NY] = kk[i, 0:NY] * r[i, 0:NY]
        loop(H, H + NX, own_scaled, 8)

        def own_sensitivity(i):
            value = gp[i]
            z = sd[i] * value + coupled(cd, gp, i, value, 1)
            zp1[i] = z
            vp1[i] = wd[i] * z
        loop(H - 1, H + NX + 1, own_sensitivity, 10)
        contribute(2 * n + 1, zp1, vp1, 2)
        if n == 0:
            arrive()
            gather_send(0, "apart")
        gather_send(2 * n + 1)
        share_send(2 * n)
        if n != 0:
            arrive()

        def scaled(i):
            gg[i] = kk[i] * r[i]
        loop(2, RX - 2, scaled, 12)

        def sensitivity(i):
            value = gg[i]
            zz[i] = sd[i] * value + coupled(cd, gg, i, value, 1)
        loop(3, RX - 3, sensitivity, 10)

        second = z2.at[n]

        def weighted(i, value):
            wkeep[n, i - H] = value[0:NY]
            z = weight[i - H] * value[0:NY]
            put(second, ystage.at[4 + 2 * n], i, i - H, z)
            zp2[i, 0:NY] = z
            vp2[i, 0:NY] = wd[i, 0:NY] * z
        solve(zz, 2 * n, 0, weighted, n == 0, between)
        send_z2 = fine(second, 4 + 2 * n, 2, 1)
        if n == 1:
            during()
        contribute(2 * n + 2, zp2, vp2, 1)
        gather_send(2 * n + 2)
        share_send(2 * n + 1)
        halo_send(*send_z2)
        if n == 0:
            during()
        halo_wait(*send_z2)
        halo_done(*send_z2)

        def adjoint(i, value):
            pp[i] = value
        solve(second, 2 * n + 1, 1, adjoint, False, after)

        def assemble(i):
            p = pp[i]
            misfit = kk[i] * (sd[i] * p - coupled(cd, pp, i, p, 1))
            keep(i, misfit[0:NY] + prior_row(r, i))
        loop(H, H + NX, assemble, 8)

    def arrive_first():
        halo_wait(*send_src)
        halo_done(*send_src)
        halo_done(*send_st)

    zero = jnp.zeros((NY, NZ), F32)
    sums = {}

    def first_products():
        total = [zero, zero]
        for i in range(NX):
            r, w = src[i + H, 0:NY], wkeep[0, i]
            total[0] = total[0] + r * r
            total[1] = total[1] + weight[i] * w * w + r * prior_row(src, i + H)
        dot_prepare(0, (total[0], total[1], zero))

    def keep_first(i, value):
        put(c0, ystage.at[5], i, i - H, value)
    hessian(src, 0, keep_first, first_products, lambda: dot_send(0), arrive_first)
    send_c0 = fine(c0, 5, 2, 3)

    def arrive_second():
        halo_send(*send_c0)
        halo_wait(*send_c0)
        halo_done(*send_c0)

    def second_start():
        rr, rc = dot_wait(0)[:2]
        alpha = rr / rc
        sums.update(rr=rr, rc=rc, alpha=alpha)
        for i in range(H - 1, H + NX + 1):
            r1f[i] = src[i] - alpha * c0[i]
        total = [zero, zero, zero]
        for i in range(NX):
            r = r1f[i + H, 0:NY]
            total[0] = total[0] + r * r
            total[1] = total[1] + r * prior_row(r1f, i + H)
            total[2] = total[2] + r * c0[i + H, 0:NY]
        for j in range(3):
            partial[j] = total[j]

    def second_products():
        weighted = zero
        for i in range(NX):
            w = wkeep[0, i] - sums["alpha"] * wkeep[1, i]
            weighted = weighted + weight[i] * w * w
        dot_prepare(1, (partial[0], partial[1] + weighted, partial[2]))
        dot_send(1)

    def keep_second(i, value):
        kc[i - H] = value
    hessian(c0, 1, keep_second, second_products, lambda: None, arrive_second, second_start)

    norm, product, cross = dot_wait(1)
    alpha = sums["alpha"]
    ratio = norm / sums["rr"]
    beta = norm / (product + 2.0 * ratio * cross + ratio * ratio * sums["rc"])

    def finish(i):
        r, c, later = src[i + H, 0:NY], c0[i + H, 0:NY], r1f[i + H, 0:NY]
        curved = c - alpha * kc[i]
        step_ref[i] = alpha * r + beta * (later + ratio * r)
        resid_ref[i] = later - beta * (curved + ratio * c)
    loop(0, NX, finish)


def scratch():
    vmem = lambda *shape: pltpu.VMEM(shape, F32)
    fine = lambda *lead: vmem(*lead, RX, ROWS, NZ)
    level1 = lambda *lead: vmem(*lead, RX1, ROWS, NZ)
    dma = pltpu.SemaphoreType.DMA
    return [
        fine(), fine(), fine(), fine(), fine(), fine(2), level1(),
        vmem(7, 2, NX, H, NZ), vmem(7, 2, RX, H, NZ), vmem(2, NX // 2, H, NZ), vmem(2, RX1, H, NZ),
        vmem(NX, NY, NZ), pltpu.VMEM((1, SENSORS), jnp.int32), vmem(1, SENSORS), fine(), vmem(2, NX, NY, NZ), vmem(3, NY, NZ),
        fine(), fine(6), fine(), fine(6), fine(), fine(), fine(), fine(), vmem(1, 8, 128), fine(),
        level1(), level1(6), level1(), level1(), level1(), vmem(4, ROWS, NZ),
        fine(), fine(), fine(), fine(), fine(), level1(), level1(),
        vmem(4, 2, ROWS, NZ), vmem(4, 2, 2, 8, NZ), vmem(4, 2, ROWS, NZ), vmem(4, 2, 2, 8, NZ), vmem(4, 2, 2, 8, NZ),
        vmem(WIN, PX, 2, NZ), vmem(4, WIN, PX, PIECES, 2, NZ), vmem(2, NZ), vmem(4, PIECES, 2, NZ), vmem(WIN, 8, NZ), vmem(6, WIN, 8, NZ), vmem(WIN, 8, NZ),
        vmem(WIN, 8, NZ), vmem(WIN, 8, NZ), vmem(NX, NY, NZ), vmem(NX, NY, NZ),
        vmem(2, PX * PY, 3, 128), vmem(2, 3, 128),
        dma((3, 8)), dma((5, 8)), dma((2, WIN)), dma((3, WIN)), dma((1,)), dma((2,)), dma((6,)),
    ]


def on_device(log_conductivity, state, gradient, prior_sample, sensor_cells, noise_precision):
    block = jax.ShapeDtypeStruct(log_conductivity.shape, F32)
    vmem = pl.BlockSpec(memory_space=pltpu.VMEM)
    return pl.pallas_call(
        kernel,
        out_shape=(block, block),
        in_specs=[pl.BlockSpec(memory_space=pltpu.HBM)] * 6,
        out_specs=(vmem, vmem),
        scratch_shapes=scratch(),
        compiler_params=pltpu.CompilerParams(
            collective_id=0, has_side_effects=True, vmem_limit_bytes=24 * 1024 * 1024),
    )(*(pltpu.with_memory_space_constraint(x, pltpu.HBM) for x in (
        log_conductivity, state, gradient, prior_sample,
        sensor_cells.reshape(1, SENSORS), noise_precision.reshape(1, SENSORS))))


def solution(mesh):
    field, sensors = P(("ens", "gx"), "gy", None), P(("ens", "gx", "gy"))
    return jax.shard_map(
        on_device,
        mesh=mesh,
        in_specs=(field, field, field, field, sensors, sensors),
        out_specs=(field, field),
        check_vma=False,
    )
```
